32 devices in a mesh: rep: 8 (over z, core), tp: 4 (over y, x).
Axes of the slice: x: 2, y: 2, z: 4, core: 2. Of those that a mesh axis runs over, the one named last changes fastest.
Arguments:
- hidden: bfloat16 [32, 4608], P('rep'), may hold values from -6 to 6
- positions: int32 [32], P('rep'), may hold values from 1 to 1023
- key_cache: bfloat16 [32, 16, 1024, 128], P('rep', 'tp'), may hold values from -6 to 6
- value_cache: bfloat16 [32, 16, 1024, 128], P('rep', 'tp'), may hold values from -6 to 6
- norm_gain: float32 [4608], replicated, may hold values from 0.1 to 1.9
- q_proj: bfloat16 [4096, 4608], P(('rep', 'tp')), may hold values from -0.09375 to 0.09375
- k_proj: bfloat16 [2048, 4608], P(('rep', 'tp')), may hold values from -0.09375 to 0.09375
- v_proj: bfloat16 [2048, 4608], P(('rep', 'tp')), may hold values from -0.09375 to 0.09375
- o_proj: bfloat16 [4608, 4096], P(('rep', 'tp')), may hold values from -0.09375 to 0.09375
- post_gain: float32 [4608], P('tp'), may hold values from 0.1 to 1.9
Outputs:
- joined_qkv: bfloat16 [4608, 8192], P(None, 'tp')
- wo_heads: bfloat16 [4096, 4608], P('tp')
- attn_out: bfloat16 [32, 4608], P('rep', 'tp')
The draws below stay inside these ranges and needn't reach their ends.
All inputs are finite; a program needn't handle non-finite values.
Results may differ from the reference program's by a relative error of at most 0.008.
Values may be sent and summed in bfloat16 or wider, within the bound.
A program may use at most 128 MiB of HBM per device.

```python
import jax
import jax.numpy as jnp
from jax import lax

D = 4608
HEADS = 32
KV_HEADS = 16
HEAD_DIM = 128
CTX = 1024
BATCH = 32
QKV_COLS = 8192
N_TP = 4


def touch_ends(entries, own_key, smallest, high):
    index_at = [jax.random.randint(jax.random.fold_in(own_key, axis), (), 0, length) for axis, length in enumerate(entries.shape)]
    main_axis = entries.shape.index(max(entries.shape))
    next_to = index_at[:main_axis] + [(index_at[main_axis] + 1) % entries.shape[main_axis]] + index_at[main_axis + 1:]
    return entries.at[tuple(index_at)].set(smallest).at[tuple(next_to)].set(high)


def block_scale(key, dims, pieces, low, high):
    def one(position, parts):
        draws = jax.random.uniform(jax.random.fold_in(jax.random.fold_in(key, 6), position), (parts,), jnp.float32, low / len(pieces), high / len(pieces))
        return jnp.repeat(jnp.exp(draws), dims[position] // parts).reshape((-1,) + (1,) * (len(dims) - position - 1))

    loudness = one(*pieces[0])
    for cut in pieces[1:]:
        loudness = loudness * one(*cut)
    return loudness


def normal_values(key, shape, deviation, limit, cuts=(), kind=jnp.bfloat16):
    entries = deviation * jax.random.normal(key, shape, jnp.float32)
    if cuts:
        entries = entries * block_scale(key, shape, cuts, -0.22, 0.18)
    return jnp.clip(entries, -limit, limit).astype(kind)


def setup_inputs(seed: int = 0) -> dict:
    arg_keys = jax.random.split(jax.random.key(seed), 11)
    return {
        "hidden": normal_values(arg_keys[0], (BATCH, D), 1.0, 6.0, ((0, 8),)),
        "positions": touch_ends(jax.random.randint(arg_keys[1], (BATCH,), 1, CTX), jax.random.fold_in(arg_keys[1], 1), 1, CTX - 1).astype(jnp.int32),
        "key_cache": normal_values(arg_keys[2], (BATCH, KV_HEADS, CTX, HEAD_DIM), 1.0, 6.0, ((0, 8), (1, 4))),
        "value_cache": normal_values(arg_keys[3], (BATCH, KV_HEADS, CTX, HEAD_DIM), 1.0, 6.0, ((0, 8), (1, 4))),
        "norm_gain": jnp.clip(1.0 + 0.18 * jax.random.normal(arg_keys[4], (D,), jnp.float32), 0.1, 1.9),
        "q_proj": normal_values(arg_keys[5], (HEADS * HEAD_DIM, D), D ** -0.5, 0.09375, ((0, 32),)),
        "k_proj": normal_values(arg_keys[6], (KV_HEADS * HEAD_DIM, D), D ** -0.5, 0.09375, ((0, 32),)),
        "v_proj": normal_values(arg_keys[7], (KV_HEADS * HEAD_DIM, D), D ** -0.5, 0.09375, ((0, 32),)),
        "o_proj": normal_values(arg_keys[8], (D, HEADS * HEAD_DIM), (HEADS * HEAD_DIM) ** -0.5, 0.09375, ((0, 32),)),
        "post_gain": jnp.clip(1.0 + 0.18 * jax.random.normal(arg_keys[9], (D,), jnp.float32), 0.1, 1.9),
    }


score_scale = 144.0 ** (-0.5)
soft_cap = 50.0

def rms_scale(values, gain):
    mean_square = lax.optimization_barrier(jnp.mean(values * values, axis=-1, keepdims=True))
    return values * lax.rsqrt(mean_square + 1e-06) * gain

def rotate(values, positions):
    half = values.shape[-1] // 2
    freq = 10000.0 ** (-2.0 * jnp.arange(half, dtype=jnp.float32) / values.shape[-1])
    angle = positions.astype(jnp.float32)[:, None] * freq[None, :]
    cosine = jnp.cos(angle)[:, None, :]
    sine = jnp.sin(angle)[:, None, :]
    first = values[..., :half]
    second = values[..., half:]
    return jnp.concatenate([first * cosine - second * sine, second * cosine + first * sine], axis=-1)

def reference(hidden, positions, key_cache, value_cache, norm_gain, q_proj, k_proj, v_proj, o_proj, post_gain):
    q_cols = jnp.transpose(q_proj).reshape(D, N_TP, -1)
    k_cols = jnp.transpose(k_proj).reshape(D, N_TP, -1)
    v_cols = jnp.transpose(v_proj).reshape(D, N_TP, -1)
    joined_qkv = jnp.concatenate([q_cols, k_cols, v_cols], axis=2).reshape(D, QKV_COLS)
    wo_heads = jnp.transpose(o_proj)
    normed = rms_scale(hidden.astype(jnp.float32), norm_gain).astype(jnp.bfloat16)
    query = jnp.dot(normed, jnp.transpose(q_proj), preferred_element_type=jnp.float32).reshape(BATCH, HEADS, HEAD_DIM)
    keys_new = jnp.dot(normed, jnp.transpose(k_proj), preferred_element_type=jnp.float32).reshape(BATCH, KV_HEADS, HEAD_DIM)
    values_new = jnp.dot(normed, jnp.transpose(v_proj), preferred_element_type=jnp.float32).reshape(BATCH, KV_HEADS, HEAD_DIM)
    query_rot = rotate(query, positions).astype(jnp.bfloat16)
    rotated_keys = rotate(keys_new, positions).astype(jnp.bfloat16)
    values_rot = values_new.astype(jnp.bfloat16)
    group = HEADS // KV_HEADS
    grouped_heads = query_rot.astype(jnp.float32).reshape(BATCH, KV_HEADS, group, HEAD_DIM)
    scores = jnp.einsum('bkgd,bkld->bkgl', grouped_heads, key_cache.astype(jnp.float32)) * score_scale
    capped = soft_cap * jnp.tanh(scores / soft_cap)
    valid = jnp.arange(CTX, dtype=jnp.int32)[None, :] < positions[:, None]
    weight_raw = jnp.where(valid[:, None, None, :], jnp.exp(capped), 0.0)
    self_score = lax.optimization_barrier(jnp.sum(grouped_heads * rotated_keys.astype(jnp.float32)[:, :, None, :], axis=-1)) * score_scale
    self_raw = jnp.exp(soft_cap * jnp.tanh(self_score / soft_cap))
    denom = lax.optimization_barrier(jnp.sum(weight_raw, axis=-1)) + self_raw
    weights = (weight_raw / denom[..., None]).astype(jnp.bfloat16)
    self_weight = (self_raw / denom).astype(jnp.bfloat16)
    attention = jnp.einsum('bkgl,bkld->bkgd', weights.astype(jnp.float32), value_cache.astype(jnp.float32))
    attention = attention + self_weight.astype(jnp.float32)[..., None] * values_rot.astype(jnp.float32)[:, :, None, :]
    attention = attention.reshape(BATCH, HEADS * HEAD_DIM).astype(jnp.bfloat16)
    projected = jnp.dot(attention, wo_heads, preferred_element_type=jnp.float32)
    attn_out = rms_scale(projected, post_gain).astype(jnp.bfloat16)
    return (joined_qkv, wo_heads, attn_out)
```

```python
import functools

import jax
import jax.numpy as jnp
import numpy as np
from jax import lax
from jax.experimental import pallas as pl
from jax.experimental.pallas import tpu as pltpu
from jax.sharding import PartitionSpec as P

MESH = pl.DeviceIdType.MESH
score_scale = 144.0 ** (-0.5)
soft_cap = 50.0


def rms_scale(values, gain):
    mean_square = jnp.mean(values * values, axis=-1, keepdims=True)
    return values * lax.rsqrt(mean_square + 1e-06) * gain


def rotate(values, positions):
    half = values.shape[-1] // 2
    freq = 10000.0 ** (-2.0 * jnp.arange(half, dtype=jnp.float32) / values.shape[-1])
    angle = positions.astype(jnp.float32)[:, None] * freq[None, :]
    cosine = jnp.cos(angle)[:, None, :]
    sine = jnp.sin(angle)[:, None, :]
    first = values[..., :half]
    second = values[..., half:]
    return jnp.concatenate(
        [first * cosine - second * sine, second * cosine + first * sine], axis=-1
    )


def join_kernel(per_tp, q_rows, k_rows, *refs):
    slot = lax.rem(lax.axis_index("rep"), per_tp)
    parts, out_ref = refs[:-1], refs[-1]
    tp_count = parts[0].shape[0]
    q_all = tp_count * per_tp * q_rows
    k_all = tp_count * per_tp * k_rows
    for step in range(per_tp):
        who = lax.rem(slot + step, per_tp)
        q_ref, kv_ref = parts[2 * step], parts[2 * step + 1]
        for start, ref, low, rows in (
            (0, q_ref, 0, q_rows),
            (q_all, kv_ref, 0, k_rows),
            (q_all + k_all, kv_ref, k_rows, k_rows),
        ):
            block = ref[:, low : low + rows, :].reshape(tp_count * rows, -1)
            at = pl.multiple_of(start + who * (tp_count * rows), 128)
            out_ref[:, pl.ds(at, tp_count * rows)] = jnp.transpose(block)


def join(per_tp, pairs):
    tp_count, q_rows, width = pairs[0][0].shape
    k_rows = pairs[0][1].shape[1] // 2
    columns = tp_count * per_tp * (q_rows + 2 * k_rows)
    stripe = 256
    operands, specs = [], []
    for pair in pairs:
        for matrix in pair:
            operands.append(matrix)
            specs.append(
                pl.BlockSpec((tp_count, matrix.shape[1], stripe), lambda j: (0, 0, j))
            )
    size = width * columns * 2
    return pl.pallas_call(
        functools.partial(join_kernel, per_tp, q_rows, k_rows),
        grid=(width // stripe,),
        in_specs=specs,
        out_specs=pl.BlockSpec((stripe, columns), lambda j: (j, 0)),
        out_shape=jax.ShapeDtypeStruct((width, columns), jnp.bfloat16),
        cost_estimate=pl.CostEstimate(flops=0, bytes_accessed=2 * size, transcendentals=0),
        name="join",
    )(*operands)


def turn_kernel(rows_ref, out_ref):
    out_ref[...] = jnp.transpose(rows_ref[...])


def turn(rows):
    height, width = rows.shape
    stripe = 384 if height % 384 == 0 else 128
    return pl.pallas_call(
        turn_kernel,
        grid=(height // stripe,),
        in_specs=[pl.BlockSpec((stripe, width), lambda j: (j, 0))],
        out_specs=pl.BlockSpec((width, stripe), lambda j: (0, j)),
        out_shape=jax.ShapeDtypeStruct((width, height), rows.dtype),
        cost_estimate=pl.CostEstimate(
            flops=0, bytes_accessed=4 * height * width, transcendentals=0
        ),
        name="turn",
    )(rows)


def general_body(
    hidden, positions, key_cache, value_cache, norm_gain, q_proj, k_proj, v_proj, o_proj, post_gain
):
    tp_count = lax.axis_size("tp")
    replica_count = lax.axis_size("rep")
    per_tp = replica_count // tp_count
    model_width = hidden.shape[1]
    q_rows, k_rows = q_proj.shape[0], k_proj.shape[0]

    groups = [[i + per_tp * p for p in range(tp_count)] for i in range(per_tp)]
    shifts = [
        [
            (per_tp * p + (i + d) % per_tp, per_tp * p + i)
            for p in range(tp_count)
            for i in range(per_tp)
        ]
        for d in range(1, per_tp)
    ]

    def collect(rows):
        planes = lax.all_gather(rows[None], "rep", axis=0, tiled=True, axis_index_groups=groups)
        return lax.all_to_all(planes, "tp", split_axis=0, concat_axis=0, tiled=True)

    kv_rows = collect(jnp.concatenate([k_proj, v_proj], axis=0))
    split_cols = o_proj.reshape(o_proj.shape[0], tp_count, -1)
    rows_of_group = lax.all_to_all(split_cols, "tp", split_axis=1, concat_axis=0, tiled=True)

    batch, kv_local, length, head_dim = key_cache.shape

    def scatter_rows(values):
        wide = values.reshape(replica_count, batch, -1)
        by_rep = lax.all_to_all(wide, "rep", split_axis=0, concat_axis=0, tiled=True)
        return by_rep

    def to_block(by_rep):
        arrived = lax.all_to_all(by_rep, "tp", split_axis=0, concat_axis=0, tiled=True)
        arrived = arrived.reshape(tp_count, per_tp, batch, -1)
        return jnp.transpose(arrived, (2, 1, 0, 3))

    normed = rms_scale(hidden.astype(jnp.float32), norm_gain).astype(jnp.bfloat16)
    normed_all = lax.all_gather(normed, "rep", axis=0, tiled=True)
    contract = (((1,), (1,)), ((), ()))
    local = jnp.concatenate(
        [
            lax.dot_general(normed_all, matrix, contract, preferred_element_type=jnp.float32)
            for matrix in (q_proj, k_proj, v_proj)
        ],
        axis=1,
    )
    block = to_block(scatter_rows(local))
    q_local = tp_count * per_tp * q_rows // head_dim
    group = q_local // kv_local
    query = block[..., :q_rows].reshape(batch, q_local, head_dim)
    keys_new = block[..., q_rows : q_rows + k_rows].reshape(batch, kv_local, head_dim)
    values_new = block[..., q_rows + k_rows :].reshape(batch, kv_local, head_dim)
    query_rot = rotate(query, positions).astype(jnp.bfloat16)
    rotated_keys = rotate(keys_new, positions).astype(jnp.bfloat16)
    values_rot = values_new.astype(jnp.bfloat16)
    grouped_heads = query_rot.reshape(batch, kv_local, group, head_dim)
    scores = (
        jnp.einsum("bkgd,bkld->bkgl", grouped_heads, key_cache, preferred_element_type=jnp.float32)
        * score_scale
    )
    capped = soft_cap * jnp.tanh(scores / soft_cap)
    valid = jnp.arange(length, dtype=jnp.int32)[None, :] < positions[:, None]
    weight_raw = jnp.where(valid[:, None, None, :], jnp.exp(capped), 0.0)
    self_score = (
        jnp.einsum("juzy,juy->juz", grouped_heads, rotated_keys, preferred_element_type=jnp.float32)
        * score_scale
    )
    self_raw = jnp.exp(soft_cap * jnp.tanh(self_score / soft_cap))
    denom = jnp.sum(weight_raw, axis=-1) + self_raw
    weights = (weight_raw / denom[..., None]).astype(jnp.bfloat16)
    self_weight = (self_raw / denom).astype(jnp.bfloat16)
    attention = jnp.einsum(
        "bkgl,bkld->bkgd", weights, value_cache, preferred_element_type=jnp.float32
    )
    attention = (
        attention
        + self_weight.astype(jnp.float32)[..., None] * values_rot.astype(jnp.float32)[:, :, None, :]
    )
    attention = attention.reshape(batch, q_local * head_dim).astype(jnp.bfloat16)
    q_later, attention = lax.optimization_barrier((q_proj, attention))
    q_own = collect(q_later)
    pairs = [(q_own, kv_rows)]
    for shift in shifts:
        pairs.append((lax.ppermute(q_own, "rep", shift), lax.ppermute(kv_rows, "rep", shift)))
    joined_block = join(per_tp, pairs)
    own_all = lax.all_gather(attention, "tp", axis=1, tiled=True)
    attention_all = lax.all_gather(own_all, "rep", axis=0, tiled=True)
    projected = lax.dot_general(
        attention_all, o_proj, contract, preferred_element_type=jnp.float32
    )
    by_rep = scatter_rows(projected)
    share = to_block(by_rep).reshape(batch, -1)
    square = jnp.sum(share * share, axis=1)
    square_all = lax.all_gather(square[None], "tp", axis=0, tiled=True)
    multiplier = lax.rsqrt(jnp.sum(square_all, axis=0) / model_width + 1e-06)
    result = share * multiplier[:, None] * post_gain
    rows_of_group, result = lax.optimization_barrier((rows_of_group, result))
    complete_rows = lax.all_gather(rows_of_group, "rep", axis=0, tiled=True)
    out_block = turn(complete_rows.reshape(model_width, -1))
    return (joined_block, out_block, result.astype(jnp.bfloat16))


def move_kernel(
    sizes,
    q_ref, k_ref, v_ref, o_ref,
    hidden_ref, positions_ref, keys_ref, values_ref, gain_ref, post_ref, freq_ref,
    joined, heads, result,
    stage, q_own, kv_own, o_rows,
    hidden, positions, keys, values, gain, post, freq,
    fresh, q_heads, k_heads, v_heads, attended, partial, others, squares, squares_in,
    early_sems, share_send, share_recv, square_send, square_recv,
    local_sems, kv_sems, rows_send, rows_recv,
    line_send, line_recv, plane_send, plane_recv,
    twin_send, twin_recv, twin_wo_send, twin_wo_recv,
):
    planes, cores, cols, pieces = sizes
    rep, t = lax.axis_index("rep"), lax.axis_index("tp")
    z, c = rep // cores, lax.rem(rep, cores)
    other = 1 - c
    width = q_ref.shape[1]
    deep = width // pieces
    q_rows, k_rows = q_ref.shape[0], k_ref.shape[0]
    o_own = o_ref.shape[0]
    block = cols * cores * o_own
    half = heads.shape[0] // cores
    wo_rows = half // pieces
    moving = 2 * pieces
    total = 3 * pieces
    q_all = cores * cols * q_rows
    k_all = cores * cols * k_rows
    even = lax.rem(t, 2) == 0

    def at(zz, cc, tt):
        return (zz * cores + cc, tt)

    def column(tt, j, cc):
        parity = lax.rem(tt, 2)
        q_at = (cc * cols + tt) * q_rows
        kv_at = q_all + parity * k_all + (cc * cols + tt - parity) * k_rows
        is_q = (j < pieces).astype(jnp.int32)
        return pl.multiple_of(is_q * q_at + (1 - is_q) * kv_at, 128)

    def slot(tt, j, cc):
        row = pl.multiple_of(lax.rem(j, pieces) * deep, 128)
        return joined.at[pl.ds(row, deep), pl.ds(column(tt, j, cc), 128)]

    def wo_slot(zz, j, cc):
        row = pl.multiple_of(cc * half + (j - moving) * wo_rows, 128)
        col = pl.multiple_of(zz * block, 128)
        return heads.at[pl.ds(row, wo_rows), pl.ds(col, block)]

    def remote(src, dst, send, recv, device):
        return pltpu.make_async_remote_copy(
            src_ref=src, dst_ref=dst, send_sem=send, recv_sem=recv,
            device_id=device, device_id_type=MESH,
        )

    def line_copy(zz, j, way, device):
        return remote(stage.at[zz, j], stage.at[zz, j], line_send.at[way, zz, j],
                      line_recv.at[zz, j], device)

    def line_wo_copy(zz, j, way, device):
        return remote(wo_slot(zz, j, c), wo_slot(zz, j, c), line_send.at[way, zz, j],
                      line_recv.at[zz, j], device)

    def plane_copy(zz, j):
        return remote(stage.at[zz, j], slot(t, j, c), plane_send.at[zz, j],
                      plane_recv.at[t, j], at(z, c, zz))

    def plane_arrival(tt, j):
        return remote(slot(tt, j, c), slot(tt, j, c), plane_send.at[0, j],
                      plane_recv.at[tt, j], at(z, c, tt))

    def twin_copy(src, tt, j, cc):
        return remote(src, slot(tt, j, cc), twin_send.at[tt, j], twin_recv.at[tt, j], at(z, other, t))

    def twin_wo_copy(zz, j, cc):
        return remote(wo_slot(zz, j, cc), wo_slot(zz, j, cc), twin_wo_send.at[zz, j - moving],
                      twin_wo_recv.at[zz, j - moving], at(z, other, t))

    def rows_copy(dc, dt):
        cc, tt = lax.rem(c + dc, cores), lax.rem(t + dt, cols)
        mine = c * cols + t
        src_at = pl.multiple_of((tt * cores + cc) * half, 128)
        dst_at = pl.multiple_of(mine * o_own, 16)
        return remote(o_ref.at[:, pl.ds(src_at, half)], o_rows.at[pl.ds(dst_at, o_own), :],
                      rows_send.at[dc * cols + dt], rows_recv.at[mine], at(z, cc, tt))

    def rows_arrival(dc, dt):
        cc, tt = lax.rem(c + dc, cores), lax.rem(t + dt, cols)
        theirs = cc * cols + tt
        dst_at = pl.multiple_of(theirs * o_own, 16)
        view = o_rows.at[pl.ds(dst_at, o_own), :]
        return remote(view, view, rows_send.at[dc * cols + dt], rows_recv.at[theirs], at(z, cc, tt))

    peers = [(dc, dt) for dc in range(cores) for dt in range(cols) if dc or dt]

    barrier = pltpu.get_barrier_semaphore()
    for dc, dt in peers:
        pl.semaphore_signal(
            barrier, inc=1, device_id=at(z, lax.rem(c + dc, cores), lax.rem(t + dt, cols)),
            device_id_type=MESH)

    @pl.when(z > 0)
    def _():
        pl.semaphore_signal(barrier, inc=1, device_id=at(z - 1, c, t), device_id_type=MESH)

    @pl.when(z < planes - 1)
    def _():
        pl.semaphore_signal(barrier, inc=1, device_id=at(z + 1, c, t), device_id_type=MESH)

    load_q = pltpu.make_async_copy(q_ref, q_own, local_sems.at[0])
    load_q.start()
    mine = c * cols + t
    load_o = pltpu.make_async_copy(
        o_ref.at[:, pl.ds(pl.multiple_of((t * cores + c) * half, 128), half)],
        o_rows.at[pl.ds(pl.multiple_of(mine * o_own, 16), o_own), :], local_sems.at[1])
    load_o.start()
    load_k = pltpu.make_async_copy(k_ref, kv_own.at[pl.ds(0, k_rows)], local_sems.at[2])
    load_v = pltpu.make_async_copy(v_ref, kv_own.at[pl.ds(k_rows, k_rows)], local_sems.at[2])

    @pl.when(even)
    def _():
        load_k.start()

    @pl.when(jnp.logical_not(even))
    def _():
        load_v.start()

    give_v = remote(v_ref, kv_own.at[pl.ds(0, k_rows)], kv_sems.at[0], kv_sems.at[1], at(z, c, t + 1 - 2 * lax.rem(t, 2)))
    give_k = remote(k_ref, kv_own.at[pl.ds(k_rows, k_rows)], kv_sems.at[0], kv_sems.at[1], at(z, c, t + 1 - 2 * lax.rem(t, 2)))

    early = [
        pltpu.make_async_copy(source, target, early_sems.at[i])
        for i, (source, target) in enumerate((
            (hidden_ref, hidden), (positions_ref, positions), (gain_ref, gain), (post_ref, post),
            (freq_ref, freq), (keys_ref, keys), (values_ref, values)))
    ]

    batch, kv_local, length, head_dim = keys_ref.shape
    q_local = q_all // head_dim
    group = q_local // kv_local
    f32, bf16 = jnp.float32, jnp.bfloat16

    def project():
        for copy in early[:5]:
            copy.wait()
        wide = hidden[...].astype(f32)
        mean_square = jnp.mean(wide * wide, axis=-1, keepdims=True)
        normed = (wide * lax.rsqrt(mean_square + 1e-06) * gain[...]).astype(bf16)

        def columns(i, carry):
            span = pl.ds(pl.multiple_of(i * 256, 256), 256)
            fresh[:, span] = jnp.dot(normed, joined[:, span], preferred_element_type=f32)
            return carry

        lax.fori_loop(0, fresh.shape[1] // 256, columns, 0)
        angle = jnp.concatenate(
            [positions[b].astype(f32) * freq[...] for b in range(batch)], axis=0)
        cosine, sine = jnp.cos(angle), jnp.sin(angle)
        lane = lax.broadcasted_iota(jnp.int32, angle.shape, 1)
        sine = jnp.where(lane < head_dim // 2, -sine, sine)

        def turned(start):
            x = fresh[:, start : start + head_dim]
            swapped = pltpu.roll(x, head_dim // 2, 1)
            return (x * cosine + swapped * sine).astype(bf16).astype(f32)

        for h in range(kv_local):
            key = turned(q_all + h * head_dim)
            at_v = q_all + k_all + h * head_dim
            value = fresh[:, at_v : at_v + head_dim].astype(bf16).astype(f32)
            for g in range(group):
                n = h * group + g
                query = turned(n * head_dim)
                for b in range(batch):
                    q_heads[b, n : n + 1, :] = query[b : b + 1]
                    k_heads[b, n : n + 1, :] = key[b : b + 1]
                    v_heads[b, n : n + 1, :] = value[b : b + 1]

    def attend():
        for copy in early[5:]:
            copy.wait()
        over = (((1,), (1,)), ((), ()))
        slots = lax.broadcasted_iota(jnp.int32, (q_local, length), 1)
        owner = lax.broadcasted_iota(jnp.int32, (q_local, 1), 0) // group
        for b in range(batch):
            query = q_heads[b]
            narrow = query.astype(bf16)
            scores = jnp.zeros((q_local, length), f32)
            for h in range(kv_local):
                one = lax.dot_general(narrow, keys[b, h], over, preferred_element_type=f32)
                scores = jnp.where(owner == h, one, scores)
            raw = jnp.exp(soft_cap * jnp.tanh(scores * score_scale / soft_cap))
            raw = jnp.where(slots < positions[b], raw, 0.0)
            self_score = jnp.sum(query * k_heads[b], axis=-1, keepdims=True) * score_scale
            self_raw = jnp.exp(soft_cap * jnp.tanh(self_score / soft_cap))
            denom = jnp.sum(raw, axis=-1, keepdims=True) + self_raw
            weights = (raw / denom).astype(bf16)
            self_weight = (self_raw / denom).astype(bf16).astype(f32)
            mixed = jnp.zeros((q_local, head_dim), f32)
            for h in range(kv_local):
                one = jnp.dot(weights, values[b, h], preferred_element_type=f32)
                mixed = jnp.where(owner == h, one, mixed)
            mixed = mixed + self_weight * v_heads[b]
            for n in range(q_local):
                attended[b : b + 1, n * head_dim : (n + 1) * head_dim] = mixed[n : n + 1]

    def share_copy(p, device):
        return remote(partial.at[p], others.at[t], share_send.at[p], share_recv.at[t], device)

    def square_copy(p):
        return remote(squares, squares_in.at[t], square_send.at[p], square_recv.at[t], at(z, c, p))

    def finish():
        narrow = attended[...].astype(bf16)

        def slices(p, carry):
            span = pl.ds(pl.multiple_of(p * block, 128), block)
            partial[p] = jnp.dot(narrow, heads[:, span], preferred_element_type=f32)
            return carry

        lax.fori_loop(0, cols, slices, 0)
        for dt in range(1, cols):
            p = lax.rem(t + dt, cols)
            share_copy(p, at(z, c, p)).start()
        share = partial[t]
        for dt in range(1, cols):
            p = lax.rem(t + dt, cols)
            remote(others.at[p], others.at[p], share_send.at[p], share_recv.at[p], at(z, c, p)).wait_recv()
            share = share + others[p]
        square = jnp.sum(share * share, axis=-1, keepdims=True)
        squares[...] = jnp.broadcast_to(square, squares.shape)
        for dt in range(1, cols):
            square_copy(lax.rem(t + dt, cols)).start()
        total_square = square
        for dt in range(1, cols):
            p = lax.rem(t + dt, cols)
            remote(squares_in.at[p], squares_in.at[p], square_send.at[p], square_recv.at[p],
                   at(z, c, p)).wait_recv()
            total_square = total_square + squares_in[p][:, :1]
        multiplier = lax.rsqrt(total_square / width + 1e-06)
        result[...] = (share * multiplier * post[...]).astype(result.dtype)
        for dt in range(1, cols):
            p = lax.rem(t + dt, cols)
            share_copy(p, at(z, c, p)).wait_send()
            square_copy(p).wait_send()

    def prepare(j):
        @pl.when(j < pieces)
        def _():
            span = pl.ds(pl.multiple_of(j * deep, 128), deep)
            stage[z, j] = jnp.transpose(q_own[:, span])

        @pl.when(j == pieces)
        def _():
            @pl.when(even)
            def _():
                load_k.wait()
                give_k.wait_recv()

            @pl.when(jnp.logical_not(even))
            def _():
                load_v.wait()
                give_v.wait_recv()

        @pl.when(jnp.logical_and(j >= pieces, j < moving))
        def _():
            span = pl.ds(pl.multiple_of((j - pieces) * deep, 128), deep)
            stage[z, j] = jnp.transpose(kv_own[:, span])

        @pl.when(j == moving)
        def _():
            load_o.wait()
            for dc, dt in peers:
                rows_arrival(dc, dt).wait_recv()

        @pl.when(jnp.logical_and(j >= moving, j < total))
        def _():
            col = pl.multiple_of((j - moving) * wo_rows, 128)
            row = pl.multiple_of(c * half + (j - moving) * wo_rows, 128)
            heads[pl.ds(row, wo_rows), pl.ds(pl.multiple_of(z * block, 128), block)] = jnp.transpose(
                o_rows[:, pl.ds(col, wo_rows)])

    def send_line(zz, j, way):
        target = at(z - 1, c, t) if way == 0 else at(z + 1, c, t)
        room = z > 0 if way == 0 else z < planes - 1

        @pl.when(jnp.logical_and(room, j < moving))
        def _():
            line_copy(zz, j, way, target).start()

        @pl.when(jnp.logical_and(room, j >= moving))
        def _():
            line_wo_copy(zz, j, way, target).start()

    def wait_line(zz, j):
        @pl.when(j < moving)
        def _():
            line_copy(zz, j, 0, at(z, other, t)).wait_recv()

        @pl.when(j >= moving)
        def _():
            line_wo_copy(zz, j, 0, at(z, other, t)).wait_recv()

    def deliver(zz, j):
        @pl.when(jnp.logical_and(j < moving, t != zz))
        def _():
            plane_copy(zz, j).start()

        @pl.when(jnp.logical_and(j < moving, t == zz))
        def _():
            row = pl.multiple_of(lax.rem(j, pieces) * deep, 128)
            joined[pl.ds(row, deep), pl.ds(column(t, j, c), 128)] = stage[zz, j]
            twin_copy(stage.at[zz, j], t, j, c).start()

        @pl.when(j >= moving)
        def _():
            twin_wo_copy(zz, j, c).start()

    for copy in early[:5]:
        copy.start()
    load_q.wait()
    prepare(jnp.int32(0))
    prepare(jnp.int32(1))
    n_line = (z > 0).astype(jnp.int32) + (z < planes - 1).astype(jnp.int32)
    pl.semaphore_wait(barrier, len(peers) + n_line)

    def rounds(r, carry):
        @pl.when(r < total)
        def _():
            send_line(z, r, 0)
            send_line(z, r, 1)
            deliver(z, r)

        @pl.when(r == 0)
        def _():
            @pl.when(even)
            def _():
                give_v.start()

            @pl.when(jnp.logical_not(even))
            def _():
                give_k.start()

        @pl.when(r == 1)
        def _():
            for dc, dt in peers:
                rows_copy(dc, dt).start()
            for copy in early[5:]:
                copy.start()

        @pl.when(r + 2 < total)
        def _():
            prepare(r + 2)

        for k in range(1, planes):
            for way in (0, 1):
                zz = z + k if way == 0 else z - k
                j = r - k
                inside = zz < planes if way == 0 else zz >= 0

                @pl.when(jnp.logical_and(inside, jnp.logical_and(j >= 0, j < total)))
                def _():
                    wait_line(zz, j)
                    send_line(zz, j, way)
                    deliver(zz, j)

        far = jnp.where(z > t, z - t, t - z)
        j = r - far - 1

        @pl.when(jnp.logical_and(j >= 0, j < moving))
        def _():
            for dt in range(1, cols):
                tt = lax.rem(t + dt, cols)
                plane_arrival(tt, j).wait_recv()
                twin_copy(slot(tt, j, c), tt, j, c).start()

        @pl.when(r == moving + 1 + far)
        def _():
            lax.fori_loop(0, moving, twin_in, 0)
            project()

        @pl.when(r == moving + 2 + far)
        def _():
            attend()
        return carry

    def twin_in(j, carry):
        for tt in range(cols):
            twin_copy(slot(tt, j, other), tt, j, other).wait_recv()
        return carry

    lax.fori_loop(0, total + planes - 1, rounds, 0)

    def twin_wo_in(j, carry):
        for zz in range(planes):
            twin_wo_copy(zz, j, other).wait_recv()
        return carry

    lax.fori_loop(moving, total, twin_wo_in, 0)
    finish()

    def sent(j, carry):
        for zz in range(planes):
            for way in (0, 1):
                room = z > 0 if way == 0 else z < planes - 1
                passes = z <= zz if way == 0 else z >= zz

                @pl.when(jnp.logical_and(room, passes))
                def _():
                    @pl.when(j < moving)
                    def _():
                        line_copy(zz, j, way, at(z, other, t)).wait_send()

                    @pl.when(j >= moving)
                    def _():
                        line_wo_copy(zz, j, way, at(z, other, t)).wait_send()

            @pl.when(jnp.logical_and(j < moving, t != zz))
            def _():
                plane_copy(zz, j).wait_send()

            @pl.when(j < moving)
            def _():
                twin_copy(slot(zz, j, c), zz, j, c).wait_send()

            @pl.when(j >= moving)
            def _():
                twin_wo_copy(zz, j, c).wait_send()
        return carry

    lax.fori_loop(0, total, sent, 0)
    for dc, dt in peers:
        rows_copy(dc, dt).wait_send()

    @pl.when(even)
    def _():
        give_v.wait_send()

    @pl.when(jnp.logical_not(even))
    def _():
        give_k.wait_send()


def line_body(hidden, positions, key_cache, value_cache, norm_gain, q_proj, k_proj, v_proj, o_proj, post_gain):
    cols = lax.axis_size("tp")
    cores = 2
    planes = lax.axis_size("rep") // cores
    pieces = 4
    width = q_proj.shape[1]
    deep = width // pieces
    q_rows, k_rows, o_own = q_proj.shape[0], k_proj.shape[0], o_proj.shape[0]
    features = o_proj.shape[1] // cols
    columns = cores * cols * (q_rows + 2 * k_rows)
    model = o_own * cores * cols * planes
    bf = jnp.bfloat16
    dma = pltpu.SemaphoreType.DMA
    hbm = pl.BlockSpec(memory_space=pltpu.HBM)
    f32 = jnp.float32
    batch, kv_local, length, head_dim = key_cache.shape
    q_local = cores * cols * q_rows // head_dim
    half = head_dim // 2
    freq = 10000.0 ** (-2.0 * np.arange(half) / head_dim)
    freq = jnp.asarray(np.concatenate([freq, freq])[None], f32)
    share = post_gain.shape[0]
    moving, total = 2 * pieces, 3 * pieces
    out = pl.pallas_call(
        functools.partial(move_kernel, (planes, cores, cols, pieces)),
        in_specs=[hbm] * 11,
        out_shape=[
            pltpu.VMEM((width, columns), bf),
            pltpu.VMEM((features, model), bf),
            jax.ShapeDtypeStruct((hidden.shape[0], post_gain.shape[0]), bf),
        ],
        out_specs=[pl.BlockSpec(memory_space=pltpu.VMEM)] * 3,
        scratch_shapes=[
            pltpu.VMEM((planes, moving, deep, 128), bf),
            pltpu.VMEM((q_rows, width), bf),
            pltpu.VMEM((2 * k_rows, width), bf),
            pltpu.VMEM((cores * cols * o_own, features // cores), bf),
            pltpu.VMEM(hidden.shape, bf), pltpu.SMEM(positions.shape, jnp.int32),
            pltpu.VMEM(key_cache.shape, bf), pltpu.VMEM(value_cache.shape, bf),
            pltpu.VMEM((1, width), f32), pltpu.VMEM((1, share), f32), pltpu.VMEM((1, head_dim), f32),
            pltpu.VMEM((batch, columns), f32), pltpu.VMEM((batch, q_local, head_dim), f32),
            pltpu.VMEM((batch, q_local, head_dim), f32), pltpu.VMEM((batch, q_local, head_dim), f32),
            pltpu.VMEM((batch, features), f32), pltpu.VMEM((cols, batch, share), f32),
            pltpu.VMEM((cols, batch, share), f32), pltpu.VMEM((batch, 128), f32),
            pltpu.VMEM((cols, batch, 128), f32),
            dma((7,)), dma((cols,)), dma((cols,)), dma((cols,)), dma((cols,)),
            dma((3,)), dma((2,)), dma((cores * cols,)), dma((cores * cols,)),
            dma((2, planes, total)), dma((planes, total)), dma((planes, moving)), dma((cols, moving)),
            dma((cols, moving)), dma((cols, moving)), dma((planes, pieces)), dma((planes, pieces)),
        ],
        compiler_params=pltpu.CompilerParams(
            collective_id=0, has_side_effects=True, vmem_limit_bytes=VLIM),
        name="move",
    )(q_proj, k_proj, v_proj, o_proj, hidden, positions, key_cache, value_cache,
      norm_gain[None], post_gain[None], freq)
    return tuple(out)

VLIM = 34 * 2**20


def body(*args):
    cols, reps = lax.axis_size("tp"), lax.axis_size("rep")
    key_cache, q_proj, k_proj, o_proj = args[2], args[5], args[6], args[8]
    lanes = 128
    fits = (
        reps == 2 * cols
        and cols % 2 == 0
        and key_cache.shape[3] == lanes
        and q_proj.shape[0] == lanes
        and 2 * k_proj.shape[0] == lanes
        and o_proj.shape[0] % 16 == 0
        and q_proj.shape[1] % (4 * lanes) == 0
        and o_proj.shape[1] % (8 * lanes * cols) == 0
        and (2 * cols * o_proj.shape[0]) % lanes == 0
    )
    return (line_body if fits else general_body)(*args)


def solution(mesh):
    in_specs = (
        P("rep", None), P("rep"), P("rep", "tp", None, None), P("rep", "tp", None, None), P(),
        P(("rep", "tp"), None), P(("rep", "tp"), None), P(("rep", "tp"), None), P(("rep", "tp"), None), P("tp"),
    )
    out_specs = (P(None, "tp"), P("tp", None), P("rep", "tp"))
    return jax.shard_map(body, mesh=mesh, in_specs=in_specs, out_specs=out_specs, check_vma=False)
```

```python
import functools

import jax
import jax.numpy as jnp
import numpy as np
from jax import lax
from jax.experimental import pallas as pl
from jax.experimental.pallas import tpu as pltpu
from jax.sharding import PartitionSpec as P

MESH = pl.DeviceIdType.MESH
score_scale = 144.0 ** (-0.5)
soft_cap = 50.0


def rms_scale(values, gain):
    mean_square = jnp.mean(values * values, axis=-1, keepdims=True)
    return values * lax.rsqrt(mean_square + 1e-06) * gain


def rotate(values, positions):
    half = values.shape[-1] // 2
    freq = 10000.0 ** (-2.0 * jnp.arange(half, dtype=jnp.float32) / values.shape[-1])
    angle = positions.astype(jnp.float32)[:, None] * freq[None, :]
    cosine = jnp.cos(angle)[:, None, :]
    sine = jnp.sin(angle)[:, None, :]
    first = values[..., :half]
    second = values[..., half:]
    return jnp.concatenate(
        [first * cosine - second * sine, second * cosine + first * sine], axis=-1
    )


def join_kernel(per_tp, q_rows, k_rows, *refs):
    slot = lax.rem(lax.axis_index("rep"), per_tp)
    parts, out_ref = refs[:-1], refs[-1]
    tp_count = parts[0].shape[0]
    q_all = tp_count * per_tp * q_rows
    k_all = tp_count * per_tp * k_rows
    for step in range(per_tp):
        who = lax.rem(slot + step, per_tp)
        q_ref, kv_ref = parts[2 * step], parts[2 * step + 1]
        for start, ref, low, rows in (
            (0, q_ref, 0, q_rows),
            (q_all, kv_ref, 0, k_rows),
            (q_all + k_all, kv_ref, k_rows, k_rows),
        ):
            block = ref[:, low : low + rows, :].reshape(tp_count * rows, -1)
            at = pl.multiple_of(start + who * (tp_count * rows), 128)
            out_ref[:, pl.ds(at, tp_count * rows)] = jnp.transpose(block)


def join(per_tp, pairs):
    tp_count, q_rows, width = pairs[0][0].shape
    k_rows = pairs[0][1].shape[1] // 2
    columns = tp_count * per_tp * (q_rows + 2 * k_rows)
    stripe = 256
    operands, specs = [], []
    for pair in pairs:
        for matrix in pair:
            operands.append(matrix)
            specs.append(
                pl.BlockSpec((tp_count, matrix.shape[1], stripe), lambda j: (0, 0, j))
            )
    size = width * columns * 2
    return pl.pallas_call(
        functools.partial(join_kernel, per_tp, q_rows, k_rows),
        grid=(width // stripe,),
        in_specs=specs,
        out_specs=pl.BlockSpec((stripe, columns), lambda j: (j, 0)),
        out_shape=jax.ShapeDtypeStruct((width, columns), jnp.bfloat16),
        cost_estimate=pl.CostEstimate(flops=0, bytes_accessed=2 * size, transcendentals=0),
        name="join",
    )(*operands)


def turn_kernel(rows_ref, out_ref):
    out_ref[...] = jnp.transpose(rows_ref[...])


def turn(rows):
    height, width = rows.shape
    stripe = 384 if height % 384 == 0 else 128
    return pl.pallas_call(
        turn_kernel,
        grid=(height // stripe,),
        in_specs=[pl.BlockSpec((stripe, width), lambda j: (j, 0))],
        out_specs=pl.BlockSpec((width, stripe), lambda j: (0, j)),
        out_shape=jax.ShapeDtypeStruct((width, height), rows.dtype),
        cost_estimate=pl.CostEstimate(
            flops=0, bytes_accessed=4 * height * width, transcendentals=0
        ),
        name="turn",
    )(rows)


def general_body(
    hidden, positions, key_cache, value_cache, norm_gain, q_proj, k_proj, v_proj, o_proj, post_gain
):
    tp_count = lax.axis_size("tp")
    replica_count = lax.axis_size("rep")
    per_tp = replica_count // tp_count
    model_width = hidden.shape[1]
    q_rows, k_rows = q_proj.shape[0], k_proj.shape[0]

    groups = [[i + per_tp * p for p in range(tp_count)] for i in range(per_tp)]
    shifts = [
        [
            (per_tp * p + (i + d) % per_tp, per_tp * p + i)
            for p in range(tp_count)
            for i in range(per_tp)
        ]
        for d in range(1, per_tp)
    ]

    def collect(rows):
        planes = lax.all_gather(rows[None], "rep", axis=0, tiled=True, axis_index_groups=groups)
        return lax.all_to_all(planes, "tp", split_axis=0, concat_axis=0, tiled=True)

    kv_rows = collect(jnp.concatenate([k_proj, v_proj], axis=0))
    split_cols = o_proj.reshape(o_proj.shape[0], tp_count, -1)
    rows_of_group = lax.all_to_all(split_cols, "tp", split_axis=1, concat_axis=0, tiled=True)

    batch, kv_local, length, head_dim = key_cache.shape

    def scatter_rows(values):
        wide = values.reshape(replica_count, batch, -1)
        by_rep = lax.all_to_all(wide, "rep", split_axis=0, concat_axis=0, tiled=True)
        return by_rep

    def to_block(by_rep):
        arrived = lax.all_to_all(by_rep, "tp", split_axis=0, concat_axis=0, tiled=True)
        arrived = arrived.reshape(tp_count, per_tp, batch, -1)
        return jnp.transpose(arrived, (2, 1, 0, 3))

    normed = rms_scale(hidden.astype(jnp.float32), norm_gain).astype(jnp.bfloat16)
    normed_all = lax.all_gather(normed, "rep", axis=0, tiled=True)
    contract = (((1,), (1,)), ((), ()))
    local = jnp.concatenate(
        [
            lax.dot_general(normed_all, matrix, contract, preferred_element_type=jnp.float32)
            for matrix in (q_proj, k_proj, v_proj)
        ],
        axis=1,
    )
    block = to_block(scatter_rows(local))
    q_local = tp_count * per_tp * q_rows // head_dim
    group = q_local // kv_local
    query = block[..., :q_rows].reshape(batch, q_local, head_dim)
    keys_new = block[..., q_rows : q_rows + k_rows].reshape(batch, kv_local, head_dim)
    values_new = block[..., q_rows + k_rows :].reshape(batch, kv_local, head_dim)
    query_rot = rotate(query, positions).astype(jnp.bfloat16)
    rotated_keys = rotate(keys_new, positions).astype(jnp.bfloat16)
    values_rot = values_new.astype(jnp.bfloat16)
    grouped_heads = query_rot.reshape(batch, kv_local, group, head_dim)
    scores = (
        jnp.einsum("bkgd,bkld->bkgl", grouped_heads, key_cache, preferred_element_type=jnp.float32)
        * score_scale
    )
    capped = soft_cap * jnp.tanh(scores / soft_cap)
    valid = jnp.arange(length, dtype=jnp.int32)[None, :] < positions[:, None]
    weight_raw = jnp.where(valid[:, None, None, :], jnp.exp(capped), 0.0)
    self_score = (
        jnp.einsum("juzy,juy->juz", grouped_heads, rotated_keys, preferred_element_type=jnp.float32)
        * score_scale
    )
    self_raw = jnp.exp(soft_cap * jnp.tanh(self_score / soft_cap))
    denom = jnp.sum(weight_raw, axis=-1) + self_raw
    weights = (weight_raw / denom[..., None]).astype(jnp.bfloat16)
    self_weight = (self_raw / denom).astype(jnp.bfloat16)
    attention = jnp.einsum(
        "bkgl,bkld->bkgd", weights, value_cache, preferred_element_type=jnp.float32
    )
    attention = (
        attention
        + self_weight.astype(jnp.float32)[..., None] * values_rot.astype(jnp.float32)[:, :, None, :]
    )
    attention = attention.reshape(batch, q_local * head_dim).astype(jnp.bfloat16)
    q_later, attention = lax.optimization_barrier((q_proj, attention))
    q_own = collect(q_later)
    pairs = [(q_own, kv_rows)]
    for shift in shifts:
        pairs.append((lax.ppermute(q_own, "rep", shift), lax.ppermute(kv_rows, "rep", shift)))
    joined_block = join(per_tp, pairs)
    own_all = lax.all_gather(attention, "tp", axis=1, tiled=True)
    attention_all = lax.all_gather(own_all, "rep", axis=0, tiled=True)
    projected = lax.dot_general(
        attention_all, o_proj, contract, preferred_element_type=jnp.float32
    )
    by_rep = scatter_rows(projected)
    share = to_block(by_rep).reshape(batch, -1)
    square = jnp.sum(share * share, axis=1)
    square_all = lax.all_gather(square[None], "tp", axis=0, tiled=True)
    multiplier = lax.rsqrt(jnp.sum(square_all, axis=0) / model_width + 1e-06)
    result = share * multiplier[:, None] * post_gain
    rows_of_group, result = lax.optimization_barrier((rows_of_group, result))
    complete_rows = lax.all_gather(rows_of_group, "rep", axis=0, tiled=True)
    out_block = turn(complete_rows.reshape(model_width, -1))
    return (joined_block, out_block, result.astype(jnp.bfloat16))


def move_kernel(
    sizes,
    q_ref, k_ref, v_ref, o_ref,
    hidden_ref, positions_ref, keys_ref, values_ref, gain_ref, post_ref, freq_ref,
    joined, heads, result,
    stage, q_own, kv_own, o_rows,
    hidden, positions, keys, values, gain, post, freq,
    fresh, q_heads, k_heads, v_heads, attended, partial, partial_sum, others,
    early_sems, share_send, share_recv,
    local_sems, kv_sems, rows_send, rows_recv,
    line_send, line_recv, plane_send, plane_recv,
    twin_send, twin_recv, twin_wo_send, twin_wo_recv,
):
    planes, cores, cols, pieces = sizes
    rep, t = lax.axis_index("rep"), lax.axis_index("tp")
    z, c = rep // cores, lax.rem(rep, cores)
    other = 1 - c
    width = q_ref.shape[1]
    deep = width // pieces
    q_rows, k_rows = q_ref.shape[0], k_ref.shape[0]
    o_own = o_ref.shape[0]
    block = cols * cores * o_own
    half = heads.shape[0] // cores
    wo_rows = half // pieces
    moving = 2 * pieces
    total = 3 * pieces
    q_all = cores * cols * q_rows
    k_all = cores * cols * k_rows
    even = lax.rem(t, 2) == 0

    def at(zz, cc, tt):
        return (zz * cores + cc, tt)

    def column(tt, j, cc):
        parity = lax.rem(tt, 2)
        q_at = (cc * cols + tt) * q_rows
        kv_at = q_all + parity * k_all + (cc * cols + tt - parity) * k_rows
        is_q = (j < pieces).astype(jnp.int32)
        return pl.multiple_of(is_q * q_at + (1 - is_q) * kv_at, 128)

    def slot(tt, j, cc):
        row = pl.multiple_of(lax.rem(j, pieces) * deep, 128)
        return joined.at[pl.ds(row, deep), pl.ds(column(tt, j, cc), 128)]

    def wo_slot(zz, j, cc):
        row = pl.multiple_of(cc * half + (j - moving) * wo_rows, 128)
        col = pl.multiple_of(zz * block, 128)
        return heads.at[pl.ds(row, wo_rows), pl.ds(col, block)]

    def remote(src, dst, send, recv, device):
        return pltpu.make_async_remote_copy(
            src_ref=src, dst_ref=dst, send_sem=send, recv_sem=recv,
            device_id=device, device_id_type=MESH,
        )

    def line_copy(zz, j, way, device):
        return remote(stage.at[zz, j], stage.at[zz, j], line_send.at[way, zz, j],
                      line_recv.at[zz, j], device)

    def line_wo_copy(zz, j, way, device):
        return remote(wo_slot(zz, j, c), wo_slot(zz, j, c), line_send.at[way, zz, j],
                      line_recv.at[zz, j], device)

    def plane_copy(zz, j):
        return remote(stage.at[zz, j], slot(t, j, c), plane_send.at[zz, j],
                      plane_recv.at[t, j], at(z, c, zz))

    def plane_arrival(tt, j):
        return remote(slot(tt, j, c), slot(tt, j, c), plane_send.at[0, j],
                      plane_recv.at[tt, j], at(z, c, tt))

    def twin_copy(src, tt, j, cc):
        return remote(src, slot(tt, j, cc), twin_send.at[tt, j], twin_recv.at[tt, j], at(z, other, t))

    def twin_wo_copy(zz, j, cc):
        return remote(wo_slot(zz, j, cc), wo_slot(zz, j, cc), twin_wo_send.at[zz, j - moving],
                      twin_wo_recv.at[zz, j - moving], at(z, other, t))

    def rows_copy(dc, dt):
        cc, tt = lax.rem(c + dc, cores), lax.rem(t + dt, cols)
        mine = c * cols + t
        src_at = pl.multiple_of((tt * cores + cc) * half, 128)
        dst_at = pl.multiple_of(mine * o_own, 16)
        return remote(o_ref.at[:, pl.ds(src_at, half)], o_rows.at[pl.ds(dst_at, o_own), :],
                      rows_send.at[dc * cols + dt], rows_recv.at[mine], at(z, cc, tt))

    def rows_arrival(dc, dt):
        cc, tt = lax.rem(c + dc, cores), lax.rem(t + dt, cols)
        theirs = cc * cols + tt
        dst_at = pl.multiple_of(theirs * o_own, 16)
        view = o_rows.at[pl.ds(dst_at, o_own), :]
        return remote(view, view, rows_send.at[dc * cols + dt], rows_recv.at[theirs], at(z, cc, tt))

    peers = [(dc, dt) for dc in range(cores) for dt in range(cols) if dc or dt]

    barrier = pltpu.get_barrier_semaphore()
    for dc, dt in peers:
        pl.semaphore_signal(
            barrier, inc=1, device_id=at(z, lax.rem(c + dc, cores), lax.rem(t + dt, cols)),
            device_id_type=MESH)

    @pl.when(z > 0)
    def _():
        pl.semaphore_signal(barrier, inc=1, device_id=at(z - 1, c, t), device_id_type=MESH)

    @pl.when(z < planes - 1)
    def _():
        pl.semaphore_signal(barrier, inc=1, device_id=at(z + 1, c, t), device_id_type=MESH)

    load_q = pltpu.make_async_copy(q_ref, q_own, local_sems.at[0])
    load_q.start()
    mine = c * cols + t
    load_o = pltpu.make_async_copy(
        o_ref.at[:, pl.ds(pl.multiple_of((t * cores + c) * half, 128), half)],
        o_rows.at[pl.ds(pl.multiple_of(mine * o_own, 16), o_own), :], local_sems.at[1])
    load_o.start()
    load_k = pltpu.make_async_copy(k_ref, kv_own.at[pl.ds(0, k_rows)], local_sems.at[2])
    load_v = pltpu.make_async_copy(v_ref, kv_own.at[pl.ds(k_rows, k_rows)], local_sems.at[2])

    @pl.when(even)
    def _():
        load_k.start()

    @pl.when(jnp.logical_not(even))
    def _():
        load_v.start()

    give_v = remote(v_ref, kv_own.at[pl.ds(0, k_rows)], kv_sems.at[0], kv_sems.at[1], at(z, c, t + 1 - 2 * lax.rem(t, 2)))
    give_k = remote(k_ref, kv_own.at[pl.ds(k_rows, k_rows)], kv_sems.at[0], kv_sems.at[1], at(z, c, t + 1 - 2 * lax.rem(t, 2)))

    early = [
        pltpu.make_async_copy(source, target, early_sems.at[i])
        for i, (source, target) in enumerate((
            (hidden_ref, hidden), (positions_ref, positions), (gain_ref, gain), (post_ref, post),
            (freq_ref, freq), (keys_ref, keys), (values_ref, values)))
    ]

    batch, kv_local, length, head_dim = keys_ref.shape
    q_local = q_all // head_dim
    group = q_local // kv_local
    f32, bf16 = jnp.float32, jnp.bfloat16

    def project():
        for copy in early[:5]:
            copy.wait()
        wide = hidden[...].astype(f32)
        mean_square = jnp.mean(wide * wide, axis=-1, keepdims=True)
        normed = (wide * lax.rsqrt(mean_square + 1e-06) * gain[...].reshape(1, -1)).astype(bf16)

        def columns(i, carry):
            span = pl.ds(pl.multiple_of(i * 256, 256), 256)
            fresh[:, span] = jnp.dot(normed, joined[:, span], preferred_element_type=f32)
            return carry

        lax.fori_loop(0, fresh.shape[1] // 256, columns, 0)
        angle = jnp.concatenate(
            [positions[b].astype(f32) * freq[...] for b in range(batch)], axis=0)
        cosine, sine = jnp.cos(angle), jnp.sin(angle)
        lane = lax.broadcasted_iota(jnp.int32, angle.shape, 1)
        sine = jnp.where(lane < head_dim // 2, -sine, sine)

        def turned(start):
            x = fresh[:, start : start + head_dim]
            swapped = pltpu.roll(x, head_dim // 2, 1)
            return (x * cosine + swapped * sine).astype(bf16).astype(f32)

        for h in range(kv_local):
            key = turned(q_all + h * head_dim)
            at_v = q_all + k_all + h * head_dim
            value = fresh[:, at_v : at_v + head_dim].astype(bf16).astype(f32)
            for g in range(group):
                n = h * group + g
                query = turned(n * head_dim)
                for b in range(batch):
                    q_heads[b, n : n + 1, :] = query[b : b + 1]
                    k_heads[b, n : n + 1, :] = key[b : b + 1]
                    v_heads[b, n : n + 1, :] = value[b : b + 1]

    def attend():
        for copy in early[5:]:
            copy.wait()
        over = (((1,), (1,)), ((), ()))
        slots = lax.broadcasted_iota(jnp.int32, (q_local, length), 1)
        owner = lax.broadcasted_iota(jnp.int32, (q_local, 1), 0) // group
        for b in range(batch):
            query = q_heads[b]
            narrow = query.astype(bf16)
            scores = jnp.zeros((q_local, length), f32)
            for h in range(kv_local):
                one = lax.dot_general(narrow, keys[b, h], over, preferred_element_type=f32)
                scores = jnp.where(owner == h, one, scores)
            raw = jnp.exp(soft_cap * jnp.tanh(scores * score_scale / soft_cap))
            raw = jnp.where(slots < positions[b], raw, 0.0)
            self_score = jnp.sum(query * k_heads[b], axis=-1, keepdims=True) * score_scale
            self_raw = jnp.exp(soft_cap * jnp.tanh(self_score / soft_cap))
            denom = jnp.sum(raw, axis=-1, keepdims=True) + self_raw
            weights = (raw / denom).astype(bf16)
            self_weight = (self_raw / denom).astype(bf16).astype(f32)
            mixed = jnp.zeros((q_local, head_dim), f32)
            for h in range(kv_local):
                one = jnp.dot(weights, values[b, h], preferred_element_type=f32)
                mixed = jnp.where(owner == h, one, mixed)
            mixed = mixed + self_weight * v_heads[b]
            for n in range(q_local):
                attended[b : b + 1, n * head_dim : (n + 1) * head_dim] = mixed[n : n + 1]

    far_end = jnp.where(2 * z < planes, planes - 1, 0)

    def share_copy(zz, dt):
        p = lax.rem(t + dt, cols)
        return remote(partial.at[zz], others.at[zz, t], share_send.at[zz, dt], share_recv.at[zz, t], at(z, c, p))

    def share_arrival(zz, dt):
        p = lax.rem(t + dt, cols)
        view = others.at[zz, p]
        return remote(view, view, share_send.at[zz, dt], share_recv.at[zz, p], at(z, c, p))

    def add_slice(zz):
        for j in range(moving, total):
            twin_wo_copy(zz, j, other).wait_recv()
        narrow = attended[...].astype(bf16)
        span = pl.ds(pl.multiple_of(zz * block, 128), block)
        partial[zz] = jnp.dot(narrow, heads[:, span], preferred_element_type=f32)
        for dt in range(1, cols):
            share_copy(zz, dt).start()

    def sum_slice(zz):
        share = partial[zz]
        for dt in range(1, cols):
            share_arrival(zz, dt).wait_recv()
            share = share + others[zz, lax.rem(t + dt, cols)]
        partial_sum[zz] = share
        return jnp.sum(share * share, axis=-1, keepdims=True)

    def near(step):
        return lax.rem(far_end + 1 + step, planes)

    def finish():
        add_slice(far_end)
        square = jnp.zeros((batch, 1), f32)
        for step in range(planes - 1):
            square = square + sum_slice(near(step))
        square = square + sum_slice(far_end)
        multiplier = lax.rsqrt(square / width + 1e-06)
        result[...] = (partial_sum[t] * multiplier * post[...].reshape(1, -1)).astype(result.dtype)
        for zz in range(planes):
            for dt in range(1, cols):
                share_copy(zz, dt).wait_send()

    def prepare(j):
        @pl.when(j < pieces)
        def _():
            span = pl.ds(pl.multiple_of(j * deep, 128), deep)
            stage[z, j] = jnp.transpose(q_own[:, span])

        @pl.when(j == pieces)
        def _():
            @pl.when(even)
            def _():
                load_k.wait()
                give_k.wait_recv()

            @pl.when(jnp.logical_not(even))
            def _():
                load_v.wait()
                give_v.wait_recv()

        @pl.when(jnp.logical_and(j >= pieces, j < moving))
        def _():
            span = pl.ds(pl.multiple_of((j - pieces) * deep, 128), deep)
            stage[z, j] = jnp.transpose(kv_own[:, span])

        @pl.when(j == moving)
        def _():
            load_o.wait()
            for dc, dt in peers:
                rows_arrival(dc, dt).wait_recv()

        @pl.when(jnp.logical_and(j >= moving, j < total))
        def _():
            col = pl.multiple_of((j - moving) * wo_rows, 128)
            row = pl.multiple_of(c * half + (j - moving) * wo_rows, 128)
            heads[pl.ds(row, wo_rows), pl.ds(pl.multiple_of(z * block, 128), block)] = jnp.transpose(
                o_rows[:, pl.ds(col, wo_rows)])

    def send_line(zz, j, way):
        target = at(z - 1, c, t) if way == 0 else at(z + 1, c, t)
        room = z > 0 if way == 0 else z < planes - 1

        @pl.when(jnp.logical_and(room, j < moving))
        def _():
            line_copy(zz, j, way, target).start()

        @pl.when(jnp.logical_and(room, j >= moving))
        def _():
            line_wo_copy(zz, j, way, target).start()

    def wait_line(zz, j):
        @pl.when(j < moving)
        def _():
            line_copy(zz, j, 0, at(z, other, t)).wait_recv()

        @pl.when(j >= moving)
        def _():
            line_wo_copy(zz, j, 0, at(z, other, t)).wait_recv()

    def deliver(zz, j):
        @pl.when(jnp.logical_and(j < moving, t != zz))
        def _():
            plane_copy(zz, j).start()

        @pl.when(jnp.logical_and(j < moving, t == zz))
        def _():
            row = pl.multiple_of(lax.rem(j, pieces) * deep, 128)
            joined[pl.ds(row, deep), pl.ds(column(t, j, c), 128)] = stage[zz, j]
            twin_copy(stage.at[zz, j], t, j, c).start()

        @pl.when(j >= moving)
        def _():
            twin_wo_copy(zz, j, c).start()

    for copy in early[:5]:
        copy.start()
    load_q.wait()
    prepare(jnp.int32(0))
    n_line = (z > 0).astype(jnp.int32) + (z < planes - 1).astype(jnp.int32)
    pl.semaphore_wait(barrier, len(peers) + n_line)

    def rounds(r, carry):
        @pl.when(r < total)
        def _():
            send_line(z, r, 0)
            send_line(z, r, 1)
            deliver(z, r)

        @pl.when(r == 0)
        def _():
            @pl.when(even)
            def _():
                give_v.start()

            @pl.when(jnp.logical_not(even))
            def _():
                give_k.start()

        @pl.when(r == 3)
        def _():
            for dc, dt in peers:
                rows_copy(dc, dt).start()
            for copy in early[5:]:
                copy.start()

        @pl.when(r + 1 < total)
        def _():
            prepare(r + 1)

        for k in range(1, planes):
            for way in (0, 1):
                zz = z + k if way == 0 else z - k
                j = r - k
                inside = zz < planes if way == 0 else zz >= 0

                @pl.when(jnp.logical_and(inside, jnp.logical_and(j >= 0, j < total)))
                def _():
                    wait_line(zz, j)
                    send_line(zz, j, way)
                    deliver(zz, j)

        far = jnp.where(z > t, z - t, t - z)
        j = r - far - 1

        @pl.when(jnp.logical_and(j >= 0, j < moving))
        def _():
            for dt in range(1, cols):
                tt = lax.rem(t + dt, cols)
                plane_arrival(tt, j).wait_recv()
                twin_copy(slot(tt, j, c), tt, j, c).start()

        @pl.when(r == moving + 1 + far)
        def _():
            lax.fori_loop(0, moving, twin_in, 0)
            project()

        @pl.when(r == moving + 2 + far)
        def _():
            attend()
        return carry

    def twin_in(j, carry):
        for tt in range(cols):
            twin_copy(slot(tt, j, other), tt, j, other).wait_recv()
        return carry

    lax.fori_loop(0, total + planes - 2, rounds, 0)
    for step in range(planes - 1):
        add_slice(near(step))
    rounds(jnp.int32(total + planes - 2), 0)
    finish()

    def sent(j, carry):
        for zz in range(planes):
            for way in (0, 1):
                room = z > 0 if way == 0 else z < planes - 1
                passes = z <= zz if way == 0 else z >= zz

                @pl.when(jnp.logical_and(room, passes))
                def _():
                    @pl.when(j < moving)
                    def _():
                        line_copy(zz, j, way, at(z, other, t)).wait_send()

                    @pl.when(j >= moving)
                    def _():
                        line_wo_copy(zz, j, way, at(z, other, t)).wait_send()

            @pl.when(jnp.logical_and(j < moving, t != zz))
            def _():
                plane_copy(zz, j).wait_send()

            @pl.when(j < moving)
            def _():
                twin_copy(slot(zz, j, c), zz, j, c).wait_send()

            @pl.when(j >= moving)
            def _():
                twin_wo_copy(zz, j, c).wait_send()
        return carry

    lax.fori_loop(0, total, sent, 0)
    for dc, dt in peers:
        rows_copy(dc, dt).wait_send()

    @pl.when(even)
    def _():
        give_v.wait_send()

    @pl.when(jnp.logical_not(even))
    def _():
        give_k.wait_send()


def line_body(hidden, positions, key_cache, value_cache, norm_gain, q_proj, k_proj, v_proj, o_proj, post_gain):
    cols = lax.axis_size("tp")
    cores = 2
    planes = lax.axis_size("rep") // cores
    pieces = 4
    width = q_proj.shape[1]
    deep = width // pieces
    q_rows, k_rows, o_own = q_proj.shape[0], k_proj.shape[0], o_proj.shape[0]
    features = o_proj.shape[1] // cols
    columns = cores * cols * (q_rows + 2 * k_rows)
    model = o_own * cores * cols * planes
    bf = jnp.bfloat16
    dma = pltpu.SemaphoreType.DMA
    hbm = pl.BlockSpec(memory_space=pltpu.HBM)
    f32 = jnp.float32
    batch, kv_local, length, head_dim = key_cache.shape
    q_local = cores * cols * q_rows // head_dim
    half = head_dim // 2
    freq = 10000.0 ** (-2.0 * np.arange(half) / head_dim)
    freq = jnp.asarray(np.concatenate([freq, freq])[None], f32)
    share = post_gain.shape[0]
    moving, total = 2 * pieces, 3 * pieces
    out = pl.pallas_call(
        functools.partial(move_kernel, (planes, cores, cols, pieces)),
        in_specs=[hbm] * 11,
        out_shape=[
            pltpu.VMEM((width, columns), bf),
            pltpu.VMEM((features, model), bf),
            pltpu.VMEM((hidden.shape[0], post_gain.shape[0]), bf),
        ],
        out_specs=[pl.BlockSpec(memory_space=pltpu.VMEM)] * 3,
        scratch_shapes=[
            pltpu.VMEM((planes, moving, deep, 128), bf),
            pltpu.VMEM((q_rows, width), bf),
            pltpu.VMEM((2 * k_rows, width), bf),
            pltpu.VMEM((cores * cols * o_own, features // cores), bf),
            pltpu.VMEM(hidden.shape, bf), pltpu.SMEM(positions.shape, jnp.int32),
            pltpu.VMEM(key_cache.shape, bf), pltpu.VMEM(value_cache.shape, bf),
            pltpu.VMEM((width,), f32), pltpu.VMEM((share,), f32), pltpu.VMEM((1, head_dim), f32),
            pltpu.VMEM((batch, columns), f32), pltpu.VMEM((batch, q_local, head_dim), f32),
            pltpu.VMEM((batch, q_local, head_dim), f32), pltpu.VMEM((batch, q_local, head_dim), f32),
            pltpu.VMEM((batch, features), f32), pltpu.VMEM((planes, batch, share), f32),
            pltpu.VMEM((planes, batch, share), f32), pltpu.VMEM((planes, cols, batch, share), f32),
            dma((7,)), dma((planes, cols)), dma((planes, cols)),
            dma((3,)), dma((2,)), dma((cores * cols,)), dma((cores * cols,)),
            dma((2, planes, total)), dma((planes, total)), dma((planes, moving)), dma((cols, moving)),
            dma((cols, moving)), dma((cols, moving)), dma((planes, pieces)), dma((planes, pieces)),
        ],
        compiler_params=pltpu.CompilerParams(
            collective_id=0, has_side_effects=True, vmem_limit_bytes=34 * 2**20),
        name="move",
    )(q_proj, k_proj, v_proj, o_proj, hidden, positions, key_cache, value_cache,
      norm_gain, post_gain, freq)
    joined, heads, result = out

    def spill_kernel(a, b, r, a_out, b_out, r_out, sems):
        copies = [pltpu.make_async_copy(r, r_out, sems.at[0])]
        for source, target in ((a, a_out), (b, b_out)):
            rows = source.shape[0] // 4
            for i in range(4):
                span = pl.ds(i * rows, rows)
                copies.append(pltpu.make_async_copy(source.at[span], target.at[span], sems.at[len(copies)]))
        for copy in copies:
            copy.start()
        for copy in copies:
            copy.wait()

    vmem = pl.BlockSpec(memory_space=pltpu.VMEM)
    return tuple(pl.pallas_call(
        spill_kernel,
        in_specs=[vmem] * 3,
        out_specs=[hbm] * 3,
        out_shape=[jax.ShapeDtypeStruct(x.shape, x.dtype) for x in (joined, heads, result)],
        scratch_shapes=[dma((9,))],
        compiler_params=pltpu.CompilerParams(vmem_limit_bytes=2**20),
        name="spill",
    )(joined, heads, result))


def body(*args):
    cols, reps = lax.axis_size("tp"), lax.axis_size("rep")
    key_cache, q_proj, k_proj, o_proj = args[2], args[5], args[6], args[8]
    lanes = 128
    fits = (
        reps == 2 * cols
        and cols % 2 == 0
        and key_cache.shape[3] == lanes
        and q_proj.shape[0] == lanes
        and 2 * k_proj.shape[0] == lanes
        and o_proj.shape[0] % 16 == 0
        and q_proj.shape[1] % (4 * lanes) == 0
        and o_proj.shape[1] % (8 * lanes * cols) == 0
        and (2 * cols * o_proj.shape[0]) % lanes == 0
    )
    return (line_body if fits else general_body)(*args)


def solution(mesh):
    in_specs = (
        P("rep", None), P("rep"), P("rep", "tp", None, None), P("rep", "tp", None, None), P(),
        P(("rep", "tp"), None), P(("rep", "tp"), None), P(("rep", "tp"), None), P(("rep", "tp"), None), P("tp"),
    )
    out_specs = (P(None, "tp"), P("tp", None), P("rep", "tp"))
    return jax.shard_map(body, mesh=mesh, in_specs=in_specs, out_specs=out_specs, check_vma=False)
```

```python
import functools

import jax
import jax.numpy as jnp
import numpy as np
from jax import lax
from jax.experimental import pallas as pl
from jax.experimental.pallas import tpu as pltpu
from jax.sharding import PartitionSpec as P

MESH = pl.DeviceIdType.MESH
score_scale = 144.0 ** (-0.5)
soft_cap = 50.0


def rms_scale(values, gain):
    mean_square = jnp.mean(values * values, axis=-1, keepdims=True)
    return values * lax.rsqrt(mean_square + 1e-06) * gain


def rotate(values, positions):
    half = values.shape[-1] // 2
    freq = 10000.0 ** (-2.0 * jnp.arange(half, dtype=jnp.float32) / values.shape[-1])
    angle = positions.astype(jnp.float32)[:, None] * freq[None, :]
    cosine = jnp.cos(angle)[:, None, :]
    sine = jnp.sin(angle)[:, None, :]
    first = values[..., :half]
    second = values[..., half:]
    return jnp.concatenate(
        [first * cosine - second * sine, second * cosine + first * sine], axis=-1
    )


def join_kernel(per_tp, q_rows, k_rows, *refs):
    slot = lax.rem(lax.axis_index("rep"), per_tp)
    parts, out_ref = refs[:-1], refs[-1]
    tp_count = parts[0].shape[0]
    q_all = tp_count * per_tp * q_rows
    k_all = tp_count * per_tp * k_rows
    for step in range(per_tp):
        who = lax.rem(slot + step, per_tp)
        q_ref, kv_ref = parts[2 * step], parts[2 * step + 1]
        for start, ref, low, rows in (
            (0, q_ref, 0, q_rows),
            (q_all, kv_ref, 0, k_rows),
            (q_all + k_all, kv_ref, k_rows, k_rows),
        ):
            block = ref[:, low : low + rows, :].reshape(tp_count * rows, -1)
            at = pl.multiple_of(start + who * (tp_count * rows), 128)
            out_ref[:, pl.ds(at, tp_count * rows)] = jnp.transpose(block)


def join(per_tp, pairs):
    tp_count, q_rows, width = pairs[0][0].shape
    k_rows = pairs[0][1].shape[1] // 2
    columns = tp_count * per_tp * (q_rows + 2 * k_rows)
    stripe = 256
    operands, specs = [], []
    for pair in pairs:
        for matrix in pair:
            operands.append(matrix)
            specs.append(
                pl.BlockSpec((tp_count, matrix.shape[1], stripe), lambda j: (0, 0, j))
            )
    size = width * columns * 2
    return pl.pallas_call(
        functools.partial(join_kernel, per_tp, q_rows, k_rows),
        grid=(width // stripe,),
        in_specs=specs,
        out_specs=pl.BlockSpec((stripe, columns), lambda j: (j, 0)),
        out_shape=jax.ShapeDtypeStruct((width, columns), jnp.bfloat16),
        cost_estimate=pl.CostEstimate(flops=0, bytes_accessed=2 * size, transcendentals=0),
        name="join",
    )(*operands)


def turn_kernel(rows_ref, out_ref):
    out_ref[...] = jnp.transpose(rows_ref[...])


def turn(rows):
    height, width = rows.shape
    stripe = 384 if height % 384 == 0 else 128
    return pl.pallas_call(
        turn_kernel,
        grid=(height // stripe,),
        in_specs=[pl.BlockSpec((stripe, width), lambda j: (j, 0))],
        out_specs=pl.BlockSpec((width, stripe), lambda j: (0, j)),
        out_shape=jax.ShapeDtypeStruct((width, height), rows.dtype),
        cost_estimate=pl.CostEstimate(
            flops=0, bytes_accessed=4 * height * width, transcendentals=0
        ),
        name="turn",
    )(rows)


def general_body(
    hidden, positions, key_cache, value_cache, norm_gain, q_proj, k_proj, v_proj, o_proj, post_gain
):
    tp_count = lax.axis_size("tp")
    replica_count = lax.axis_size("rep")
    per_tp = replica_count // tp_count
    model_width = hidden.shape[1]
    q_rows, k_rows = q_proj.shape[0], k_proj.shape[0]

    groups = [[i + per_tp * p for p in range(tp_count)] for i in range(per_tp)]
    shifts = [
        [
            (per_tp * p + (i + d) % per_tp, per_tp * p + i)
            for p in range(tp_count)
            for i in range(per_tp)
        ]
        for d in range(1, per_tp)
    ]

    def collect(rows):
        planes = lax.all_gather(rows[None], "rep", axis=0, tiled=True, axis_index_groups=groups)
        return lax.all_to_all(planes, "tp", split_axis=0, concat_axis=0, tiled=True)

    kv_rows = collect(jnp.concatenate([k_proj, v_proj], axis=0))
    split_cols = o_proj.reshape(o_proj.shape[0], tp_count, -1)
    rows_of_group = lax.all_to_all(split_cols, "tp", split_axis=1, concat_axis=0, tiled=True)

    batch, kv_local, length, head_dim = key_cache.shape

    def scatter_rows(values):
        wide = values.reshape(replica_count, batch, -1)
        by_rep = lax.all_to_all(wide, "rep", split_axis=0, concat_axis=0, tiled=True)
        return by_rep

    def to_block(by_rep):
        arrived = lax.all_to_all(by_rep, "tp", split_axis=0, concat_axis=0, tiled=True)
        arrived = arrived.reshape(tp_count, per_tp, batch, -1)
        return jnp.transpose(arrived, (2, 1, 0, 3))

    normed = rms_scale(hidden.astype(jnp.float32), norm_gain).astype(jnp.bfloat16)
    normed_all = lax.all_gather(normed, "rep", axis=0, tiled=True)
    contract = (((1,), (1,)), ((), ()))
    local = jnp.concatenate(
        [
            lax.dot_general(normed_all, matrix, contract, preferred_element_type=jnp.float32)
            for matrix in (q_proj, k_proj, v_proj)
        ],
        axis=1,
    )
    block = to_block(scatter_rows(local))
    q_local = tp_count * per_tp * q_rows // head_dim
    group = q_local // kv_local
    query = block[..., :q_rows].reshape(batch, q_local, head_dim)
    keys_new = block[..., q_rows : q_rows + k_rows].reshape(batch, kv_local, head_dim)
    values_new = block[..., q_rows + k_rows :].reshape(batch, kv_local, head_dim)
    query_rot = rotate(query, positions).astype(jnp.bfloat16)
    rotated_keys = rotate(keys_new, positions).astype(jnp.bfloat16)
    values_rot = values_new.astype(jnp.bfloat16)
    grouped_heads = query_rot.reshape(batch, kv_local, group, head_dim)
    scores = (
        jnp.einsum("bkgd,bkld->bkgl", grouped_heads, key_cache, preferred_element_type=jnp.float32)
        * score_scale
    )
    capped = soft_cap * jnp.tanh(scores / soft_cap)
    valid = jnp.arange(length, dtype=jnp.int32)[None, :] < positions[:, None]
    weight_raw = jnp.where(valid[:, None, None, :], jnp.exp(capped), 0.0)
    self_score = (
        jnp.einsum("juzy,juy->juz", grouped_heads, rotated_keys, preferred_element_type=jnp.float32)
        * score_scale
    )
    self_raw = jnp.exp(soft_cap * jnp.tanh(self_score / soft_cap))
    denom = jnp.sum(weight_raw, axis=-1) + self_raw
    weights = (weight_raw / denom[..., None]).astype(jnp.bfloat16)
    self_weight = (self_raw / denom).astype(jnp.bfloat16)
    attention = jnp.einsum(
        "bkgl,bkld->bkgd", weights, value_cache, preferred_element_type=jnp.float32
    )
    attention = (
        attention
        + self_weight.astype(jnp.float32)[..., None] * values_rot.astype(jnp.float32)[:, :, None, :]
    )
    attention = attention.reshape(batch, q_local * head_dim).astype(jnp.bfloat16)
    q_later, attention = lax.optimization_barrier((q_proj, attention))
    q_own = collect(q_later)
    pairs = [(q_own, kv_rows)]
    for shift in shifts:
        pairs.append((lax.ppermute(q_own, "rep", shift), lax.ppermute(kv_rows, "rep", shift)))
    joined_block = join(per_tp, pairs)
    own_all = lax.all_gather(attention, "tp", axis=1, tiled=True)
    attention_all = lax.all_gather(own_all, "rep", axis=0, tiled=True)
    projected = lax.dot_general(
        attention_all, o_proj, contract, preferred_element_type=jnp.float32
    )
    by_rep = scatter_rows(projected)
    share = to_block(by_rep).reshape(batch, -1)
    square = jnp.sum(share * share, axis=1)
    square_all = lax.all_gather(square[None], "tp", axis=0, tiled=True)
    multiplier = lax.rsqrt(jnp.sum(square_all, axis=0) / model_width + 1e-06)
    result = share * multiplier[:, None] * post_gain
    rows_of_group, result = lax.optimization_barrier((rows_of_group, result))
    complete_rows = lax.all_gather(rows_of_group, "rep", axis=0, tiled=True)
    out_block = turn(complete_rows.reshape(model_width, -1))
    return (joined_block, out_block, result.astype(jnp.bfloat16))


def move_kernel(
    sizes,
    q_ref, k_ref, v_ref, o_ref,
    hidden_ref, positions_ref, keys_ref, values_ref, gain_ref, post_ref, freq_ref,
    joined, heads, result,
    stage, q_own, kv_own, o_rows,
    hidden, positions, keys, values, gain, post, freq,
    fresh, q_heads, k_heads, v_heads, attended, partial, partial_sum, others,
    early_sems, share_send, share_recv,
    local_sems, kv_sems, rows_send, rows_recv,
    line_send, line_recv, plane_send, plane_recv,
    twin_send, twin_recv, twin_wo_send, twin_wo_recv,
):
    planes, cores, cols, pieces = sizes
    rep, t = lax.axis_index("rep"), lax.axis_index("tp")
    z, c = rep // cores, lax.rem(rep, cores)
    other = 1 - c
    width = q_ref.shape[1]
    deep = width // pieces
    q_rows, k_rows = q_ref.shape[0], k_ref.shape[0]
    o_own = o_ref.shape[0]
    block = cols * cores * o_own
    half = heads.shape[0] // cores
    wo_rows = half // pieces
    moving = 2 * pieces
    total = 3 * pieces
    q_all = cores * cols * q_rows
    k_all = cores * cols * k_rows
    even = lax.rem(t, 2) == 0

    def at(zz, cc, tt):
        return (zz * cores + cc, tt)

    def column(tt, j, cc):
        parity = lax.rem(tt, 2)
        q_at = (cc * cols + tt) * q_rows
        kv_at = q_all + parity * k_all + (cc * cols + tt - parity) * k_rows
        is_q = (j < pieces).astype(jnp.int32)
        return pl.multiple_of(is_q * q_at + (1 - is_q) * kv_at, 128)

    def slot(tt, j, cc):
        row = pl.multiple_of(lax.rem(j, pieces) * deep, 128)
        return joined.at[pl.ds(row, deep), pl.ds(column(tt, j, cc), 128)]

    def wo_slot(zz, j, cc):
        row = pl.multiple_of(cc * half + (j - moving) * wo_rows, 128)
        col = pl.multiple_of(zz * block, 128)
        return heads.at[pl.ds(row, wo_rows), pl.ds(col, block)]

    def remote(src, dst, send, recv, device):
        return pltpu.make_async_remote_copy(
            src_ref=src, dst_ref=dst, send_sem=send, recv_sem=recv,
            device_id=device, device_id_type=MESH,
        )

    def line_copy(zz, j, way, device):
        return remote(stage.at[zz, j], stage.at[zz, j], line_send.at[way],
                      line_recv.at[zz, j], device)

    def line_wo_copy(zz, j, way, device):
        return remote(wo_slot(zz, j, c), wo_slot(zz, j, c), line_send.at[way],
                      line_recv.at[zz, j], device)

    def plane_copy(zz, j):
        return remote(stage.at[zz, j], slot(t, j, c), plane_send.at[0],
                      plane_recv.at[j], at(z, c, zz))

    def wait_bytes(view, sem):
        pltpu.make_async_copy(view, view, sem).wait()

    def twin_copy(src, tt, j, cc):
        return remote(src, slot(tt, j, cc), twin_send.at[0], twin_recv.at[0], at(z, other, t))

    def twin_wo_copy(zz, j, cc):
        return remote(wo_slot(zz, j, cc), wo_slot(zz, j, cc), twin_wo_send.at[0],
                      twin_wo_recv.at[zz], at(z, other, t))

    def rows_copy(dc, dt):
        cc, tt = lax.rem(c + dc, cores), lax.rem(t + dt, cols)
        mine = c * cols + t
        src_at = pl.multiple_of((tt * cores + cc) * half, 128)
        dst_at = pl.multiple_of(mine * o_own, 16)
        return remote(o_ref.at[:, pl.ds(src_at, half)], o_rows.at[pl.ds(dst_at, o_own), :],
                      rows_send.at[0], rows_recv.at[0], at(z, cc, tt))

    peers = [(dc, dt) for dc in range(cores) for dt in range(cols) if dc or dt]

    barrier = pltpu.get_barrier_semaphore()
    for dc, dt in peers:
        pl.semaphore_signal(
            barrier, inc=1, device_id=at(z, lax.rem(c + dc, cores), lax.rem(t + dt, cols)),
            device_id_type=MESH)

    @pl.when(z > 0)
    def _():
        pl.semaphore_signal(barrier, inc=1, device_id=at(z - 1, c, t), device_id_type=MESH)

    @pl.when(z < planes - 1)
    def _():
        pl.semaphore_signal(barrier, inc=1, device_id=at(z + 1, c, t), device_id_type=MESH)

    load_q = pltpu.make_async_copy(q_ref, q_own, local_sems.at[0])
    load_q.start()
    mine = c * cols + t
    load_o = pltpu.make_async_copy(
        o_ref.at[:, pl.ds(pl.multiple_of((t * cores + c) * half, 128), half)],
        o_rows.at[pl.ds(pl.multiple_of(mine * o_own, 16), o_own), :], local_sems.at[1])
    load_o.start()
    load_k = pltpu.make_async_copy(k_ref, kv_own.at[pl.ds(0, k_rows)], local_sems.at[2])
    load_v = pltpu.make_async_copy(v_ref, kv_own.at[pl.ds(k_rows, k_rows)], local_sems.at[2])

    @pl.when(even)
    def _():
        load_k.start()

    @pl.when(jnp.logical_not(even))
    def _():
        load_v.start()

    give_v = remote(v_ref, kv_own.at[pl.ds(0, k_rows)], kv_sems.at[0], kv_sems.at[1], at(z, c, t + 1 - 2 * lax.rem(t, 2)))
    give_k = remote(k_ref, kv_own.at[pl.ds(k_rows, k_rows)], kv_sems.at[0], kv_sems.at[1], at(z, c, t + 1 - 2 * lax.rem(t, 2)))

    early = [
        pltpu.make_async_copy(source, target, early_sems.at[i])
        for i, (source, target) in enumerate((
            (hidden_ref, hidden), (positions_ref, positions), (gain_ref, gain), (post_ref, post),
            (freq_ref, freq), (keys_ref, keys), (values_ref, values)))
    ]

    batch, kv_local, length, head_dim = keys_ref.shape
    q_local = q_all // head_dim
    group = q_local // kv_local
    f32, bf16 = jnp.float32, jnp.bfloat16

    def project():
        for copy in early[:5]:
            copy.wait()
        wide = hidden[...].astype(f32)
        mean_square = jnp.mean(wide * wide, axis=-1, keepdims=True)
        normed = (wide * lax.rsqrt(mean_square + 1e-06) * gain[...].reshape(1, -1)).astype(bf16)

        def columns(i, carry):
            span = pl.ds(pl.multiple_of(i * 256, 256), 256)
            fresh[:, span] = jnp.dot(normed, joined[:, span], preferred_element_type=f32)
            return carry

        lax.fori_loop(0, fresh.shape[1] // 256, columns, 0)
        angle = jnp.concatenate(
            [positions[b].astype(f32) * freq[...] for b in range(batch)], axis=0)
        cosine, sine = jnp.cos(angle), jnp.sin(angle)
        lane = lax.broadcasted_iota(jnp.int32, angle.shape, 1)
        sine = jnp.where(lane < head_dim // 2, -sine, sine)

        def turned(start):
            x = fresh[:, start : start + head_dim]
            swapped = pltpu.roll(x, head_dim // 2, 1)
            return (x * cosine + swapped * sine).astype(bf16).astype(f32)

        for h in range(kv_local):
            key = turned(q_all + h * head_dim)
            at_v = q_all + k_all + h * head_dim
            value = fresh[:, at_v : at_v + head_dim].astype(bf16).astype(f32)
            for g in range(group):
                n = h * group + g
                query = turned(n * head_dim)
                for b in range(batch):
                    q_heads[b, n : n + 1, :] = query[b : b + 1]
                    k_heads[b, n : n + 1, :] = key[b : b + 1]
                    v_heads[b, n : n + 1, :] = value[b : b + 1]

    def attend():
        for copy in early[5:]:
            copy.wait()
        over = (((1,), (1,)), ((), ()))
        slots = lax.broadcasted_iota(jnp.int32, (q_local, length), 1)
        owner = lax.broadcasted_iota(jnp.int32, (q_local, 1), 0) // group
        for b in range(batch):
            query = q_heads[b]
            narrow = query.astype(bf16)
            scores = jnp.zeros((q_local, length), f32)
            for h in range(kv_local):
                one = lax.dot_general(narrow, keys[b, h], over, preferred_element_type=f32)
                scores = jnp.where(owner == h, one, scores)
            raw = jnp.exp(soft_cap * jnp.tanh(scores * score_scale / soft_cap))
            raw = jnp.where(slots < positions[b], raw, 0.0)
            self_score = jnp.sum(query * k_heads[b], axis=-1, keepdims=True) * score_scale
            self_raw = jnp.exp(soft_cap * jnp.tanh(self_score / soft_cap))
            denom = jnp.sum(raw, axis=-1, keepdims=True) + self_raw
            weights = (raw / denom).astype(bf16)
            self_weight = (self_raw / denom).astype(bf16).astype(f32)
            mixed = jnp.zeros((q_local, head_dim), f32)
            for h in range(kv_local):
                one = jnp.dot(weights, values[b, h], preferred_element_type=f32)
                mixed = jnp.where(owner == h, one, mixed)
            mixed = mixed + self_weight * v_heads[b]
            for n in range(q_local):
                attended[b : b + 1, n * head_dim : (n + 1) * head_dim] = mixed[n : n + 1]

    far_end = jnp.where(2 * z < planes, planes - 1, 0)

    def share_copy(zz, dt):
        p = lax.rem(t + dt, cols)
        return remote(partial.at[zz], others.at[zz, t], share_send.at[0], share_recv.at[zz], at(z, c, p))

    def add_slice(zz):
        row = pl.multiple_of(other * half, 128)
        col = pl.multiple_of(zz * block, 128)
        wait_bytes(heads.at[pl.ds(row, half), pl.ds(col, block)], twin_wo_recv.at[zz])
        narrow = attended[...].astype(bf16)
        span = pl.ds(pl.multiple_of(zz * block, 128), block)
        partial[zz] = jnp.dot(narrow, heads[:, span], preferred_element_type=f32)
        for dt in range(1, cols):
            share_copy(zz, dt).start()

    def sum_slice(zz):
        share = partial[zz]
        wait_bytes(others.at[0, pl.ds(0, cols - 1)], share_recv.at[zz])
        for dt in range(1, cols):
            share = share + others[zz, lax.rem(t + dt, cols)]
        partial_sum[zz] = share
        return jnp.sum(share * share, axis=-1, keepdims=True)

    def near(step):
        return lax.rem(far_end + 1 + step, planes)

    def finish():
        add_slice(far_end)
        square = jnp.zeros((batch, 1), f32)
        for step in range(planes - 1):
            square = square + sum_slice(near(step))
        square = square + sum_slice(far_end)
        multiplier = lax.rsqrt(square / width + 1e-06)
        result[...] = (partial_sum[t] * multiplier * post[...].reshape(1, -1)).astype(result.dtype)
        wait_bytes(others.at[pl.ds(0, cols - 1)], share_send.at[0])

    def prepare(j):
        @pl.when(j < pieces)
        def _():
            span = pl.ds(pl.multiple_of(j * deep, 128), deep)
            stage[z, j] = jnp.transpose(q_own[:, span])

        @pl.when(j == pieces)
        def _():
            @pl.when(even)
            def _():
                load_k.wait()
                give_k.wait_recv()

            @pl.when(jnp.logical_not(even))
            def _():
                load_v.wait()
                give_v.wait_recv()

        @pl.when(jnp.logical_and(j >= pieces, j < moving))
        def _():
            span = pl.ds(pl.multiple_of((j - pieces) * deep, 128), deep)
            stage[z, j] = jnp.transpose(kv_own[:, span])

        @pl.when(j == moving)
        def _():
            load_o.wait()
            wait_bytes(o_rows.at[pl.ds(0, len(peers) * o_own)], rows_recv.at[0])

        @pl.when(jnp.logical_and(j >= moving, j < total))
        def _():
            col = pl.multiple_of((j - moving) * wo_rows, 128)
            row = pl.multiple_of(c * half + (j - moving) * wo_rows, 128)
            heads[pl.ds(row, wo_rows), pl.ds(pl.multiple_of(z * block, 128), block)] = jnp.transpose(
                o_rows[:, pl.ds(col, wo_rows)])

    def send_line(zz, j, way):
        target = at(z - 1, c, t) if way == 0 else at(z + 1, c, t)
        room = z > 0 if way == 0 else z < planes - 1

        @pl.when(jnp.logical_and(room, j < moving))
        def _():
            line_copy(zz, j, way, target).start()

        @pl.when(jnp.logical_and(room, j >= moving))
        def _():
            line_wo_copy(zz, j, way, target).start()

    def wait_line(zz, j):
        @pl.when(j < moving)
        def _():
            line_copy(zz, j, 0, at(z, other, t)).wait_recv()

        @pl.when(j >= moving)
        def _():
            line_wo_copy(zz, j, 0, at(z, other, t)).wait_recv()

    def deliver(zz, j):
        @pl.when(jnp.logical_and(j < moving, t != zz))
        def _():
            plane_copy(zz, j).start()

        @pl.when(jnp.logical_and(j < moving, t == zz))
        def _():
            row = pl.multiple_of(lax.rem(j, pieces) * deep, 128)
            joined[pl.ds(row, deep), pl.ds(column(t, j, c), 128)] = stage[zz, j]
            twin_copy(stage.at[zz, j], t, j, c).start()

        @pl.when(j >= moving)
        def _():
            twin_wo_copy(zz, j, c).start()

    for copy in early[:5]:
        copy.start()
    load_q.wait()
    prepare(jnp.int32(0))
    n_line = (z > 0).astype(jnp.int32) + (z < planes - 1).astype(jnp.int32)
    pl.semaphore_wait(barrier, len(peers) + n_line)

    def rounds(r, carry):
        @pl.when(r < total)
        def _():
            send_line(z, r, 0)
            send_line(z, r, 1)
            deliver(z, r)

        @pl.when(r == 0)
        def _():
            @pl.when(even)
            def _():
                give_v.start()

            @pl.when(jnp.logical_not(even))
            def _():
                give_k.start()

        @pl.when(r == 3)
        def _():
            for dc, dt in peers:
                rows_copy(dc, dt).start()
            for copy in early[5:]:
                copy.start()

        @pl.when(r + 1 < total)
        def _():
            prepare(r + 1)

        for k in range(1, planes):
            for way in (0, 1):
                zz = z + k if way == 0 else z - k
                j = r - k
                inside = zz < planes if way == 0 else zz >= 0

                @pl.when(jnp.logical_and(inside, jnp.logical_and(j >= 0, j < total)))
                def _():
                    wait_line(zz, j)
                    send_line(zz, j, way)
                    deliver(zz, j)

        far = jnp.where(z > t, z - t, t - z)
        j = r - far - 1

        @pl.when(jnp.logical_and(j >= 0, j < moving))
        def _():
            wait_bytes(stage.at[0, pl.ds(0, cols - 1)], plane_recv.at[j])
            for dt in range(1, cols):
                tt = lax.rem(t + dt, cols)
                twin_copy(slot(tt, j, c), tt, j, c).start()

        @pl.when(r == moving + 1 + far)
        def _():
            wait_bytes(joined.at[pl.ds(0, width // cores)], twin_recv.at[0])
            project()

        @pl.when(r == moving + 2 + far)
        def _():
            attend()
        return carry

    lax.fori_loop(0, total + planes - 2, rounds, 0)
    for step in range(planes - 1):
        add_slice(near(step))
    rounds(jnp.int32(total + planes - 2), 0)
    finish()

    unit = deep * 128 // joined.shape[1]
    for way, count in ((0, planes - z), (1, z + 1)):
        for m in range(1, planes):

            @pl.when(count == m)
            def _():
                wait_bytes(joined.at[pl.ds(0, m * total * unit)], line_send.at[way])
    wait_bytes(joined.at[pl.ds(0, (planes - 1) * moving * unit)], plane_send.at[0])
    wait_bytes(joined.at[pl.ds(0, width // cores)], twin_send.at[0])
    wait_bytes(heads.at[pl.ds(0, half)], twin_wo_send.at[0])
    wait_bytes(o_rows.at[pl.ds(0, len(peers) * o_own)], rows_send.at[0])

    @pl.when(even)
    def _():
        give_v.wait_send()

    @pl.when(jnp.logical_not(even))
    def _():
        give_k.wait_send()


def line_body(hidden, positions, key_cache, value_cache, norm_gain, q_proj, k_proj, v_proj, o_proj, post_gain):
    cols = lax.axis_size("tp")
    cores = 2
    planes = lax.axis_size("rep") // cores
    pieces = 4
    width = q_proj.shape[1]
    deep = width // pieces
    q_rows, k_rows, o_own = q_proj.shape[0], k_proj.shape[0], o_proj.shape[0]
    features = o_proj.shape[1] // cols
    columns = cores * cols * (q_rows + 2 * k_rows)
    model = o_own * cores * cols * planes
    bf = jnp.bfloat16
    dma = pltpu.SemaphoreType.DMA
    hbm = pl.BlockSpec(memory_space=pltpu.HBM)
    f32 = jnp.float32
    batch, kv_local, length, head_dim = key_cache.shape
    q_local = cores * cols * q_rows // head_dim
    half = head_dim // 2
    freq = 10000.0 ** (-2.0 * np.arange(half) / head_dim)
    freq = jnp.asarray(np.concatenate([freq, freq])[None], f32)
    share = post_gain.shape[0]
    moving, total = 2 * pieces, 3 * pieces
    out = pl.pallas_call(
        functools.partial(move_kernel, (planes, cores, cols, pieces)),
        in_specs=[hbm] * 11,
        out_shape=[
            pltpu.VMEM((width, columns), bf),
            pltpu.VMEM((features, model), bf),
            pltpu.VMEM((hidden.shape[0], post_gain.shape[0]), bf),
        ],
        out_specs=[pl.BlockSpec(memory_space=pltpu.VMEM)] * 3,
        scratch_shapes=[
            pltpu.VMEM((planes, moving, deep, 128), bf),
            pltpu.VMEM((q_rows, width), bf),
            pltpu.VMEM((2 * k_rows, width), bf),
            pltpu.VMEM((cores * cols * o_own, features // cores), bf),
            pltpu.VMEM(hidden.shape, bf), pltpu.SMEM(positions.shape, jnp.int32),
            pltpu.VMEM(key_cache.shape, bf), pltpu.VMEM(value_cache.shape, bf),
            pltpu.VMEM((width,), f32), pltpu.VMEM((share,), f32), pltpu.VMEM((1, head_dim), f32),
            pltpu.VMEM((batch, columns), f32), pltpu.VMEM((batch, q_local, head_dim), f32),
            pltpu.VMEM((batch, q_local, head_dim), f32), pltpu.VMEM((batch, q_local, head_dim), f32),
            pltpu.VMEM((batch, features), f32), pltpu.VMEM((planes, batch, share), f32),
            pltpu.VMEM((planes, batch, share), f32), pltpu.VMEM((planes, cols, batch, share), f32),
            dma((7,)), dma((1,)), dma((planes,)),
            dma((3,)), dma((2,)), dma((1,)), dma((1,)),
            dma((2,)), dma((planes, total)), dma((1,)), dma((moving,)),
            dma((1,)), dma((1,)), dma((1,)), dma((planes,)),
        ],
        compiler_params=pltpu.CompilerParams(
            collective_id=0, has_side_effects=True, vmem_limit_bytes=34 * 2**20),
        name="move",
    )(q_proj, k_proj, v_proj, o_proj, hidden, positions, key_cache, value_cache,
      norm_gain, post_gain, freq)
    joined, heads, result = out

    def spill_kernel(a, b, r, a_out, b_out, r_out, sems):
        copies = [pltpu.make_async_copy(r, r_out, sems.at[0])]
        for source, target in ((a, a_out), (b, b_out)):
            rows = source.shape[0] // 4
            for i in range(4):
                span = pl.ds(i * rows, rows)
                copies.append(pltpu.make_async_copy(source.at[span], target.at[span], sems.at[len(copies)]))
        for copy in copies:
            copy.start()
        for copy in copies:
            copy.wait()

    vmem = pl.BlockSpec(memory_space=pltpu.VMEM)
    return tuple(pl.pallas_call(
        spill_kernel,
        in_specs=[vmem] * 3,
        out_specs=[hbm] * 3,
        out_shape=[jax.ShapeDtypeStruct(x.shape, x.dtype) for x in (joined, heads, result)],
        scratch_shapes=[dma((9,))],
        compiler_params=pltpu.CompilerParams(vmem_limit_bytes=2**20),
        name="spill",
    )(joined, heads, result))


def body(*args):
    cols, reps = lax.axis_size("tp"), lax.axis_size("rep")
    key_cache, q_proj, k_proj, o_proj = args[2], args[5], args[6], args[8]
    lanes = 128
    fits = (
        reps == 2 * cols
        and cols % 2 == 0
        and key_cache.shape[3] == lanes
        and q_proj.shape[0] == lanes
        and 2 * k_proj.shape[0] == lanes
        and o_proj.shape[0] % 16 == 0
        and q_proj.shape[1] % (4 * lanes) == 0
        and o_proj.shape[1] % (8 * lanes * cols) == 0
        and (2 * cols * o_proj.shape[0]) % lanes == 0
    )
    return (line_body if fits else general_body)(*args)


def solution(mesh):
    in_specs = (
        P("rep", None), P("rep"), P("rep", "tp", None, None), P("rep", "tp", None, None), P(),
        P(("rep", "tp"), None), P(("rep", "tp"), None), P(("rep", "tp"), None), P(("rep", "tp"), None), P("tp"),
    )
    out_specs = (P(None, "tp"), P("tp", None), P("rep", "tp"))
    return jax.shard_map(body, mesh=mesh, in_specs=in_specs, out_specs=out_specs, check_vma=False)
```

```python
import functools

import jax
import jax.numpy as jnp
import numpy as np
from jax import lax
from jax.experimental import pallas as pl
from jax.experimental.pallas import tpu as pltpu
from jax.sharding import PartitionSpec as P

MESH = pl.DeviceIdType.MESH
score_scale = 144.0 ** (-0.5)
soft_cap = 50.0


def rms_scale(values, gain):
    mean_square = jnp.mean(values * values, axis=-1, keepdims=True)
    return values * lax.rsqrt(mean_square + 1e-06) * gain


def rotate(values, positions):
    half = values.shape[-1] // 2
    freq = 10000.0 ** (-2.0 * jnp.arange(half, dtype=jnp.float32) / values.shape[-1])
    angle = positions.astype(jnp.float32)[:, None] * freq[None, :]
    cosine = jnp.cos(angle)[:, None, :]
    sine = jnp.sin(angle)[:, None, :]
    first = values[..., :half]
    second = values[..., half:]
    return jnp.concatenate(
        [first * cosine - second * sine, second * cosine + first * sine], axis=-1
    )


def join_kernel(per_tp, q_rows, k_rows, *refs):
    slot = lax.rem(lax.axis_index("rep"), per_tp)
    parts, out_ref = refs[:-1], refs[-1]
    tp_count = parts[0].shape[0]
    q_all = tp_count * per_tp * q_rows
    k_all = tp_count * per_tp * k_rows
    for step in range(per_tp):
        who = lax.rem(slot + step, per_tp)
        q_ref, kv_ref = parts[2 * step], parts[2 * step + 1]
        for start, ref, low, rows in (
            (0, q_ref, 0, q_rows),
            (q_all, kv_ref, 0, k_rows),
            (q_all + k_all, kv_ref, k_rows, k_rows),
        ):
            block = ref[:, low : low + rows, :].reshape(tp_count * rows, -1)
            at = pl.multiple_of(start + who * (tp_count * rows), 128)
            out_ref[:, pl.ds(at, tp_count * rows)] = jnp.transpose(block)


def join(per_tp, pairs):
    tp_count, q_rows, width = pairs[0][0].shape
    k_rows = pairs[0][1].shape[1] // 2
    columns = tp_count * per_tp * (q_rows + 2 * k_rows)
    stripe = 256
    operands, specs = [], []
    for pair in pairs:
        for matrix in pair:
            operands.append(matrix)
            specs.append(
                pl.BlockSpec((tp_count, matrix.shape[1], stripe), lambda j: (0, 0, j))
            )
    size = width * columns * 2
    return pl.pallas_call(
        functools.partial(join_kernel, per_tp, q_rows, k_rows),
        grid=(width // stripe,),
        in_specs=specs,
        out_specs=pl.BlockSpec((stripe, columns), lambda j: (j, 0)),
        out_shape=jax.ShapeDtypeStruct((width, columns), jnp.bfloat16),
        cost_estimate=pl.CostEstimate(flops=0, bytes_accessed=2 * size, transcendentals=0),
        name="join",
    )(*operands)


def turn_kernel(rows_ref, out_ref):
    out_ref[...] = jnp.transpose(rows_ref[...])


def turn(rows):
    height, width = rows.shape
    stripe = 384 if height % 384 == 0 else 128
    return pl.pallas_call(
        turn_kernel,
        grid=(height // stripe,),
        in_specs=[pl.BlockSpec((stripe, width), lambda j: (j, 0))],
        out_specs=pl.BlockSpec((width, stripe), lambda j: (0, j)),
        out_shape=jax.ShapeDtypeStruct((width, height), rows.dtype),
        cost_estimate=pl.CostEstimate(
            flops=0, bytes_accessed=4 * height * width, transcendentals=0
        ),
        name="turn",
    )(rows)


def general_body(
    hidden, positions, key_cache, value_cache, norm_gain, q_proj, k_proj, v_proj, o_proj, post_gain
):
    tp_count = lax.axis_size("tp")
    replica_count = lax.axis_size("rep")
    per_tp = replica_count // tp_count
    model_width = hidden.shape[1]
    q_rows, k_rows = q_proj.shape[0], k_proj.shape[0]

    groups = [[i + per_tp * p for p in range(tp_count)] for i in range(per_tp)]
    shifts = [
        [
            (per_tp * p + (i + d) % per_tp, per_tp * p + i)
            for p in range(tp_count)
            for i in range(per_tp)
        ]
        for d in range(1, per_tp)
    ]

    def collect(rows):
        planes = lax.all_gather(rows[None], "rep", axis=0, tiled=True, axis_index_groups=groups)
        return lax.all_to_all(planes, "tp", split_axis=0, concat_axis=0, tiled=True)

    kv_rows = collect(jnp.concatenate([k_proj, v_proj], axis=0))
    split_cols = o_proj.reshape(o_proj.shape[0], tp_count, -1)
    rows_of_group = lax.all_to_all(split_cols, "tp", split_axis=1, concat_axis=0, tiled=True)

    batch, kv_local, length, head_dim = key_cache.shape

    def scatter_rows(values):
        wide = values.reshape(replica_count, batch, -1)
        by_rep = lax.all_to_all(wide, "rep", split_axis=0, concat_axis=0, tiled=True)
        return by_rep

    def to_block(by_rep):
        arrived = lax.all_to_all(by_rep, "tp", split_axis=0, concat_axis=0, tiled=True)
        arrived = arrived.reshape(tp_count, per_tp, batch, -1)
        return jnp.transpose(arrived, (2, 1, 0, 3))

    normed = rms_scale(hidden.astype(jnp.float32), norm_gain).astype(jnp.bfloat16)
    normed_all = lax.all_gather(normed, "rep", axis=0, tiled=True)
    contract = (((1,), (1,)), ((), ()))
    local = jnp.concatenate(
        [
            lax.dot_general(normed_all, matrix, contract, preferred_element_type=jnp.float32)
            for matrix in (q_proj, k_proj, v_proj)
        ],
        axis=1,
    )
    block = to_block(scatter_rows(local))
    q_local = tp_count * per_tp * q_rows // head_dim
    group = q_local // kv_local
    query = block[..., :q_rows].reshape(batch, q_local, head_dim)
    keys_new = block[..., q_rows : q_rows + k_rows].reshape(batch, kv_local, head_dim)
    values_new = block[..., q_rows + k_rows :].reshape(batch, kv_local, head_dim)
    query_rot = rotate(query, positions).astype(jnp.bfloat16)
    rotated_keys = rotate(keys_new, positions).astype(jnp.bfloat16)
    values_rot = values_new.astype(jnp.bfloat16)
    grouped_heads = query_rot.reshape(batch, kv_local, group, head_dim)
    scores = (
        jnp.einsum("bkgd,bkld->bkgl", grouped_heads, key_cache, preferred_element_type=jnp.float32)
        * score_scale
    )
    capped = soft_cap * jnp.tanh(scores / soft_cap)
    valid = jnp.arange(length, dtype=jnp.int32)[None, :] < positions[:, None]
    weight_raw = jnp.where(valid[:, None, None, :], jnp.exp(capped), 0.0)
    self_score = (
        jnp.einsum("juzy,juy->juz", grouped_heads, rotated_keys, preferred_element_type=jnp.float32)
        * score_scale
    )
    self_raw = jnp.exp(soft_cap * jnp.tanh(self_score / soft_cap))
    denom = jnp.sum(weight_raw, axis=-1) + self_raw
    weights = (weight_raw / denom[..., None]).astype(jnp.bfloat16)
    self_weight = (self_raw / denom).astype(jnp.bfloat16)
    attention = jnp.einsum(
        "bkgl,bkld->bkgd", weights, value_cache, preferred_element_type=jnp.float32
    )
    attention = (
        attention
        + self_weight.astype(jnp.float32)[..., None] * values_rot.astype(jnp.float32)[:, :, None, :]
    )
    attention = attention.reshape(batch, q_local * head_dim).astype(jnp.bfloat16)
    q_later, attention = lax.optimization_barrier((q_proj, attention))
    q_own = collect(q_later)
    pairs = [(q_own, kv_rows)]
    for shift in shifts:
        pairs.append((lax.ppermute(q_own, "rep", shift), lax.ppermute(kv_rows, "rep", shift)))
    joined_block = join(per_tp, pairs)
    own_all = lax.all_gather(attention, "tp", axis=1, tiled=True)
    attention_all = lax.all_gather(own_all, "rep", axis=0, tiled=True)
    projected = lax.dot_general(
        attention_all, o_proj, contract, preferred_element_type=jnp.float32
    )
    by_rep = scatter_rows(projected)
    share = to_block(by_rep).reshape(batch, -1)
    square = jnp.sum(share * share, axis=1)
    square_all = lax.all_gather(square[None], "tp", axis=0, tiled=True)
    multiplier = lax.rsqrt(jnp.sum(square_all, axis=0) / model_width + 1e-06)
    result = share * multiplier[:, None] * post_gain
    rows_of_group, result = lax.optimization_barrier((rows_of_group, result))
    complete_rows = lax.all_gather(rows_of_group, "rep", axis=0, tiled=True)
    out_block = turn(complete_rows.reshape(model_width, -1))
    return (joined_block, out_block, result.astype(jnp.bfloat16))


def move_kernel(
    sizes,
    q_ref, k_ref, v_ref, o_ref,
    hidden_ref, positions_ref, keys_ref, values_ref, gain_ref, post_ref, freq_ref,
    joined, heads, result,
    stage, q_own, kv_own, o_rows,
    hidden, positions, keys, values, gain, post, freq,
    fresh, q_heads, k_heads, v_heads, attended, far_attended, far_partial, partial, partial_sum, others,
    early_sems, far_sems, share_send, share_recv,
    local_sems, kv_sems, rows_send, rows_recv,
    line_send, line_recv, plane_send, plane_recv,
    twin_send, twin_recv, twin_wo_send, twin_wo_recv,
):
    planes, cores, cols, pieces = sizes
    rep, t = lax.axis_index("rep"), lax.axis_index("tp")
    z, c = rep // cores, lax.rem(rep, cores)
    other = 1 - c
    width = q_ref.shape[1]
    deep = width // pieces
    q_rows, k_rows = q_ref.shape[0], k_ref.shape[0]
    o_own = o_ref.shape[0]
    block = cols * cores * o_own
    half = heads.shape[0] // cores
    wo_rows = half // pieces
    moving = 2 * pieces
    total = 3 * pieces
    q_all = cores * cols * q_rows
    k_all = cores * cols * k_rows
    even = lax.rem(t, 2) == 0

    def at(zz, cc, tt):
        return (zz * cores + cc, tt)

    def column(tt, j, cc):
        parity = lax.rem(tt, 2)
        q_at = (cc * cols + tt) * q_rows
        kv_at = q_all + parity * k_all + (cc * cols + tt - parity) * k_rows
        is_q = (j < pieces).astype(jnp.int32)
        return pl.multiple_of(is_q * q_at + (1 - is_q) * kv_at, 128)

    def slot(tt, j, cc):
        row = pl.multiple_of(lax.rem(j, pieces) * deep, 128)
        return joined.at[pl.ds(row, deep), pl.ds(column(tt, j, cc), 128)]

    def wo_slot(zz, j, cc):
        row = pl.multiple_of(cc * half + (j - moving) * wo_rows, 128)
        col = pl.multiple_of(zz * block, 128)
        return heads.at[pl.ds(row, wo_rows), pl.ds(col, block)]

    def remote(src, dst, send, recv, device):
        return pltpu.make_async_remote_copy(
            src_ref=src, dst_ref=dst, send_sem=send, recv_sem=recv,
            device_id=device, device_id_type=MESH,
        )

    def line_copy(zz, j, way, device):
        return remote(stage.at[zz, j], stage.at[zz, j], line_send.at[way],
                      line_recv.at[zz, j], device)

    def line_wo_copy(zz, j, way, device):
        return remote(wo_slot(zz, j, c), wo_slot(zz, j, c), line_send.at[way],
                      line_recv.at[zz, j], device)

    def plane_copy(zz, j):
        return remote(stage.at[zz, j], slot(t, j, c), plane_send.at[0],
                      plane_recv.at[j], at(z, c, zz))

    def wait_bytes(view, sem):
        pltpu.make_async_copy(view, view, sem).wait()

    def twin_copy(src, tt, j, cc):
        return remote(src, slot(tt, j, cc), twin_send.at[0], twin_recv.at[0], at(z, other, t))

    def twin_wo_copy(zz, j, cc):
        return remote(wo_slot(zz, j, cc), wo_slot(zz, j, cc), twin_wo_send.at[0],
                      twin_wo_recv.at[zz], at(z, other, t))

    def rows_copy(dc, dt):
        cc, tt = lax.rem(c + dc, cores), lax.rem(t + dt, cols)
        mine = c * cols + t
        src_at = pl.multiple_of((tt * cores + cc) * half, 128)
        dst_at = pl.multiple_of(mine * o_own, 16)
        return remote(o_ref.at[:, pl.ds(src_at, half)], o_rows.at[pl.ds(dst_at, o_own), :],
                      rows_send.at[0], rows_recv.at[0], at(z, cc, tt))

    peers = [(dc, dt) for dc in range(cores) for dt in range(cols) if dc or dt]

    barrier = pltpu.get_barrier_semaphore()
    for dc, dt in peers:
        pl.semaphore_signal(
            barrier, inc=1, device_id=at(z, lax.rem(c + dc, cores), lax.rem(t + dt, cols)),
            device_id_type=MESH)

    @pl.when(z > 0)
    def _():
        pl.semaphore_signal(barrier, inc=1, device_id=at(z - 1, c, t), device_id_type=MESH)

    @pl.when(z < planes - 1)
    def _():
        pl.semaphore_signal(barrier, inc=1, device_id=at(z + 1, c, t), device_id_type=MESH)

    far_end = jnp.where(2 * z < planes, planes - 1, 0)
    is_end = jnp.logical_or(z == 0, z == planes - 1)

    @pl.when(is_end)
    def _():
        pl.semaphore_signal(barrier, inc=1, device_id=at(far_end, c, t), device_id_type=MESH)

    load_q = pltpu.make_async_copy(q_ref, q_own, local_sems.at[0])
    load_q.start()
    mine = c * cols + t
    load_o = pltpu.make_async_copy(
        o_ref.at[:, pl.ds(pl.multiple_of((t * cores + c) * half, 128), half)],
        o_rows.at[pl.ds(pl.multiple_of(mine * o_own, 16), o_own), :], local_sems.at[1])
    load_o.start()
    load_k = pltpu.make_async_copy(k_ref, kv_own.at[pl.ds(0, k_rows)], local_sems.at[2])
    load_v = pltpu.make_async_copy(v_ref, kv_own.at[pl.ds(k_rows, k_rows)], local_sems.at[2])

    @pl.when(even)
    def _():
        load_k.start()

    @pl.when(jnp.logical_not(even))
    def _():
        load_v.start()

    give_v = remote(v_ref, kv_own.at[pl.ds(0, k_rows)], kv_sems.at[0], kv_sems.at[1], at(z, c, t + 1 - 2 * lax.rem(t, 2)))
    give_k = remote(k_ref, kv_own.at[pl.ds(k_rows, k_rows)], kv_sems.at[0], kv_sems.at[1], at(z, c, t + 1 - 2 * lax.rem(t, 2)))

    early = [
        pltpu.make_async_copy(source, target, early_sems.at[i])
        for i, (source, target) in enumerate((
            (hidden_ref, hidden), (positions_ref, positions), (gain_ref, gain), (post_ref, post),
            (freq_ref, freq), (keys_ref, keys), (values_ref, values)))
    ]

    batch, kv_local, length, head_dim = keys_ref.shape
    q_local = q_all // head_dim
    group = q_local // kv_local
    f32, bf16 = jnp.float32, jnp.bfloat16

    def project():
        for copy in early[:5]:
            copy.wait()
        wide = hidden[...].astype(f32)
        mean_square = jnp.mean(wide * wide, axis=-1, keepdims=True)
        normed = (wide * lax.rsqrt(mean_square + 1e-06) * gain[...].reshape(1, -1)).astype(bf16)

        def columns(i, carry):
            span = pl.ds(pl.multiple_of(i * 256, 256), 256)
            fresh[:, span] = jnp.dot(normed, joined[:, span], preferred_element_type=f32)
            return carry

        lax.fori_loop(0, fresh.shape[1] // 256, columns, 0)
        angle = jnp.concatenate(
            [positions[b].astype(f32) * freq[...] for b in range(batch)], axis=0)
        cosine, sine = jnp.cos(angle), jnp.sin(angle)
        lane = lax.broadcasted_iota(jnp.int32, angle.shape, 1)
        sine = jnp.where(lane < head_dim // 2, -sine, sine)

        def turned(start):
            x = fresh[:, start : start + head_dim]
            swapped = pltpu.roll(x, head_dim // 2, 1)
            return (x * cosine + swapped * sine).astype(bf16).astype(f32)

        for h in range(kv_local):
            key = turned(q_all + h * head_dim)
            at_v = q_all + k_all + h * head_dim
            value = fresh[:, at_v : at_v + head_dim].astype(bf16).astype(f32)
            for g in range(group):
                n = h * group + g
                query = turned(n * head_dim)
                for b in range(batch):
                    q_heads[b, n : n + 1, :] = query[b : b + 1]
                    k_heads[b, n : n + 1, :] = key[b : b + 1]
                    v_heads[b, n : n + 1, :] = value[b : b + 1]

    def attend():
        for copy in early[5:]:
            copy.wait()
        over = (((1,), (1,)), ((), ()))
        slots = lax.broadcasted_iota(jnp.int32, (q_local, length), 1)
        owner = lax.broadcasted_iota(jnp.int32, (q_local, 1), 0) // group
        for b in range(batch):
            query = q_heads[b]
            narrow = query.astype(bf16)
            scores = jnp.zeros((q_local, length), f32)
            for h in range(kv_local):
                one = lax.dot_general(narrow, keys[b, h], over, preferred_element_type=f32)
                scores = jnp.where(owner == h, one, scores)
            raw = jnp.exp(soft_cap * jnp.tanh(scores * score_scale / soft_cap))
            raw = jnp.where(slots < positions[b], raw, 0.0)
            self_score = jnp.sum(query * k_heads[b], axis=-1, keepdims=True) * score_scale
            self_raw = jnp.exp(soft_cap * jnp.tanh(self_score / soft_cap))
            denom = jnp.sum(raw, axis=-1, keepdims=True) + self_raw
            weights = (raw / denom).astype(bf16)
            self_weight = (self_raw / denom).astype(bf16).astype(f32)
            mixed = jnp.zeros((q_local, head_dim), f32)
            for h in range(kv_local):
                one = jnp.dot(weights, values[b, h], preferred_element_type=f32)
                mixed = jnp.where(owner == h, one, mixed)
            mixed = mixed + self_weight * v_heads[b]
            for n in range(q_local):
                attended[b : b + 1, n * head_dim : (n + 1) * head_dim] = mixed[n : n + 1]

    def share_copy(zz, dt):
        p = lax.rem(t + dt, cols)
        return remote(partial.at[zz], others.at[zz, t], share_send.at[0], share_recv.at[zz], at(z, c, p))

    def take_heads(zz):
        row = pl.multiple_of(other * half, 128)
        col = pl.multiple_of(zz * block, 128)
        wait_bytes(heads.at[pl.ds(row, half), pl.ds(col, block)], twin_wo_recv.at[zz])

    def project_slice(source, zz):
        span = pl.ds(pl.multiple_of(zz * block, 128), block)
        return jnp.dot(source[...].astype(bf16), heads[:, span], preferred_element_type=f32)

    def answer_far():
        ask_far.wait_recv()
        take_heads(z)
        far_partial[...] = project_slice(far_attended, z)
        tell_far.start()
        partial[z] = project_slice(attended, z)
        share_out(z)

    def share_out(zz):
        for dt in range(1, cols):
            share_copy(zz, dt).start()

    def add_slice(zz):
        take_heads(zz)
        partial[zz] = project_slice(attended, zz)
        share_out(zz)

    ask_far = remote(attended, far_attended, far_sems.at[0], far_sems.at[1], at(far_end, c, t))
    tell_far = remote(far_partial, partial.at[z], far_sems.at[2], far_sems.at[3], at(far_end, c, t))

    def sum_slice(zz):
        share = partial[zz]
        wait_bytes(others.at[0, pl.ds(0, cols - 1)], share_recv.at[zz])
        for dt in range(1, cols):
            share = share + others[zz, lax.rem(t + dt, cols)]
        partial_sum[zz] = share
        return jnp.sum(share * share, axis=-1, keepdims=True)

    def near(step):
        return lax.rem(far_end + 1 + step, planes)

    def finish():
        square = jnp.zeros((batch, 1), f32)
        for step in range(planes - 1):
            square = square + sum_slice(near(step))
        square = square + sum_slice(far_end)
        multiplier = lax.rsqrt(square / width + 1e-06)
        result[...] = (partial_sum[t] * multiplier * post[...].reshape(1, -1)).astype(result.dtype)
        wait_bytes(others.at[pl.ds(0, cols - 1)], share_send.at[0])

    def prepare(j):
        @pl.when(j < pieces)
        def _():
            span = pl.ds(pl.multiple_of(j * deep, 128), deep)
            stage[z, j] = jnp.transpose(q_own[:, span])

        @pl.when(j == pieces)
        def _():
            @pl.when(even)
            def _():
                load_k.wait()
                give_k.wait_recv()

            @pl.when(jnp.logical_not(even))
            def _():
                load_v.wait()
                give_v.wait_recv()

        @pl.when(jnp.logical_and(j >= pieces, j < moving))
        def _():
            span = pl.ds(pl.multiple_of((j - pieces) * deep, 128), deep)
            stage[z, j] = jnp.transpose(kv_own[:, span])

        @pl.when(j == moving)
        def _():
            load_o.wait()
            wait_bytes(o_rows.at[pl.ds(0, len(peers) * o_own)], rows_recv.at[0])

        @pl.when(jnp.logical_and(j >= moving, j < total))
        def _():
            col = pl.multiple_of((j - moving) * wo_rows, 128)
            row = pl.multiple_of(c * half + (j - moving) * wo_rows, 128)
            heads[pl.ds(row, wo_rows), pl.ds(pl.multiple_of(z * block, 128), block)] = jnp.transpose(
                o_rows[:, pl.ds(col, wo_rows)])

    def send_line(zz, j, way):
        target = at(z - 1, c, t) if way == 0 else at(z + 1, c, t)
        room = z > 0 if way == 0 else z < planes - 1

        @pl.when(jnp.logical_and(room, j < moving))
        def _():
            line_copy(zz, j, way, target).start()

        @pl.when(jnp.logical_and(room, j >= moving))
        def _():
            line_wo_copy(zz, j, way, target).start()

    def wait_line(zz, j):
        @pl.when(j < moving)
        def _():
            line_copy(zz, j, 0, at(z, other, t)).wait_recv()

        @pl.when(j >= moving)
        def _():
            line_wo_copy(zz, j, 0, at(z, other, t)).wait_recv()

    def deliver(zz, j):
        @pl.when(jnp.logical_and(j < moving, t != zz))
        def _():
            plane_copy(zz, j).start()

        @pl.when(jnp.logical_and(j < moving, t == zz))
        def _():
            row = pl.multiple_of(lax.rem(j, pieces) * deep, 128)
            joined[pl.ds(row, deep), pl.ds(column(t, j, c), 128)] = stage[zz, j]
            twin_copy(stage.at[zz, j], t, j, c).start()

        @pl.when(j >= moving)
        def _():
            twin_wo_copy(zz, j, c).start()

    for copy in early[:5]:
        copy.start()
    load_q.wait()
    prepare(jnp.int32(0))
    n_line = (z > 0).astype(jnp.int32) + (z < planes - 1).astype(jnp.int32) + is_end.astype(jnp.int32)
    pl.semaphore_wait(barrier, len(peers) + n_line)

    def rounds(r, carry):
        @pl.when(r < total)
        def _():
            send_line(z, r, 0)
            send_line(z, r, 1)
            deliver(z, r)

        @pl.when(r == 0)
        def _():
            @pl.when(even)
            def _():
                give_v.start()

            @pl.when(jnp.logical_not(even))
            def _():
                give_k.start()

        @pl.when(r == 3)
        def _():
            for dc, dt in peers:
                rows_copy(dc, dt).start()
            for copy in early[5:]:
                copy.start()

        @pl.when(r + 1 < total)
        def _():
            prepare(r + 1)

        for k in range(1, planes):
            if k == planes - 1:
                pl.when(jnp.logical_and(is_end, r == total + planes - 3))(answer_far)
            for way in (0, 1):
                zz = z + k if way == 0 else z - k
                j = r - k
                inside = zz < planes if way == 0 else zz >= 0

                @pl.when(jnp.logical_and(inside, jnp.logical_and(j >= 0, j < total)))
                def _():
                    wait_line(zz, j)
                    send_line(zz, j, way)
                    deliver(zz, j)

        far = jnp.where(z > t, z - t, t - z)
        j = r - far - 1

        @pl.when(jnp.logical_and(j >= 0, j < moving))
        def _():
            wait_bytes(stage.at[0, pl.ds(0, cols - 1)], plane_recv.at[j])
            for dt in range(1, cols):
                tt = lax.rem(t + dt, cols)
                twin_copy(slot(tt, j, c), tt, j, c).start()

        @pl.when(r == moving + 1 + far)
        def _():
            wait_bytes(joined.at[pl.ds(0, width // cores)], twin_recv.at[0])
            project()
            attend()

            @pl.when(is_end)
            def _():
                ask_far.start()

        return carry

    lax.fori_loop(0, total + planes - 2, rounds, 0)

    @pl.when(is_end)
    def _():
        for k in range(1, planes - 1):
            add_slice(jnp.where(z == 0, k, planes - 1 - k))
        remote(partial.at[far_end], partial.at[far_end], far_sems.at[2], far_sems.at[3],
               at(far_end, c, t)).wait_recv()
        share_out(far_end)

    rounds(jnp.int32(total + planes - 2), 0)

    @pl.when(jnp.logical_not(is_end))
    def _():
        for zz in range(planes):
            add_slice(zz)

    finish()

    @pl.when(is_end)
    def _():
        take_heads(far_end)
        ask_far.wait_send()
        tell_far.wait_send()

    unit = deep * 128 // joined.shape[1]
    for way, count in ((0, planes - z), (1, z + 1)):
        for m in range(1, planes):

            @pl.when(count == m)
            def _():
                wait_bytes(joined.at[pl.ds(0, m * total * unit)], line_send.at[way])
    wait_bytes(joined.at[pl.ds(0, (planes - 1) * moving * unit)], plane_send.at[0])
    wait_bytes(joined.at[pl.ds(0, width // cores)], twin_send.at[0])
    wait_bytes(heads.at[pl.ds(0, half)], twin_wo_send.at[0])
    wait_bytes(o_rows.at[pl.ds(0, len(peers) * o_own)], rows_send.at[0])

    @pl.when(even)
    def _():
        give_v.wait_send()

    @pl.when(jnp.logical_not(even))
    def _():
        give_k.wait_send()


def line_body(hidden, positions, key_cache, value_cache, norm_gain, q_proj, k_proj, v_proj, o_proj, post_gain):
    cols = lax.axis_size("tp")
    cores = 2
    planes = lax.axis_size("rep") // cores
    pieces = 4
    width = q_proj.shape[1]
    deep = width // pieces
    q_rows, k_rows, o_own = q_proj.shape[0], k_proj.shape[0], o_proj.shape[0]
    features = o_proj.shape[1] // cols
    columns = cores * cols * (q_rows + 2 * k_rows)
    model = o_own * cores * cols * planes
    bf = jnp.bfloat16
    dma = pltpu.SemaphoreType.DMA
    hbm = pl.BlockSpec(memory_space=pltpu.HBM)
    f32 = jnp.float32
    batch, kv_local, length, head_dim = key_cache.shape
    q_local = cores * cols * q_rows // head_dim
    half = head_dim // 2
    freq = 10000.0 ** (-2.0 * np.arange(half) / head_dim)
    freq = jnp.asarray(np.concatenate([freq, freq])[None], f32)
    share = post_gain.shape[0]
    moving, total = 2 * pieces, 3 * pieces
    out = pl.pallas_call(
        functools.partial(move_kernel, (planes, cores, cols, pieces)),
        in_specs=[hbm] * 11,
        out_shape=[
            pltpu.VMEM((width, columns), bf),
            pltpu.VMEM((features, model), bf),
            pltpu.VMEM((hidden.shape[0], post_gain.shape[0]), bf),
        ],
        out_specs=[pl.BlockSpec(memory_space=pltpu.VMEM)] * 3,
        scratch_shapes=[
            pltpu.VMEM((planes, moving, deep, 128), bf),
            pltpu.VMEM((q_rows, width), bf),
            pltpu.VMEM((2 * k_rows, width), bf),
            pltpu.VMEM((cores * cols * o_own, features // cores), bf),
            pltpu.VMEM(hidden.shape, bf), pltpu.SMEM(positions.shape, jnp.int32),
            pltpu.VMEM(key_cache.shape, bf), pltpu.VMEM(value_cache.shape, bf),
            pltpu.VMEM((width,), f32), pltpu.VMEM((share,), f32), pltpu.VMEM((1, head_dim), f32),
            pltpu.VMEM((batch, columns), f32), pltpu.VMEM((batch, q_local, head_dim), f32),
            pltpu.VMEM((batch, q_local, head_dim), f32), pltpu.VMEM((batch, q_local, head_dim), f32),
            pltpu.VMEM((batch, features), f32), pltpu.VMEM((batch, features), f32),
            pltpu.VMEM((batch, share), f32), pltpu.VMEM((planes, batch, share), f32),
            pltpu.VMEM((planes, batch, share), f32), pltpu.VMEM((planes, cols, batch, share), f32),
            dma((7,)), dma((4,)), dma((1,)), dma((planes,)),
            dma((3,)), dma((2,)), dma((1,)), dma((1,)),
            dma((2,)), dma((planes, total)), dma((1,)), dma((moving,)),
            dma((1,)), dma((1,)), dma((1,)), dma((planes,)),
        ],
        compiler_params=pltpu.CompilerParams(
            collective_id=0, has_side_effects=True, vmem_limit_bytes=34 * 2**20),
        name="move",
    )(q_proj, k_proj, v_proj, o_proj, hidden, positions, key_cache, value_cache,
      norm_gain, post_gain, freq)
    joined, heads, result = out

    def spill_kernel(a, b, r, a_out, b_out, r_out, sems):
        copies = [pltpu.make_async_copy(r, r_out, sems.at[0])]
        for source, target in ((a, a_out), (b, b_out)):
            rows = source.shape[0] // 4
            for i in range(4):
                span = pl.ds(i * rows, rows)
                copies.append(pltpu.make_async_copy(source.at[span], target.at[span], sems.at[len(copies)]))
        for copy in copies:
            copy.start()
        for copy in copies:
            copy.wait()

    vmem = pl.BlockSpec(memory_space=pltpu.VMEM)
    return tuple(pl.pallas_call(
        spill_kernel,
        in_specs=[vmem] * 3,
        out_specs=[hbm] * 3,
        out_shape=[jax.ShapeDtypeStruct(x.shape, x.dtype) for x in (joined, heads, result)],
        scratch_shapes=[dma((9,))],
        compiler_params=pltpu.CompilerParams(vmem_limit_bytes=2**20),
        name="spill",
    )(joined, heads, result))


def body(*args):
    cols, reps = lax.axis_size("tp"), lax.axis_size("rep")
    key_cache, q_proj, k_proj, o_proj = args[2], args[5], args[6], args[8]
    lanes = 128
    fits = (
        reps == 2 * cols
        and cols % 2 == 0
        and cols > 2
        and key_cache.shape[3] == lanes
        and q_proj.shape[0] == lanes
        and 2 * k_proj.shape[0] == lanes
        and o_proj.shape[0] % 16 == 0
        and q_proj.shape[1] % (4 * lanes) == 0
        and o_proj.shape[1] % (8 * lanes * cols) == 0
        and (2 * cols * o_proj.shape[0]) % lanes == 0
    )
    return (line_body if fits else general_body)(*args)


def solution(mesh):
    in_specs = (
        P("rep", None), P("rep"), P("rep", "tp", None, None), P("rep", "tp", None, None), P(),
        P(("rep", "tp"), None), P(("rep", "tp"), None), P(("rep", "tp"), None), P(("rep", "tp"), None), P("tp"),
    )
    out_specs = (P(None, "tp"), P("tp", None), P("rep", "tp"))
    return jax.shard_map(body, mesh=mesh, in_specs=in_specs, out_specs=out_specs, check_vma=False)
```

```python
import functools

import jax
import jax.numpy as jnp
import numpy as np
from jax import lax
from jax.experimental import pallas as pl
from jax.experimental.pallas import tpu as pltpu
from jax.sharding import PartitionSpec as P

MESH = pl.DeviceIdType.MESH
score_scale = 144.0 ** (-0.5)
soft_cap = 50.0


def rms_scale(values, gain):
    mean_square = jnp.mean(values * values, axis=-1, keepdims=True)
    return values * lax.rsqrt(mean_square + 1e-06) * gain


def rotate(values, positions):
    half = values.shape[-1] // 2
    freq = 10000.0 ** (-2.0 * jnp.arange(half, dtype=jnp.float32) / values.shape[-1])
    angle = positions.astype(jnp.float32)[:, None] * freq[None, :]
    cosine = jnp.cos(angle)[:, None, :]
    sine = jnp.sin(angle)[:, None, :]
    first = values[..., :half]
    second = values[..., half:]
    return jnp.concatenate(
        [first * cosine - second * sine, second * cosine + first * sine], axis=-1
    )


def join_kernel(per_tp, q_rows, k_rows, *refs):
    slot = lax.rem(lax.axis_index("rep"), per_tp)
    parts, out_ref = refs[:-1], refs[-1]
    tp_count = parts[0].shape[0]
    q_all = tp_count * per_tp * q_rows
    k_all = tp_count * per_tp * k_rows
    for step in range(per_tp):
        who = lax.rem(slot + step, per_tp)
        q_ref, kv_ref = parts[2 * step], parts[2 * step + 1]
        for start, ref, low, rows in (
            (0, q_ref, 0, q_rows),
            (q_all, kv_ref, 0, k_rows),
            (q_all + k_all, kv_ref, k_rows, k_rows),
        ):
            block = ref[:, low : low + rows, :].reshape(tp_count * rows, -1)
            at = pl.multiple_of(start + who * (tp_count * rows), 128)
            out_ref[:, pl.ds(at, tp_count * rows)] = jnp.transpose(block)


def join(per_tp, pairs):
    tp_count, q_rows, width = pairs[0][0].shape
    k_rows = pairs[0][1].shape[1] // 2
    columns = tp_count * per_tp * (q_rows + 2 * k_rows)
    stripe = 256
    operands, specs = [], []
    for pair in pairs:
        for matrix in pair:
            operands.append(matrix)
            specs.append(
                pl.BlockSpec((tp_count, matrix.shape[1], stripe), lambda j: (0, 0, j))
            )
    size = width * columns * 2
    return pl.pallas_call(
        functools.partial(join_kernel, per_tp, q_rows, k_rows),
        grid=(width // stripe,),
        in_specs=specs,
        out_specs=pl.BlockSpec((stripe, columns), lambda j: (j, 0)),
        out_shape=jax.ShapeDtypeStruct((width, columns), jnp.bfloat16),
        cost_estimate=pl.CostEstimate(flops=0, bytes_accessed=2 * size, transcendentals=0),
        name="join",
    )(*operands)


def turn_kernel(rows_ref, out_ref):
    out_ref[...] = jnp.transpose(rows_ref[...])


def turn(rows):
    height, width = rows.shape
    stripe = 384 if height % 384 == 0 else 128
    return pl.pallas_call(
        turn_kernel,
        grid=(height // stripe,),
        in_specs=[pl.BlockSpec((stripe, width), lambda j: (j, 0))],
        out_specs=pl.BlockSpec((width, stripe), lambda j: (0, j)),
        out_shape=jax.ShapeDtypeStruct((width, height), rows.dtype),
        cost_estimate=pl.CostEstimate(
            flops=0, bytes_accessed=4 * height * width, transcendentals=0
        ),
        name="turn",
    )(rows)


def general_body(
    hidden, positions, key_cache, value_cache, norm_gain, q_proj, k_proj, v_proj, o_proj, post_gain
):
    tp_count = lax.axis_size("tp")
    replica_count = lax.axis_size("rep")
    per_tp = replica_count // tp_count
    model_width = hidden.shape[1]
    q_rows, k_rows = q_proj.shape[0], k_proj.shape[0]

    groups = [[i + per_tp * p for p in range(tp_count)] for i in range(per_tp)]
    shifts = [
        [
            (per_tp * p + (i + d) % per_tp, per_tp * p + i)
            for p in range(tp_count)
            for i in range(per_tp)
        ]
        for d in range(1, per_tp)
    ]

    def collect(rows):
        planes = lax.all_gather(rows[None], "rep", axis=0, tiled=True, axis_index_groups=groups)
        return lax.all_to_all(planes, "tp", split_axis=0, concat_axis=0, tiled=True)

    kv_rows = collect(jnp.concatenate([k_proj, v_proj], axis=0))
    split_cols = o_proj.reshape(o_proj.shape[0], tp_count, -1)
    rows_of_group = lax.all_to_all(split_cols, "tp", split_axis=1, concat_axis=0, tiled=True)

    batch, kv_local, length, head_dim = key_cache.shape

    def scatter_rows(values):
        wide = values.reshape(replica_count, batch, -1)
        by_rep = lax.all_to_all(wide, "rep", split_axis=0, concat_axis=0, tiled=True)
        return by_rep

    def to_block(by_rep):
        arrived = lax.all_to_all(by_rep, "tp", split_axis=0, concat_axis=0, tiled=True)
        arrived = arrived.reshape(tp_count, per_tp, batch, -1)
        return jnp.transpose(arrived, (2, 1, 0, 3))

    normed = rms_scale(hidden.astype(jnp.float32), norm_gain).astype(jnp.bfloat16)
    normed_all = lax.all_gather(normed, "rep", axis=0, tiled=True)
    contract = (((1,), (1,)), ((), ()))
    local = jnp.concatenate(
        [
            lax.dot_general(normed_all, matrix, contract, preferred_element_type=jnp.float32)
            for matrix in (q_proj, k_proj, v_proj)
        ],
        axis=1,
    )
    block = to_block(scatter_rows(local))
    q_local = tp_count * per_tp * q_rows // head_dim
    group = q_local // kv_local
    query = block[..., :q_rows].reshape(batch, q_local, head_dim)
    keys_new = block[..., q_rows : q_rows + k_rows].reshape(batch, kv_local, head_dim)
    values_new = block[..., q_rows + k_rows :].reshape(batch, kv_local, head_dim)
    query_rot = rotate(query, positions).astype(jnp.bfloat16)
    rotated_keys = rotate(keys_new, positions).astype(jnp.bfloat16)
    values_rot = values_new.astype(jnp.bfloat16)
    grouped_heads = query_rot.reshape(batch, kv_local, group, head_dim)
    scores = (
        jnp.einsum("bkgd,bkld->bkgl", grouped_heads, key_cache, preferred_element_type=jnp.float32)
        * score_scale
    )
    capped = soft_cap * jnp.tanh(scores / soft_cap)
    valid = jnp.arange(length, dtype=jnp.int32)[None, :] < positions[:, None]
    weight_raw = jnp.where(valid[:, None, None, :], jnp.exp(capped), 0.0)
    self_score = (
        jnp.einsum("juzy,juy->juz", grouped_heads, rotated_keys, preferred_element_type=jnp.float32)
        * score_scale
    )
    self_raw = jnp.exp(soft_cap * jnp.tanh(self_score / soft_cap))
    denom = jnp.sum(weight_raw, axis=-1) + self_raw
    weights = (weight_raw / denom[..., None]).astype(jnp.bfloat16)
    self_weight = (self_raw / denom).astype(jnp.bfloat16)
    attention = jnp.einsum(
        "bkgl,bkld->bkgd", weights, value_cache, preferred_element_type=jnp.float32
    )
    attention = (
        attention
        + self_weight.astype(jnp.float32)[..., None] * values_rot.astype(jnp.float32)[:, :, None, :]
    )
    attention = attention.reshape(batch, q_local * head_dim).astype(jnp.bfloat16)
    q_later, attention = lax.optimization_barrier((q_proj, attention))
    q_own = collect(q_later)
    pairs = [(q_own, kv_rows)]
    for shift in shifts:
        pairs.append((lax.ppermute(q_own, "rep", shift), lax.ppermute(kv_rows, "rep", shift)))
    joined_block = join(per_tp, pairs)
    own_all = lax.all_gather(attention, "tp", axis=1, tiled=True)
    attention_all = lax.all_gather(own_all, "rep", axis=0, tiled=True)
    projected = lax.dot_general(
        attention_all, o_proj, contract, preferred_element_type=jnp.float32
    )
    by_rep = scatter_rows(projected)
    share = to_block(by_rep).reshape(batch, -1)
    square = jnp.sum(share * share, axis=1)
    square_all = lax.all_gather(square[None], "tp", axis=0, tiled=True)
    multiplier = lax.rsqrt(jnp.sum(square_all, axis=0) / model_width + 1e-06)
    result = share * multiplier[:, None] * post_gain
    rows_of_group, result = lax.optimization_barrier((rows_of_group, result))
    complete_rows = lax.all_gather(rows_of_group, "rep", axis=0, tiled=True)
    out_block = turn(complete_rows.reshape(model_width, -1))
    return (joined_block, out_block, result.astype(jnp.bfloat16))


def move_kernel(
    sizes,
    q_ref, k_ref, v_ref, o_ref,
    hidden_ref, positions_ref, keys_ref, values_ref, gain_ref, post_ref, freq_ref,
    joined, heads, result,
    stage, q_own, kv_own, o_rows,
    hidden, positions, keys, values, gain, post, freq,
    fresh, q_heads, k_heads, v_heads, attended, far_attended, far_partial, partial, partial_sum, others,
    early_sems, far_sems, share_send, share_recv,
    q_sems, local_sems, kv_sems, rows_send, rows_recv,
    line_send, line_recv, plane_send, plane_recv,
    twin_send, twin_recv, twin_wo_send, twin_wo_recv,
):
    planes, cores, cols, pieces = sizes
    rep, t = lax.axis_index("rep"), lax.axis_index("tp")
    z, c = rep // cores, lax.rem(rep, cores)
    other = 1 - c
    width = q_ref.shape[1]
    deep = width // pieces
    q_rows, k_rows = q_ref.shape[0], k_ref.shape[0]
    o_own = o_ref.shape[0]
    block = cols * cores * o_own
    half = heads.shape[0] // cores
    wo_rows = half // pieces
    moving = 2 * pieces
    total = 3 * pieces
    q_all = cores * cols * q_rows
    k_all = cores * cols * k_rows
    even = lax.rem(t, 2) == 0

    def at(zz, cc, tt):
        return (zz * cores + cc, tt)

    def column(tt, j, cc):
        parity = lax.rem(tt, 2)
        q_at = (cc * cols + tt) * q_rows
        kv_at = q_all + parity * k_all + (cc * cols + tt - parity) * k_rows
        is_q = (j < pieces).astype(jnp.int32)
        return pl.multiple_of(is_q * q_at + (1 - is_q) * kv_at, 128)

    def slot(tt, j, cc):
        row = pl.multiple_of(lax.rem(j, pieces) * deep, 128)
        return joined.at[pl.ds(row, deep), pl.ds(column(tt, j, cc), 128)]

    def wo_slot(zz, j, cc):
        row = pl.multiple_of(cc * half + (j - moving) * wo_rows, 128)
        col = pl.multiple_of(zz * block, 128)
        return heads.at[pl.ds(row, wo_rows), pl.ds(col, block)]

    def remote(src, dst, send, recv, device):
        return pltpu.make_async_remote_copy(
            src_ref=src, dst_ref=dst, send_sem=send, recv_sem=recv,
            device_id=device, device_id_type=MESH,
        )

    def place(zz, to):
        return zz - (zz > to).astype(jnp.int32)

    def line_copy(zz, j, way, to, device):
        return remote(stage.at[zz, j], stage.at[zz, j], line_send.at[way],
                      line_recv.at[place(zz, to), j], device)

    def line_wo_copy(zz, j, way, to, device):
        return remote(wo_slot(zz, j, c), wo_slot(zz, j, c), line_send.at[way],
                      line_recv.at[place(zz, to), j], device)

    def plane_copy(zz, j):
        return remote(stage.at[zz, j], slot(t, j, c), plane_send.at[0],
                      plane_recv.at[j], at(z, c, zz))

    def wait_bytes(view, sem):
        pltpu.make_async_copy(view, view, sem).wait()

    def twin_copy(src, tt, j, cc):
        return remote(src, slot(tt, j, cc), twin_send.at[0], twin_recv.at[0], at(z, other, t))

    def twin_wo_copy(zz, j, cc):
        return remote(wo_slot(zz, j, cc), wo_slot(zz, j, cc), twin_wo_send.at[0],
                      twin_wo_recv.at[zz], at(z, other, t))

    def rows_copy(dc, dt):
        cc, tt = lax.rem(c + dc, cores), lax.rem(t + dt, cols)
        mine = c * cols + t
        src_at = pl.multiple_of((tt * cores + cc) * half, 128)
        dst_at = pl.multiple_of(mine * o_own, 16)
        return remote(o_ref.at[:, pl.ds(src_at, half)], o_rows.at[pl.ds(dst_at, o_own), :],
                      rows_send.at[0], rows_recv.at[0], at(z, cc, tt))

    peers = [(dc, dt) for dc in range(cores) for dt in range(cols) if dc or dt]

    barrier = pltpu.get_barrier_semaphore()
    for dc, dt in peers:
        pl.semaphore_signal(
            barrier, inc=1, device_id=at(z, lax.rem(c + dc, cores), lax.rem(t + dt, cols)),
            device_id_type=MESH)

    @pl.when(z > 0)
    def _():
        pl.semaphore_signal(barrier, inc=1, device_id=at(z - 1, c, t), device_id_type=MESH)

    @pl.when(z < planes - 1)
    def _():
        pl.semaphore_signal(barrier, inc=1, device_id=at(z + 1, c, t), device_id_type=MESH)

    far_end = jnp.where(2 * z < planes, planes - 1, 0)
    is_end = jnp.logical_or(z == 0, z == planes - 1)

    @pl.when(is_end)
    def _():
        pl.semaphore_signal(barrier, inc=1, device_id=at(far_end, c, t), device_id_type=MESH)

    def load_q(j):
        span = pl.ds(pl.multiple_of(j * deep, 128), deep)
        return pltpu.make_async_copy(q_ref.at[:, span], q_own.at[:, span], q_sems.at[j])

    for j in range(pieces):
        load_q(j).start()
    mine = c * cols + t
    load_o = pltpu.make_async_copy(
        o_ref.at[:, pl.ds(pl.multiple_of((t * cores + c) * half, 128), half)],
        o_rows.at[pl.ds(pl.multiple_of(mine * o_own, 16), o_own), :], local_sems.at[1])
    load_o.start()
    load_k = pltpu.make_async_copy(k_ref, kv_own.at[pl.ds(0, k_rows)], local_sems.at[2])
    load_v = pltpu.make_async_copy(v_ref, kv_own.at[pl.ds(k_rows, k_rows)], local_sems.at[2])

    @pl.when(even)
    def _():
        load_k.start()

    @pl.when(jnp.logical_not(even))
    def _():
        load_v.start()

    give_v = remote(v_ref, kv_own.at[pl.ds(0, k_rows)], kv_sems.at[0], kv_sems.at[1], at(z, c, t + 1 - 2 * lax.rem(t, 2)))
    give_k = remote(k_ref, kv_own.at[pl.ds(k_rows, k_rows)], kv_sems.at[0], kv_sems.at[1], at(z, c, t + 1 - 2 * lax.rem(t, 2)))

    early = [
        pltpu.make_async_copy(source, target, early_sems.at[i])
        for i, (source, target) in enumerate((
            (hidden_ref, hidden), (positions_ref, positions), (gain_ref, gain), (post_ref, post),
            (freq_ref, freq), (keys_ref, keys), (values_ref, values)))
    ]

    batch, kv_local, length, head_dim = keys_ref.shape
    q_local = q_all // head_dim
    group = q_local // kv_local
    f32, bf16 = jnp.float32, jnp.bfloat16

    def project():
        for copy in early[:5]:
            copy.wait()
        wide = hidden[...].astype(f32)
        mean_square = jnp.mean(wide * wide, axis=-1, keepdims=True)
        normed = (wide * lax.rsqrt(mean_square + 1e-06) * gain[...].reshape(1, -1)).astype(bf16)

        def columns(i, carry):
            span = pl.ds(pl.multiple_of(i * 256, 256), 256)
            fresh[:, span] = jnp.dot(normed, joined[:, span], preferred_element_type=f32)
            return carry

        lax.fori_loop(0, fresh.shape[1] // 256, columns, 0)
        angle = jnp.concatenate(
            [positions[b].astype(f32) * freq[...] for b in range(batch)], axis=0)
        cosine, sine = jnp.cos(angle), jnp.sin(angle)
        lane = lax.broadcasted_iota(jnp.int32, angle.shape, 1)
        sine = jnp.where(lane < head_dim // 2, -sine, sine)

        def turned(start):
            x = fresh[:, start : start + head_dim]
            swapped = pltpu.roll(x, head_dim // 2, 1)
            return (x * cosine + swapped * sine).astype(bf16).astype(f32)

        for h in range(kv_local):
            key = turned(q_all + h * head_dim)
            at_v = q_all + k_all + h * head_dim
            value = fresh[:, at_v : at_v + head_dim].astype(bf16).astype(f32)
            for g in range(group):
                n = h * group + g
                query = turned(n * head_dim)
                for b in range(batch):
                    q_heads[b, n : n + 1, :] = query[b : b + 1]
                    k_heads[b, n : n + 1, :] = key[b : b + 1]
                    v_heads[b, n : n + 1, :] = value[b : b + 1]

    def attend():
        for copy in early[5:]:
            copy.wait()
        over = (((1,), (1,)), ((), ()))
        slots = lax.broadcasted_iota(jnp.int32, (q_local, length), 1)
        owner = lax.broadcasted_iota(jnp.int32, (q_local, 1), 0) // group
        for b in range(batch):
            query = q_heads[b]
            narrow = query.astype(bf16)
            scores = jnp.zeros((q_local, length), f32)
            for h in range(kv_local):
                one = lax.dot_general(narrow, keys[b, h], over, preferred_element_type=f32)
                scores = jnp.where(owner == h, one, scores)
            raw = jnp.exp(soft_cap * jnp.tanh(scores * score_scale / soft_cap))
            raw = jnp.where(slots < positions[b], raw, 0.0)
            self_score = jnp.sum(query * k_heads[b], axis=-1, keepdims=True) * score_scale
            self_raw = jnp.exp(soft_cap * jnp.tanh(self_score / soft_cap))
            denom = jnp.sum(raw, axis=-1, keepdims=True) + self_raw
            weights = (raw / denom).astype(bf16)
            self_weight = (self_raw / denom).astype(bf16).astype(f32)
            mixed = jnp.zeros((q_local, head_dim), f32)
            for h in range(kv_local):
                one = jnp.dot(weights, values[b, h], preferred_element_type=f32)
                mixed = jnp.where(owner == h, one, mixed)
            mixed = mixed + self_weight * v_heads[b]
            for n in range(q_local):
                attended[b : b + 1, n * head_dim : (n + 1) * head_dim] = mixed[n : n + 1]

    def share_copy(zz, dt):
        p = lax.rem(t + dt, cols)
        return remote(partial.at[zz], others.at[zz, t], share_send.at[0], share_recv.at[zz], at(z, c, p))

    def take_heads(zz):
        row = pl.multiple_of(other * half, 128)
        col = pl.multiple_of(zz * block, 128)
        wait_bytes(heads.at[pl.ds(row, half), pl.ds(col, block)], twin_wo_recv.at[zz])

    def project_slice(source, zz):
        span = pl.ds(pl.multiple_of(zz * block, 128), block)
        return jnp.dot(source[...].astype(bf16), heads[:, span], preferred_element_type=f32)

    def answer_far():
        ask_far.wait_recv()
        take_heads(z)
        far_partial[...] = project_slice(far_attended, z)
        tell_far.start()
        partial[z] = project_slice(attended, z)
        share_out(z)

    def share_out(zz):
        for dt in range(1, cols):
            share_copy(zz, dt).start()

    def add_slice(zz):
        take_heads(zz)
        partial[zz] = project_slice(attended, zz)
        share_out(zz)

    ask_far = remote(attended, far_attended, far_sems.at[0], far_sems.at[1], at(far_end, c, t))
    tell_far = remote(far_partial, partial.at[z], far_sems.at[2], far_sems.at[3], at(far_end, c, t))

    def sum_slice(zz):
        share = partial[zz]
        wait_bytes(others.at[0, pl.ds(0, cols - 1)], share_recv.at[zz])
        for dt in range(1, cols):
            share = share + others[zz, lax.rem(t + dt, cols)]
        partial_sum[zz] = share
        return jnp.sum(share * share, axis=-1, keepdims=True)

    def near(step):
        return lax.rem(far_end + 1 + step, planes)

    def finish():
        square = jnp.zeros((batch, 1), f32)
        for step in range(planes - 1):
            square = square + sum_slice(near(step))
        square = square + sum_slice(far_end)
        multiplier = lax.rsqrt(square / width + 1e-06)
        result[...] = (partial_sum[t] * multiplier * post[...].reshape(1, -1)).astype(result.dtype)
        wait_bytes(others.at[pl.ds(0, cols - 1)], share_send.at[0])

    def prepare(j):
        @pl.when(j < pieces)
        def _():
            load_q(j).wait()
            span = pl.ds(pl.multiple_of(j * deep, 128), deep)
            stage[z, j] = jnp.transpose(q_own[:, span])

        @pl.when(j == pieces)
        def _():
            @pl.when(even)
            def _():
                load_k.wait()
                give_k.wait_recv()

            @pl.when(jnp.logical_not(even))
            def _():
                load_v.wait()
                give_v.wait_recv()

        @pl.when(jnp.logical_and(j >= pieces, j < moving))
        def _():
            span = pl.ds(pl.multiple_of((j - pieces) * deep, 128), deep)
            stage[z, j] = jnp.transpose(kv_own[:, span])

        @pl.when(j == moving)
        def _():
            load_o.wait()
            wait_bytes(o_rows.at[pl.ds(0, len(peers) * o_own)], rows_recv.at[0])

        @pl.when(jnp.logical_and(j >= moving, j < total))
        def _():
            col = pl.multiple_of((j - moving) * wo_rows, 128)
            row = pl.multiple_of(c * half + (j - moving) * wo_rows, 128)
            heads[pl.ds(row, wo_rows), pl.ds(pl.multiple_of(z * block, 128), block)] = jnp.transpose(
                o_rows[:, pl.ds(col, wo_rows)])

    def send_line(zz, j, way):
        to = z - 1 if way == 0 else z + 1
        target = at(to, c, t)
        room = z > 0 if way == 0 else z < planes - 1

        @pl.when(jnp.logical_and(room, j < moving))
        def _():
            line_copy(zz, j, way, to, target).start()

        @pl.when(jnp.logical_and(room, j >= moving))
        def _():
            line_wo_copy(zz, j, way, to, target).start()

    def wait_line(zz, j):
        @pl.when(j < moving)
        def _():
            line_copy(zz, j, 0, z, at(z, other, t)).wait_recv()

        @pl.when(j >= moving)
        def _():
            line_wo_copy(zz, j, 0, z, at(z, other, t)).wait_recv()

    def deliver(zz, j):
        @pl.when(jnp.logical_and(j < moving, t != zz))
        def _():
            plane_copy(zz, j).start()

        @pl.when(jnp.logical_and(j < moving, t == zz))
        def _():
            row = pl.multiple_of(lax.rem(j, pieces) * deep, 128)
            joined[pl.ds(row, deep), pl.ds(column(t, j, c), 128)] = stage[zz, j]
            twin_copy(stage.at[zz, j], t, j, c).start()

        @pl.when(j >= moving)
        def _():
            twin_wo_copy(zz, j, c).start()

    for copy in early[:5]:
        copy.start()
    prepare(jnp.int32(0))
    n_line = (z > 0).astype(jnp.int32) + (z < planes - 1).astype(jnp.int32) + is_end.astype(jnp.int32)
    pl.semaphore_wait(barrier, len(peers) + n_line)

    def rounds(r, carry):
        @pl.when(r < total)
        def _():
            send_line(z, r, 0)
            send_line(z, r, 1)
            deliver(z, r)

        @pl.when(r == 0)
        def _():
            @pl.when(even)
            def _():
                give_v.start()

            @pl.when(jnp.logical_not(even))
            def _():
                give_k.start()

        @pl.when(r == 3)
        def _():
            for dc, dt in peers:
                rows_copy(dc, dt).start()
            for copy in early[5:]:
                copy.start()

        @pl.when(r + 1 < total)
        def _():
            prepare(r + 1)

        for k in range(1, planes):
            if k == planes - 1:
                pl.when(jnp.logical_and(is_end, r == total + planes - 3))(answer_far)
            for way in (0, 1):
                zz = z + k if way == 0 else z - k
                j = r - k
                inside = zz < planes if way == 0 else zz >= 0

                @pl.when(jnp.logical_and(inside, jnp.logical_and(j >= 0, j < total)))
                def _():
                    wait_line(zz, j)
                    send_line(zz, j, way)
                    deliver(zz, j)

        far = jnp.where(z > t, z - t, t - z)
        j = r - far - 1

        @pl.when(jnp.logical_and(j >= 0, j < moving))
        def _():
            wait_bytes(stage.at[0, pl.ds(0, cols - 1)], plane_recv.at[j])
            for dt in range(1, cols):
                tt = lax.rem(t + dt, cols)
                twin_copy(slot(tt, j, c), tt, j, c).start()

        @pl.when(r == moving + 1 + far)
        def _():
            wait_bytes(joined.at[pl.ds(0, width // cores)], twin_recv.at[0])
            project()
            attend()

            @pl.when(is_end)
            def _():
                ask_far.start()

        return carry

    lax.fori_loop(0, total + planes - 2, rounds, 0)

    @pl.when(is_end)
    def _():
        for k in range(1, planes - 1):
            add_slice(jnp.where(z == 0, k, planes - 1 - k))
        remote(partial.at[far_end], partial.at[far_end], far_sems.at[2], far_sems.at[3],
               at(far_end, c, t)).wait_recv()
        share_out(far_end)

    rounds(jnp.int32(total + planes - 2), 0)

    @pl.when(jnp.logical_not(is_end))
    def _():
        for zz in range(planes):
            add_slice(zz)

    finish()

    @pl.when(is_end)
    def _():
        take_heads(far_end)
        ask_far.wait_send()
        tell_far.wait_send()

    unit = deep * 128 // joined.shape[1]
    for way, count in ((0, planes - z), (1, z + 1)):
        for m in range(1, planes):

            @pl.when(count == m)
            def _():
                wait_bytes(joined.at[pl.ds(0, m * total * unit)], line_send.at[way])
    wait_bytes(joined.at[pl.ds(0, (planes - 1) * moving * unit)], plane_send.at[0])
    wait_bytes(joined.at[pl.ds(0, width // cores)], twin_send.at[0])
    wait_bytes(heads.at[pl.ds(0, half)], twin_wo_send.at[0])
    wait_bytes(o_rows.at[pl.ds(0, len(peers) * o_own)], rows_send.at[0])

    @pl.when(even)
    def _():
        give_v.wait_send()

    @pl.when(jnp.logical_not(even))
    def _():
        give_k.wait_send()


def line_body(hidden, positions, key_cache, value_cache, norm_gain, q_proj, k_proj, v_proj, o_proj, post_gain):
    cols = lax.axis_size("tp")
    cores = 2
    planes = lax.axis_size("rep") // cores
    pieces = 4
    width = q_proj.shape[1]
    deep = width // pieces
    q_rows, k_rows, o_own = q_proj.shape[0], k_proj.shape[0], o_proj.shape[0]
    features = o_proj.shape[1] // cols
    columns = cores * cols * (q_rows + 2 * k_rows)
    model = o_own * cores * cols * planes
    bf = jnp.bfloat16
    dma = pltpu.SemaphoreType.DMA
    hbm = pl.BlockSpec(memory_space=pltpu.HBM)
    f32 = jnp.float32
    batch, kv_local, length, head_dim = key_cache.shape
    q_local = cores * cols * q_rows // head_dim
    half = head_dim // 2
    freq = 10000.0 ** (-2.0 * np.arange(half) / head_dim)
    freq = jnp.asarray(np.concatenate([freq, freq])[None], f32)
    share = post_gain.shape[0]
    moving, total = 2 * pieces, 3 * pieces
    out = pl.pallas_call(
        functools.partial(move_kernel, (planes, cores, cols, pieces)),
        in_specs=[hbm] * 11,
        out_shape=[
            pltpu.VMEM((width, columns), bf),
            pltpu.VMEM((features, model), bf),
            pltpu.VMEM((hidden.shape[0], post_gain.shape[0]), bf),
        ],
        out_specs=[pl.BlockSpec(memory_space=pltpu.VMEM)] * 3,
        scratch_shapes=[
            pltpu.VMEM((planes, moving, deep, 128), bf),
            pltpu.VMEM((q_rows, width), bf),
            pltpu.VMEM((2 * k_rows, width), bf),
            pltpu.VMEM((cores * cols * o_own, features // cores), bf),
            pltpu.VMEM(hidden.shape, bf), pltpu.SMEM(positions.shape, jnp.int32),
            pltpu.VMEM(key_cache.shape, bf), pltpu.VMEM(value_cache.shape, bf),
            pltpu.VMEM((width,), f32), pltpu.VMEM((share,), f32), pltpu.VMEM((1, head_dim), f32),
            pltpu.VMEM((batch, columns), f32), pltpu.VMEM((batch, q_local, head_dim), f32),
            pltpu.VMEM((batch, q_local, head_dim), f32), pltpu.VMEM((batch, q_local, head_dim), f32),
            pltpu.VMEM((batch, features), f32), pltpu.VMEM((batch, features), f32),
            pltpu.VMEM((batch, share), f32), pltpu.VMEM((planes, batch, share), f32),
            pltpu.VMEM((planes, batch, share), f32), pltpu.VMEM((planes, cols, batch, share), f32),
            dma((7,)), dma((4,)), dma((1,)), dma((planes,)),
            dma((pieces,)), dma((3,)), dma((2,)), dma((1,)), dma((1,)),
            dma((2,)), dma((planes - 1, total)), dma((1,)), dma((moving,)),
            dma((1,)), dma((1,)), dma((1,)), dma((planes,)),
        ],
        compiler_params=pltpu.CompilerParams(
            collective_id=0, has_side_effects=True, vmem_limit_bytes=34 * 2**20),
        name="move",
    )(q_proj, k_proj, v_proj, o_proj, hidden, positions, key_cache, value_cache,
      norm_gain, post_gain, freq)
    joined, heads, result = out

    def spill_kernel(a, b, r, a_out, b_out, r_out, sems):
        small = pltpu.make_async_copy(r, r_out, sems.at[0])
        small.start()
        for i, (source, target) in enumerate(((a, a_out), (b, b_out))):
            rows = 32 * source.dtype.itemsize
            for low in range(0, source.shape[0], rows):
                span = pl.ds(low, min(rows, source.shape[0] - low))
                pltpu.make_async_copy(source.at[span], target.at[span], sems.at[i + 1]).start()
        small.wait()
        for i, (source, target) in enumerate(((a, a_out), (b, b_out))):
            pltpu.make_async_copy(source, target, sems.at[i + 1]).wait()

    vmem = pl.BlockSpec(memory_space=pltpu.VMEM)
    return tuple(pl.pallas_call(
        spill_kernel,
        in_specs=[vmem] * 3,
        out_specs=[hbm] * 3,
        out_shape=[jax.ShapeDtypeStruct(x.shape, x.dtype) for x in (joined, heads, result)],
        scratch_shapes=[dma((3,))],
        compiler_params=pltpu.CompilerParams(vmem_limit_bytes=2**20),
        name="spill",
    )(joined, heads, result))


def body(*args):
    cols, reps = lax.axis_size("tp"), lax.axis_size("rep")
    key_cache, q_proj, k_proj, o_proj = args[2], args[5], args[6], args[8]
    lanes = 128
    fits = (
        reps == 2 * cols
        and cols % 2 == 0
        and cols > 2
        and key_cache.shape[3] == lanes
        and q_proj.shape[0] == lanes
        and 2 * k_proj.shape[0] == lanes
        and o_proj.shape[0] % 16 == 0
        and q_proj.shape[1] % (4 * lanes) == 0
        and o_proj.shape[1] % (8 * lanes * cols) == 0
        and (2 * cols * o_proj.shape[0]) % lanes == 0
    )
    return (line_body if fits else general_body)(*args)


def solution(mesh):
    in_specs = (
        P("rep", None), P("rep"), P("rep", "tp", None, None), P("rep", "tp", None, None), P(),
        P(("rep", "tp"), None), P(("rep", "tp"), None), P(("rep", "tp"), None), P(("rep", "tp"), None), P("tp"),
    )
    out_specs = (P(None, "tp"), P("tp", None), P("rep", "tp"))
    return jax.shard_map(body, mesh=mesh, in_specs=in_specs, out_specs=out_specs, check_vma=False)
```

```python
import functools

import jax
import jax.numpy as jnp
import numpy as np
from jax import lax
from jax.experimental import pallas as pl
from jax.experimental.pallas import tpu as pltpu
from jax.sharding import PartitionSpec as P

MESH = pl.DeviceIdType.MESH
score_scale = 144.0 ** (-0.5)
soft_cap = 50.0


def rms_scale(values, gain):
    mean_square = jnp.mean(values * values, axis=-1, keepdims=True)
    return values * lax.rsqrt(mean_square + 1e-06) * gain


def rotate(values, positions):
    half = values.shape[-1] // 2
    freq = 10000.0 ** (-2.0 * jnp.arange(half, dtype=jnp.float32) / values.shape[-1])
    angle = positions.astype(jnp.float32)[:, None] * freq[None, :]
    cosine = jnp.cos(angle)[:, None, :]
    sine = jnp.sin(angle)[:, None, :]
    first = values[..., :half]
    second = values[..., half:]
    return jnp.concatenate(
        [first * cosine - second * sine, second * cosine + first * sine], axis=-1
    )


def join_kernel(per_tp, q_rows, k_rows, *refs):
    slot = lax.rem(lax.axis_index("rep"), per_tp)
    parts, out_ref = refs[:-1], refs[-1]
    tp_count = parts[0].shape[0]
    q_all = tp_count * per_tp * q_rows
    k_all = tp_count * per_tp * k_rows
    for step in range(per_tp):
        who = lax.rem(slot + step, per_tp)
        q_ref, kv_ref = parts[2 * step], parts[2 * step + 1]
        for start, ref, low, rows in (
            (0, q_ref, 0, q_rows),
            (q_all, kv_ref, 0, k_rows),
            (q_all + k_all, kv_ref, k_rows, k_rows),
        ):
            block = ref[:, low : low + rows, :].reshape(tp_count * rows, -1)
            at = pl.multiple_of(start + who * (tp_count * rows), 128)
            out_ref[:, pl.ds(at, tp_count * rows)] = jnp.transpose(block)


def join(per_tp, pairs):
    tp_count, q_rows, width = pairs[0][0].shape
    k_rows = pairs[0][1].shape[1] // 2
    columns = tp_count * per_tp * (q_rows + 2 * k_rows)
    stripe = 256
    operands, specs = [], []
    for pair in pairs:
        for matrix in pair:
            operands.append(matrix)
            specs.append(
                pl.BlockSpec((tp_count, matrix.shape[1], stripe), lambda j: (0, 0, j))
            )
    size = width * columns * 2
    return pl.pallas_call(
        functools.partial(join_kernel, per_tp, q_rows, k_rows),
        grid=(width // stripe,),
        in_specs=specs,
        out_specs=pl.BlockSpec((stripe, columns), lambda j: (j, 0)),
        out_shape=jax.ShapeDtypeStruct((width, columns), jnp.bfloat16),
        cost_estimate=pl.CostEstimate(flops=0, bytes_accessed=2 * size, transcendentals=0),
        name="join",
    )(*operands)


def turn_kernel(rows_ref, out_ref):
    out_ref[...] = jnp.transpose(rows_ref[...])


def turn(rows):
    height, width = rows.shape
    stripe = 384 if height % 384 == 0 else 128
    return pl.pallas_call(
        turn_kernel,
        grid=(height // stripe,),
        in_specs=[pl.BlockSpec((stripe, width), lambda j: (j, 0))],
        out_specs=pl.BlockSpec((width, stripe), lambda j: (0, j)),
        out_shape=jax.ShapeDtypeStruct((width, height), rows.dtype),
        cost_estimate=pl.CostEstimate(
            flops=0, bytes_accessed=4 * height * width, transcendentals=0
        ),
        name="turn",
    )(rows)


def general_body(
    hidden, positions, key_cache, value_cache, norm_gain, q_proj, k_proj, v_proj, o_proj, post_gain
):
    tp_count = lax.axis_size("tp")
    replica_count = lax.axis_size("rep")
    per_tp = replica_count // tp_count
    model_width = hidden.shape[1]
    q_rows, k_rows = q_proj.shape[0], k_proj.shape[0]

    groups = [[i + per_tp * p for p in range(tp_count)] for i in range(per_tp)]
    shifts = [
        [
            (per_tp * p + (i + d) % per_tp, per_tp * p + i)
            for p in range(tp_count)
            for i in range(per_tp)
        ]
        for d in range(1, per_tp)
    ]

    def collect(rows):
        planes = lax.all_gather(rows[None], "rep", axis=0, tiled=True, axis_index_groups=groups)
        return lax.all_to_all(planes, "tp", split_axis=0, concat_axis=0, tiled=True)

    kv_rows = collect(jnp.concatenate([k_proj, v_proj], axis=0))
    split_cols = o_proj.reshape(o_proj.shape[0], tp_count, -1)
    rows_of_group = lax.all_to_all(split_cols, "tp", split_axis=1, concat_axis=0, tiled=True)

    batch, kv_local, length, head_dim = key_cache.shape

    def scatter_rows(values):
        wide = values.reshape(replica_count, batch, -1)
        by_rep = lax.all_to_all(wide, "rep", split_axis=0, concat_axis=0, tiled=True)
        return by_rep

    def to_block(by_rep):
        arrived = lax.all_to_all(by_rep, "tp", split_axis=0, concat_axis=0, tiled=True)
        arrived = arrived.reshape(tp_count, per_tp, batch, -1)
        return jnp.transpose(arrived, (2, 1, 0, 3))

    normed = rms_scale(hidden.astype(jnp.float32), norm_gain).astype(jnp.bfloat16)
    normed_all = lax.all_gather(normed, "rep", axis=0, tiled=True)
    contract = (((1,), (1,)), ((), ()))
    local = jnp.concatenate(
        [
            lax.dot_general(normed_all, matrix, contract, preferred_element_type=jnp.float32)
            for matrix in (q_proj, k_proj, v_proj)
        ],
        axis=1,
    )
    block = to_block(scatter_rows(local))
    q_local = tp_count * per_tp * q_rows // head_dim
    group = q_local // kv_local
    query = block[..., :q_rows].reshape(batch, q_local, head_dim)
    keys_new = block[..., q_rows : q_rows + k_rows].reshape(batch, kv_local, head_dim)
    values_new = block[..., q_rows + k_rows :].reshape(batch, kv_local, head_dim)
    query_rot = rotate(query, positions).astype(jnp.bfloat16)
    rotated_keys = rotate(keys_new, positions).astype(jnp.bfloat16)
    values_rot = values_new.astype(jnp.bfloat16)
    grouped_heads = query_rot.reshape(batch, kv_local, group, head_dim)
    scores = (
        jnp.einsum("bkgd,bkld->bkgl", grouped_heads, key_cache, preferred_element_type=jnp.float32)
        * score_scale
    )
    capped = soft_cap * jnp.tanh(scores / soft_cap)
    valid = jnp.arange(length, dtype=jnp.int32)[None, :] < positions[:, None]
    weight_raw = jnp.where(valid[:, None, None, :], jnp.exp(capped), 0.0)
    self_score = (
        jnp.einsum("juzy,juy->juz", grouped_heads, rotated_keys, preferred_element_type=jnp.float32)
        * score_scale
    )
    self_raw = jnp.exp(soft_cap * jnp.tanh(self_score / soft_cap))
    denom = jnp.sum(weight_raw, axis=-1) + self_raw
    weights = (weight_raw / denom[..., None]).astype(jnp.bfloat16)
    self_weight = (self_raw / denom).astype(jnp.bfloat16)
    attention = jnp.einsum(
        "bkgl,bkld->bkgd", weights, value_cache, preferred_element_type=jnp.float32
    )
    attention = (
        attention
        + self_weight.astype(jnp.float32)[..., None] * values_rot.astype(jnp.float32)[:, :, None, :]
    )
    attention = attention.reshape(batch, q_local * head_dim).astype(jnp.bfloat16)
    q_later, attention = lax.optimization_barrier((q_proj, attention))
    q_own = collect(q_later)
    pairs = [(q_own, kv_rows)]
    for shift in shifts:
        pairs.append((lax.ppermute(q_own, "rep", shift), lax.ppermute(kv_rows, "rep", shift)))
    joined_block = join(per_tp, pairs)
    own_all = lax.all_gather(attention, "tp", axis=1, tiled=True)
    attention_all = lax.all_gather(own_all, "rep", axis=0, tiled=True)
    projected = lax.dot_general(
        attention_all, o_proj, contract, preferred_element_type=jnp.float32
    )
    by_rep = scatter_rows(projected)
    share = to_block(by_rep).reshape(batch, -1)
    square = jnp.sum(share * share, axis=1)
    square_all = lax.all_gather(square[None], "tp", axis=0, tiled=True)
    multiplier = lax.rsqrt(jnp.sum(square_all, axis=0) / model_width + 1e-06)
    result = share * multiplier[:, None] * post_gain
    rows_of_group, result = lax.optimization_barrier((rows_of_group, result))
    complete_rows = lax.all_gather(rows_of_group, "rep", axis=0, tiled=True)
    out_block = turn(complete_rows.reshape(model_width, -1))
    return (joined_block, out_block, result.astype(jnp.bfloat16))


def move_kernel(
    sizes,
    q_ref, k_ref, v_ref, o_ref,
    hidden_ref, positions_ref, keys_ref, values_ref, gain_ref, post_ref, freq_ref,
    joined, heads, result,
    stage, q_own, kv_own, o_rows,
    hidden, positions, keys, values, gain, post, freq,
    fresh, q_heads, k_heads, v_heads, attended, far_attended, far_partial, partial, partial_sum, others,
    early_sems, far_sems, share_send, share_recv,
    tail_sems, q_sems, local_sems, kv_sems, rows_send, rows_recv,
    line_send, line_recv, plane_send, plane_recv,
    twin_send, twin_recv, twin_wo_send, twin_wo_recv,
):
    planes, cores, cols, pieces = sizes
    rep, t = lax.axis_index("rep"), lax.axis_index("tp")
    z, c = rep // cores, lax.rem(rep, cores)
    other = 1 - c
    width = q_ref.shape[1]
    deep = width // pieces
    q_rows, k_rows = q_ref.shape[0], k_ref.shape[0]
    o_own = o_ref.shape[0]
    block = cols * cores * o_own
    half = heads.shape[0] // cores
    wo_rows = half // pieces
    tail_rows = 16
    main_rows = wo_rows - tail_rows
    moving = 2 * pieces
    total = 3 * pieces
    q_all = cores * cols * q_rows
    k_all = cores * cols * k_rows
    even = lax.rem(t, 2) == 0

    def at(zz, cc, tt):
        return (zz * cores + cc, tt)

    def column(tt, j, cc):
        parity = lax.rem(tt, 2)
        q_at = (cc * cols + tt) * q_rows
        kv_at = q_all + parity * k_all + (cc * cols + tt - parity) * k_rows
        is_q = (j < pieces).astype(jnp.int32)
        return pl.multiple_of(is_q * q_at + (1 - is_q) * kv_at, 128)

    def slot(tt, j, cc):
        row = pl.multiple_of(lax.rem(j, pieces) * deep, 128)
        return joined.at[pl.ds(row, deep), pl.ds(column(tt, j, cc), 128)]

    def wo_slot(zz, j, cc):
        row = pl.multiple_of(cc * half + (j - moving) * wo_rows, 128)
        col = pl.multiple_of(zz * block, 128)
        return heads.at[pl.ds(row, wo_rows), pl.ds(col, block)]

    def remote(src, dst, send, recv, device):
        return pltpu.make_async_remote_copy(
            src_ref=src, dst_ref=dst, send_sem=send, recv_sem=recv,
            device_id=device, device_id_type=MESH,
        )

    def place(zz, to):
        return zz - (zz > to).astype(jnp.int32)

    def line_copy(zz, j, way, to, device):
        return remote(stage.at[zz, j], stage.at[zz, j], line_send.at[way],
                      line_recv.at[place(zz, to), j], device)

    def line_wo_copy(zz, j, way, to, device):
        return remote(wo_slot(zz, j, c), wo_slot(zz, j, c), line_send.at[way],
                      line_recv.at[place(zz, to), j], device)

    def plane_copy(zz, j):
        return remote(stage.at[zz, j], slot(t, j, c), plane_send.at[0],
                      plane_recv.at[j], at(z, c, zz))

    def wait_bytes(view, sem):
        pltpu.make_async_copy(view, view, sem).wait()

    def twin_copy(src, tt, j, cc):
        return remote(src, slot(tt, j, cc), twin_send.at[0], twin_recv.at[0], at(z, other, t))

    def twin_wo_copy(zz, j, cc):
        return remote(wo_slot(zz, j, cc), wo_slot(zz, j, cc), twin_wo_send.at[0],
                      twin_wo_recv.at[zz], at(z, other, t))

    def part(zz, cc, low, rows):
        row = pl.multiple_of(cc * half + (pieces - 1) * wo_rows + low, 16)
        return heads.at[pl.ds(row, rows), pl.ds(pl.multiple_of(zz * block, 128), block)]

    def main_line(zz, way, to, device):
        view = part(zz, c, 0, main_rows)
        return remote(view, view, line_send.at[way], line_recv.at[place(zz, to), total - 1], device)

    def tail_line(zz, way, to):
        view = part(zz, c, main_rows, tail_rows)
        return (remote(view, view, line_send.at[way], tail_sems.at[0], at(to, c, t)),
                remote(view, view, tail_sems.at[2], tail_sems.at[1], at(to, other, t)))

    def main_twin(zz):
        view = part(zz, c, 0, main_rows)
        return remote(view, view, tail_sems.at[3], twin_wo_recv.at[zz], at(z, other, t))

    def rows_copy(dc, dt):
        cc, tt = lax.rem(c + dc, cores), lax.rem(t + dt, cols)
        mine = c * cols + t
        src_at = pl.multiple_of((tt * cores + cc) * half, 128)
        dst_at = pl.multiple_of(mine * o_own, 16)
        return remote(o_ref.at[:, pl.ds(src_at, half)], o_rows.at[pl.ds(dst_at, o_own), :],
                      rows_send.at[0], rows_recv.at[0], at(z, cc, tt))

    peers = [(dc, dt) for dc in range(cores) for dt in range(cols) if dc or dt]

    barrier = pltpu.get_barrier_semaphore()
    for dc, dt in peers:
        pl.semaphore_signal(
            barrier, inc=1, device_id=at(z, lax.rem(c + dc, cores), lax.rem(t + dt, cols)),
            device_id_type=MESH)

    @pl.when(z > 0)
    def _():
        pl.semaphore_signal(barrier, inc=1, device_id=at(z - 1, c, t), device_id_type=MESH)

    @pl.when(z < planes - 1)
    def _():
        pl.semaphore_signal(barrier, inc=1, device_id=at(z + 1, c, t), device_id_type=MESH)

    far_end = jnp.where(2 * z < planes, planes - 1, 0)
    is_end = jnp.logical_or(z == 0, z == planes - 1)

    is_next = jnp.logical_or(z == 1, z == planes - 2)

    @pl.when(is_end)
    def _():
        pl.semaphore_signal(barrier, inc=1, device_id=at(far_end, c, t), device_id_type=MESH)
        pl.semaphore_signal(barrier, inc=1, device_id=at(jnp.where(z == 0, 1, planes - 2), 1 - c, t),
                            device_id_type=MESH)

    def load_q(j):
        span = pl.ds(pl.multiple_of(j * deep, 128), deep)
        return pltpu.make_async_copy(q_ref.at[:, span], q_own.at[:, span], q_sems.at[j])

    for j in range(pieces):
        load_q(j).start()
    mine = c * cols + t
    load_o = pltpu.make_async_copy(
        o_ref.at[:, pl.ds(pl.multiple_of((t * cores + c) * half, 128), half)],
        o_rows.at[pl.ds(pl.multiple_of(mine * o_own, 16), o_own), :], local_sems.at[1])
    load_o.start()
    load_k = pltpu.make_async_copy(k_ref, kv_own.at[pl.ds(0, k_rows)], local_sems.at[2])
    load_v = pltpu.make_async_copy(v_ref, kv_own.at[pl.ds(k_rows, k_rows)], local_sems.at[2])

    @pl.when(even)
    def _():
        load_k.start()

    @pl.when(jnp.logical_not(even))
    def _():
        load_v.start()

    give_v = remote(v_ref, kv_own.at[pl.ds(0, k_rows)], kv_sems.at[0], kv_sems.at[1], at(z, c, t + 1 - 2 * lax.rem(t, 2)))
    give_k = remote(k_ref, kv_own.at[pl.ds(k_rows, k_rows)], kv_sems.at[0], kv_sems.at[1], at(z, c, t + 1 - 2 * lax.rem(t, 2)))

    early = [
        pltpu.make_async_copy(source, target, early_sems.at[i])
        for i, (source, target) in enumerate((
            (hidden_ref, hidden), (positions_ref, positions), (gain_ref, gain), (post_ref, post),
            (freq_ref, freq), (keys_ref, keys), (values_ref, values)))
    ]

    batch, kv_local, length, head_dim = keys_ref.shape
    q_local = q_all // head_dim
    group = q_local // kv_local
    f32, bf16 = jnp.float32, jnp.bfloat16

    def project():
        for copy in early[:5]:
            copy.wait()
        wide = hidden[...].astype(f32)
        mean_square = jnp.mean(wide * wide, axis=-1, keepdims=True)
        normed = (wide * lax.rsqrt(mean_square + 1e-06) * gain[...].reshape(1, -1)).astype(bf16)

        def columns(i, carry):
            span = pl.ds(pl.multiple_of(i * 256, 256), 256)
            fresh[:, span] = jnp.dot(normed, joined[:, span], preferred_element_type=f32)
            return carry

        lax.fori_loop(0, fresh.shape[1] // 256, columns, 0)
        angle = jnp.concatenate(
            [positions[b].astype(f32) * freq[...] for b in range(batch)], axis=0)
        cosine, sine = jnp.cos(angle), jnp.sin(angle)
        lane = lax.broadcasted_iota(jnp.int32, angle.shape, 1)
        sine = jnp.where(lane < head_dim // 2, -sine, sine)

        def turned(start):
            x = fresh[:, start : start + head_dim]
            swapped = pltpu.roll(x, head_dim // 2, 1)
            return (x * cosine + swapped * sine).astype(bf16).astype(f32)

        for h in range(kv_local):
            key = turned(q_all + h * head_dim)
            at_v = q_all + k_all + h * head_dim
            value = fresh[:, at_v : at_v + head_dim].astype(bf16).astype(f32)
            for g in range(group):
                n = h * group + g
                query = turned(n * head_dim)
                for b in range(batch):
                    q_heads[b, n : n + 1, :] = query[b : b + 1]
                    k_heads[b, n : n + 1, :] = key[b : b + 1]
                    v_heads[b, n : n + 1, :] = value[b : b + 1]

    def attend():
        for copy in early[5:]:
            copy.wait()
        over = (((1,), (1,)), ((), ()))
        slots = lax.broadcasted_iota(jnp.int32, (q_local, length), 1)
        owner = lax.broadcasted_iota(jnp.int32, (q_local, 1), 0) // group
        for b in range(batch):
            query = q_heads[b]
            narrow = query.astype(bf16)
            scores = jnp.zeros((q_local, length), f32)
            for h in range(kv_local):
                one = lax.dot_general(narrow, keys[b, h], over, preferred_element_type=f32)
                scores = jnp.where(owner == h, one, scores)
            raw = jnp.exp(soft_cap * jnp.tanh(scores * score_scale / soft_cap))
            raw = jnp.where(slots < positions[b], raw, 0.0)
            self_score = jnp.sum(query * k_heads[b], axis=-1, keepdims=True) * score_scale
            self_raw = jnp.exp(soft_cap * jnp.tanh(self_score / soft_cap))
            denom = jnp.sum(raw, axis=-1, keepdims=True) + self_raw
            weights = (raw / denom).astype(bf16)
            self_weight = (self_raw / denom).astype(bf16).astype(f32)
            mixed = jnp.zeros((q_local, head_dim), f32)
            for h in range(kv_local):
                one = jnp.dot(weights, values[b, h], preferred_element_type=f32)
                mixed = jnp.where(owner == h, one, mixed)
            mixed = mixed + self_weight * v_heads[b]
            for n in range(q_local):
                attended[b : b + 1, n * head_dim : (n + 1) * head_dim] = mixed[n : n + 1]

    def share_copy(zz, dt):
        p = lax.rem(t + dt, cols)
        return remote(partial.at[zz], others.at[zz, t], share_send.at[0], share_recv.at[zz], at(z, c, p))

    def take_heads(zz):
        row = pl.multiple_of(other * half, 128)
        col = pl.multiple_of(zz * block, 128)
        wait_bytes(heads.at[pl.ds(row, half), pl.ds(col, block)], twin_wo_recv.at[zz])

    def project_slice(source, zz):
        span = pl.ds(pl.multiple_of(zz * block, 128), block)
        return jnp.dot(source[...].astype(bf16), heads[:, span], preferred_element_type=f32)

    def answer_far():
        ask_far.wait_recv()
        take_heads(z)
        far_partial[...] = project_slice(far_attended, z)
        tell_far.start()
        partial[z] = project_slice(attended, z)
        share_out(z)

    def share_out(zz):
        for dt in range(1, cols):
            share_copy(zz, dt).start()

    def add_slice(zz):
        take_heads(zz)
        partial[zz] = project_slice(attended, zz)
        share_out(zz)

    ask_far = remote(attended, far_attended, far_sems.at[0], far_sems.at[1], at(far_end, c, t))
    tell_far = remote(far_partial, partial.at[z], far_sems.at[2], far_sems.at[3], at(far_end, c, t))

    def sum_slice(zz):
        share = partial[zz]
        wait_bytes(others.at[0, pl.ds(0, cols - 1)], share_recv.at[zz])
        for dt in range(1, cols):
            share = share + others[zz, lax.rem(t + dt, cols)]
        partial_sum[zz] = share
        return jnp.sum(share * share, axis=-1, keepdims=True)

    def near(step):
        return lax.rem(far_end + 1 + step, planes)

    def finish():
        square = jnp.zeros((batch, 1), f32)
        for step in range(planes - 1):
            square = square + sum_slice(near(step))
        square = square + sum_slice(far_end)
        multiplier = lax.rsqrt(square / width + 1e-06)
        result[...] = (partial_sum[t] * multiplier * post[...].reshape(1, -1)).astype(result.dtype)
        wait_bytes(others.at[pl.ds(0, cols - 1)], share_send.at[0])

    def prepare(j):
        @pl.when(j < pieces)
        def _():
            load_q(j).wait()
            span = pl.ds(pl.multiple_of(j * deep, 128), deep)
            stage[z, j] = jnp.transpose(q_own[:, span])

        @pl.when(j == pieces)
        def _():
            @pl.when(even)
            def _():
                load_k.wait()
                give_k.wait_recv()

            @pl.when(jnp.logical_not(even))
            def _():
                load_v.wait()
                give_v.wait_recv()

        @pl.when(jnp.logical_and(j >= pieces, j < moving))
        def _():
            span = pl.ds(pl.multiple_of((j - pieces) * deep, 128), deep)
            stage[z, j] = jnp.transpose(kv_own[:, span])

        @pl.when(j == moving)
        def _():
            load_o.wait()
            wait_bytes(o_rows.at[pl.ds(0, len(peers) * o_own)], rows_recv.at[0])

        @pl.when(jnp.logical_and(j >= moving, j < total))
        def _():
            col = pl.multiple_of((j - moving) * wo_rows, 128)
            row = pl.multiple_of(c * half + (j - moving) * wo_rows, 128)
            heads[pl.ds(row, wo_rows), pl.ds(pl.multiple_of(z * block, 128), block)] = jnp.transpose(
                o_rows[:, pl.ds(col, wo_rows)])

    def send_line(zz, j, way):
        to = z - 1 if way == 0 else z + 1
        target = at(to, c, t)
        room = z > 0 if way == 0 else z < planes - 1

        @pl.when(jnp.logical_and(room, j < moving))
        def _():
            line_copy(zz, j, way, to, target).start()

        ends = jnp.logical_and(j == total - 1, to == 0 if way == 0 else to == planes - 1)
        ends = jnp.logical_and(ends, zz == planes - 1 if way == 0 else zz == 0)

        @pl.when(jnp.logical_and(jnp.logical_and(room, j >= moving), jnp.logical_not(ends)))
        def _():
            line_wo_copy(zz, j, way, to, target).start()

        @pl.when(jnp.logical_and(room, ends))
        def _():
            main_line(zz, way, to, target).start()
            for copy in tail_line(zz, way, to):
                copy.start()

    def wait_line(zz, j):
        @pl.when(j < moving)
        def _():
            line_copy(zz, j, 0, z, at(z, other, t)).wait_recv()

        last = jnp.logical_and(j == total - 1, jnp.logical_and(is_end, zz == far_end))

        @pl.when(jnp.logical_and(j >= moving, jnp.logical_not(last)))
        def _():
            line_wo_copy(zz, j, 0, z, at(z, other, t)).wait_recv()

        @pl.when(last)
        def _():
            main_line(zz, 0, z, at(z, other, t)).wait_recv()

    def deliver(zz, j):
        @pl.when(jnp.logical_and(j < moving, t != zz))
        def _():
            plane_copy(zz, j).start()

        @pl.when(jnp.logical_and(j < moving, t == zz))
        def _():
            row = pl.multiple_of(lax.rem(j, pieces) * deep, 128)
            joined[pl.ds(row, deep), pl.ds(column(t, j, c), 128)] = stage[zz, j]
            twin_copy(stage.at[zz, j], t, j, c).start()

        last = jnp.logical_and(j == total - 1, jnp.logical_and(is_end, zz == far_end))

        @pl.when(jnp.logical_and(j >= moving, jnp.logical_not(last)))
        def _():
            twin_wo_copy(zz, j, c).start()

        @pl.when(last)
        def _():
            main_twin(zz).start()

    for copy in early[:5]:
        copy.start()
    prepare(jnp.int32(0))
    n_line = (z > 0).astype(jnp.int32) + (z < planes - 1).astype(jnp.int32) + is_end.astype(jnp.int32) + is_next.astype(jnp.int32)
    pl.semaphore_wait(barrier, len(peers) + n_line)

    def rounds(r, carry):
        @pl.when(r < total)
        def _():
            send_line(z, r, 0)
            send_line(z, r, 1)
            deliver(z, r)

        @pl.when(r == 0)
        def _():
            @pl.when(even)
            def _():
                give_v.start()

            @pl.when(jnp.logical_not(even))
            def _():
                give_k.start()

        @pl.when(r == 3)
        def _():
            for dc, dt in peers:
                rows_copy(dc, dt).start()
            for copy in early[5:]:
                copy.start()

        @pl.when(r + 1 < total)
        def _():
            prepare(r + 1)

        for k in range(1, planes):
            if k == planes - 1:
                pl.when(jnp.logical_and(is_end, r == total + planes - 3))(answer_far)
            for way in (0, 1):
                zz = z + k if way == 0 else z - k
                j = r - k
                inside = zz < planes if way == 0 else zz >= 0

                @pl.when(jnp.logical_and(inside, jnp.logical_and(j >= 0, j < total)))
                def _():
                    wait_line(zz, j)
                    send_line(zz, j, way)
                    deliver(zz, j)

        far = jnp.where(z > t, z - t, t - z)
        j = r - far - 1

        @pl.when(jnp.logical_and(j >= 0, j < moving))
        def _():
            wait_bytes(stage.at[0, pl.ds(0, cols - 1)], plane_recv.at[j])
            for dt in range(1, cols):
                tt = lax.rem(t + dt, cols)
                twin_copy(slot(tt, j, c), tt, j, c).start()

        @pl.when(r == moving + 1 + far)
        def _():
            wait_bytes(joined.at[pl.ds(0, width // cores)], twin_recv.at[0])
            project()
            attend()

            @pl.when(is_end)
            def _():
                ask_far.start()

        return carry

    lax.fori_loop(0, total + planes - 2, rounds, 0)

    @pl.when(is_end)
    def _():
        for k in range(1, planes - 1):
            add_slice(jnp.where(z == 0, k, planes - 1 - k))
        remote(partial.at[far_end], partial.at[far_end], far_sems.at[2], far_sems.at[3],
               at(far_end, c, t)).wait_recv()
        share_out(far_end)

    rounds(jnp.int32(total + planes - 2), 0)

    @pl.when(jnp.logical_not(is_end))
    def _():
        for zz in range(planes):
            add_slice(zz)

    finish()

    @pl.when(is_end)
    def _():
        row = pl.multiple_of(other * half, 128)
        col = pl.multiple_of(far_end * block, 128)
        wait_bytes(heads.at[pl.ds(row, half - tail_rows), pl.ds(col, block)], twin_wo_recv.at[far_end])
        wait_bytes(part(far_end, c, main_rows, tail_rows), tail_sems.at[0])
        wait_bytes(part(far_end, other, main_rows, tail_rows), tail_sems.at[1])
        wait_bytes(part(far_end, c, 0, main_rows), tail_sems.at[3])
        ask_far.wait_send()
        tell_far.wait_send()

    unit = deep * 128 // joined.shape[1]
    for way, count in ((0, planes - z), (1, z + 1)):
        for m in range(1, planes):

            @pl.when(count == m)
            def _():
                wait_bytes(joined.at[pl.ds(0, m * total * unit)], line_send.at[way])
    wait_bytes(joined.at[pl.ds(0, (planes - 1) * moving * unit)], plane_send.at[0])
    wait_bytes(joined.at[pl.ds(0, width // cores)], twin_send.at[0])

    @pl.when(is_end)
    def _():
        wait_bytes(heads.at[pl.ds(0, half - wo_rows // planes)], twin_wo_send.at[0])

    @pl.when(jnp.logical_not(is_end))
    def _():
        wait_bytes(heads.at[pl.ds(0, half)], twin_wo_send.at[0])

    @pl.when(is_next)
    def _():
        wait_bytes(part(z, c, main_rows, tail_rows), tail_sems.at[2])

    wait_bytes(o_rows.at[pl.ds(0, len(peers) * o_own)], rows_send.at[0])

    @pl.when(even)
    def _():
        give_v.wait_send()

    @pl.when(jnp.logical_not(even))
    def _():
        give_k.wait_send()


def line_body(hidden, positions, key_cache, value_cache, norm_gain, q_proj, k_proj, v_proj, o_proj, post_gain):
    cols = lax.axis_size("tp")
    cores = 2
    planes = lax.axis_size("rep") // cores
    pieces = 4
    width = q_proj.shape[1]
    deep = width // pieces
    q_rows, k_rows, o_own = q_proj.shape[0], k_proj.shape[0], o_proj.shape[0]
    features = o_proj.shape[1] // cols
    columns = cores * cols * (q_rows + 2 * k_rows)
    model = o_own * cores * cols * planes
    bf = jnp.bfloat16
    dma = pltpu.SemaphoreType.DMA
    hbm = pl.BlockSpec(memory_space=pltpu.HBM)
    f32 = jnp.float32
    batch, kv_local, length, head_dim = key_cache.shape
    q_local = cores * cols * q_rows // head_dim
    half = head_dim // 2
    freq = 10000.0 ** (-2.0 * np.arange(half) / head_dim)
    freq = jnp.asarray(np.concatenate([freq, freq])[None], f32)
    share = post_gain.shape[0]
    moving, total = 2 * pieces, 3 * pieces
    out = pl.pallas_call(
        functools.partial(move_kernel, (planes, cores, cols, pieces)),
        in_specs=[hbm] * 11,
        out_shape=[
            pltpu.VMEM((width, columns), bf),
            pltpu.VMEM((features, model), bf),
            pltpu.VMEM((hidden.shape[0], post_gain.shape[0]), bf),
        ],
        out_specs=[pl.BlockSpec(memory_space=pltpu.VMEM)] * 3,
        scratch_shapes=[
            pltpu.VMEM((planes, moving, deep, 128), bf),
            pltpu.VMEM((q_rows, width), bf),
            pltpu.VMEM((2 * k_rows, width), bf),
            pltpu.VMEM((cores * cols * o_own, features // cores), bf),
            pltpu.VMEM(hidden.shape, bf), pltpu.SMEM(positions.shape, jnp.int32),
            pltpu.VMEM(key_cache.shape, bf), pltpu.VMEM(value_cache.shape, bf),
            pltpu.VMEM((width,), f32), pltpu.VMEM((share,), f32), pltpu.VMEM((1, head_dim), f32),
            pltpu.VMEM((batch, columns), f32), pltpu.VMEM((batch, q_local, head_dim), f32),
            pltpu.VMEM((batch, q_local, head_dim), f32), pltpu.VMEM((batch, q_local, head_dim), f32),
            pltpu.VMEM((batch, features), f32), pltpu.VMEM((batch, features), f32),
            pltpu.VMEM((batch, share), f32), pltpu.VMEM((planes, batch, share), f32),
            pltpu.VMEM((planes, batch, share), f32), pltpu.VMEM((planes, cols, batch, share), f32),
            dma((7,)), dma((4,)), dma((1,)), dma((planes,)),
            dma((4,)), dma((pieces,)), dma((3,)), dma((2,)), dma((1,)), dma((1,)),
            dma((2,)), dma((planes - 1, total)), dma((1,)), dma((moving,)),
            dma((1,)), dma((1,)), dma((1,)), dma((planes,)),
        ],
        compiler_params=pltpu.CompilerParams(
            collective_id=0, has_side_effects=True, vmem_limit_bytes=34 * 2**20),
        name="move",
    )(q_proj, k_proj, v_proj, o_proj, hidden, positions, key_cache, value_cache,
      norm_gain, post_gain, freq)
    joined, heads, result = out

    def spill_kernel(a, b, r, a_out, b_out, r_out, sems):
        small = pltpu.make_async_copy(r, r_out, sems.at[0])
        small.start()
        for i, (source, target) in enumerate(((a, a_out), (b, b_out))):
            rows = 32 * source.dtype.itemsize
            for low in range(0, source.shape[0], rows):
                span = pl.ds(low, min(rows, source.shape[0] - low))
                pltpu.make_async_copy(source.at[span], target.at[span], sems.at[i + 1]).start()
        small.wait()
        for i, (source, target) in enumerate(((a, a_out), (b, b_out))):
            pltpu.make_async_copy(source, target, sems.at[i + 1]).wait()

    vmem = pl.BlockSpec(memory_space=pltpu.VMEM)
    return tuple(pl.pallas_call(
        spill_kernel,
        in_specs=[vmem] * 3,
        out_specs=[hbm] * 3,
        out_shape=[jax.ShapeDtypeStruct(x.shape, x.dtype) for x in (joined, heads, result)],
        scratch_shapes=[dma((3,))],
        compiler_params=pltpu.CompilerParams(vmem_limit_bytes=2**20),
        name="spill",
    )(joined, heads, result))


def body(*args):
    cols, reps = lax.axis_size("tp"), lax.axis_size("rep")
    key_cache, q_proj, k_proj, o_proj = args[2], args[5], args[6], args[8]
    lanes = 128
    fits = (
        reps == 2 * cols
        and cols % 2 == 0
        and cols > 3
        and key_cache.shape[3] == lanes
        and q_proj.shape[0] == lanes
        and 2 * k_proj.shape[0] == lanes
        and o_proj.shape[0] % 16 == 0
        and q_proj.shape[1] % (4 * lanes) == 0
        and o_proj.shape[1] % (8 * lanes * cols) == 0
        and (2 * cols * o_proj.shape[0]) % lanes == 0
    )
    return (line_body if fits else general_body)(*args)


def solution(mesh):
    in_specs = (
        P("rep", None), P("rep"), P("rep", "tp", None, None), P("rep", "tp", None, None), P(),
        P(("rep", "tp"), None), P(("rep", "tp"), None), P(("rep", "tp"), None), P(("rep", "tp"), None), P("tp"),
    )
    out_specs = (P(None, "tp"), P("tp", None), P("rep", "tp"))
    return jax.shard_map(body, mesh=mesh, in_specs=in_specs, out_specs=out_specs, check_vma=False)
```
